32 devices in a mesh: batch: 4 (over x, core), seq: 8 (over z, y).
Axes of the slice: x: 2, y: 2, z: 4, core: 2. Of those that a mesh axis runs over, the one named last changes fastest.
Arguments:
- signal: bfloat16 [4, 2048, 256], P('batch', 'seq'), may hold values from -0.3125 to 0.3125
- grad_out: bfloat16 [4, 2048, 256], P('batch', 'seq'), may hold values from -6 to 6
- filter_taps: float32 [2048, 256], P('seq'), may hold values from -0.3125 to 0.3125
- skip_gain: float32 [256], replicated, may hold values from 0.5 to 2
Outputs:
- input_grad: bfloat16 [4, 2048, 256], P('batch', 'seq')
- filter_grad: float32 [2048, 256], P('seq')
The draws below stay inside these ranges and needn't reach their ends.
All inputs are finite; a program needn't handle non-finite values.
Results may differ from the reference program's by a relative error of at most 0.001.
Values sent between devices are 32-bit elements; how exact they have to be, the bound alone decides.
A program may use at most 64 MiB of HBM per device.

```python
import jax
import jax.numpy as jnp

CHANNELS = 256
LENGTH = 2048
BATCH = 4


def levels(stream_key, dims, pieces, least, high):
    factor_of, own = 1.0, jax.random.fold_in(stream_key, 6)
    for dim, blocks in pieces:
        heights = jnp.exp(jax.random.uniform(jax.random.fold_in(own, dim), (blocks,), jnp.float32, least / len(pieces), high / len(pieces)))
        factor_of = factor_of * jnp.repeat(heights, dims[dim] // blocks).reshape([-1 if axis == dim else 1 for axis in range(len(dims))])
    return factor_of


def scatter_about(own_key, dims, width, bound, shards=(), dtype=jnp.bfloat16):
    array = width * jax.random.normal(own_key, dims, jnp.float32)
    if shards:
        array = array * levels(own_key, dims, shards, -0.22, 0.18)
    return jnp.clip(array, -bound, bound).astype(dtype)


def setup_inputs(seed: int = 0) -> dict:
    keys = jax.random.split(jax.random.key(seed), 5)
    return {
        "signal": scatter_about(keys[0], (BATCH, LENGTH, CHANNELS), (LENGTH ** -0.5), 0.3125, ((0, 4), (1, 8))),
        "grad_out": scatter_about(keys[1], (BATCH, LENGTH, CHANNELS), 1.0, 6.0, ((0, 4), (1, 8))),
        "filter_taps": scatter_about(keys[2], (LENGTH, CHANNELS), (LENGTH ** -0.5), 0.3125, ((0, 8),), jnp.float32),
        "skip_gain": jnp.clip(jax.random.uniform(keys[3], (CHANNELS,), jnp.float32, 0.5, 2.0), 0.5, 2.0),
    }


def reference(signal, grad_out, filter_taps, skip_gain):
    length = signal.shape[1]
    padded_len = 2 * length
    signal_full = signal.astype(jnp.float32)
    grad_full = grad_out.astype(jnp.float32)
    signal_spec = jnp.fft.rfft(signal_full, n=padded_len, axis=1)
    grad_spec = jnp.fft.rfft(grad_full, n=padded_len, axis=1)
    taps_spec = jnp.fft.rfft(filter_taps, n=padded_len, axis=0)
    input_conv = jnp.fft.irfft(grad_spec * jnp.conj(taps_spec)[None], n=padded_len, axis=1)[:, :length]
    input_grad = (input_conv + skip_gain[None, None, :] * grad_full).astype(jnp.bfloat16)
    summed = jnp.sum(grad_spec * jnp.conj(signal_spec), axis=0)
    filter_grad = jnp.fft.irfft(summed, n=padded_len, axis=0)[:length]
    return input_grad, filter_grad.astype(jnp.float32)
```

```python
import functools
import math

import jax
import jax.numpy as jnp
import numpy as np
from jax import lax
from jax.experimental import pallas as pl
from jax.experimental.pallas import tpu as pltpu
from jax.sharding import PartitionSpec as P

MESH = pl.DeviceIdType.MESH
F32 = jnp.float32
BF16 = jnp.bfloat16
GRAD, TAPS, SIGNAL, INPUT, FILTER, FORWARD = range(6)


def weighted(terms):
    total = None
    for factor, array in terms:
        if array is None or abs(factor) < 1e-12:
            continue
        if total is None:
            if abs(factor - 1.0) < 1e-12:
                total = array
            else:
                total = array * factor
        elif abs(factor - 1.0) < 1e-12:
            total = total + array
        elif abs(factor + 1.0) < 1e-12:
            total = total - array
        else:
            total = total + array * factor
    return total


def added(left, right):
    return weighted([(1.0, left), (1.0, right)])


def subtracted(left, right):
    return weighted([(1.0, left), (-1.0, right)])


def turn(real, imag, cos_turn, sin_turn):
    if imag is None:
        return real * cos_turn, -(real * sin_turn)
    return real * cos_turn + imag * sin_turn, imag * cos_turn - real * sin_turn


def coarse_forward(blocks):
    count = len(blocks)
    result = [None] * (count + 1)
    for k in range(count // 2 + 1):
        sums = []
        for parity in (0, 1):
            angles = [(math.pi * ((s * k) % (2 * count)) / count, s) for s in range(parity, count, 2)]
            sums.append(
                (
                    weighted([(math.cos(a), blocks[s]) for a, s in angles]),
                    weighted([(-math.sin(a), blocks[s]) for a, s in angles]),
                )
            )
        (even_re, even_im), (odd_re, odd_im) = sums
        result[k] = (added(even_re, odd_re), added(even_im, odd_im))
        if k != count - k:
            result[count - k] = (subtracted(even_re, odd_re), subtracted(odd_im, even_im))
    return result


def coarse_inverse(terms, scale):
    count = len(terms) - 1
    pairs = []
    for k in range(count // 2 + 1):
        weight = scale if k == 0 else 2.0 * scale
        real, imag = terms[k]
        if k == count - k:
            pairs.append((weight, real, imag, real, imag))
        else:
            other_re, other_im = terms[count - k]
            pairs.append((weight, real + other_re, imag - other_im, real - other_re, imag + other_im))
    blocks = []
    for s in range(count):
        parts = []
        for k, (weight, even_re, even_im, odd_re, odd_im) in enumerate(pairs):
            angle = math.pi * ((s * k) % (2 * count)) / count
            parts.append((weight * math.cos(angle) * (1 if abs(math.cos(angle)) > 1e-9 else 0), odd_re if s % 2 else even_re))
            parts.append((weight * math.sin(angle) * (1 if abs(math.sin(angle)) > 1e-9 else 0), odd_im if s % 2 else even_im))
        blocks.append(weighted(parts))
    return blocks


def fused_kernel(
    groups, seqs,
    signal_hbm, grad_hbm, tap_hbm, skip_hbm, high_hbm, low_hbm, cos_hbm, sin_hbm,
    input_in, filter_in, skip_term_ref,
    signal_ref, grad_ref, tap_ref, skip_ref, high_ref, low_ref, cos_ref, sin_ref,
    grad_out_buf, signal_out_buf, tap_out_buf, grad_in, signal_in, tap_in,
    input_out, filter_out,
    tap_rows, tap_spec, grad_rows, grad_spec, signal_rows, signal_spec, input_rows, filter_rows, filter_spec,
    send_sems, recv_sems, load_sems,
):
    count = groups * seqs
    coarse = seqs + 1
    own, rows = grad_in.shape[1:]
    channels = count * own
    group, seq = lax.axis_index("batch"), lax.axis_index("seq")
    me = group * seqs + seq
    scale = 1.0 / (2 * seqs * rows)
    re, im = pl.ds(0, rows), pl.ds(rows, rows)

    parity, pair = lax.rem(group, 2), lax.div(group, 2)
    half_seqs, half_groups = seqs // 2, groups // 2
    upper, inner = lax.div(seq, half_seqs), lax.rem(seq, half_seqs)

    def load(index, source, target):
        return pltpu.make_async_copy(source, target, load_sems.at[index])

    loads = [
        load(index, source, target)
        for index, (source, target) in enumerate(
            (
                (grad_hbm, grad_ref), (tap_hbm, tap_ref), (signal_hbm, signal_ref),
                (cos_hbm, cos_ref), (sin_hbm, sin_ref), (high_hbm, high_ref),
                (low_hbm, low_ref), (skip_hbm, skip_ref),
            )
        )
    ]
    loads[GRAD].start()
    loads[TAPS].start()

    def seq_at(step):
        other = lax.rem(upper + 1 + lax.div(step, half_seqs), 2)
        return other * half_seqs + lax.rem(inner + step, half_seqs)

    def peer(step):
        to_seq = seq_at(lax.div(step, groups))
        to_group = lax.rem(group + step, groups)
        return to_group * seqs + to_seq, to_group, to_seq

    def over_peers(body, total, own_step):
        lax.fori_loop(0, own_step, body, 0, unroll=min(4, own_step))
        lax.fori_loop(own_step + 1, total, body, 0, unroll=min(3, total - own_step - 1))

    barrier = pltpu.get_barrier_semaphore()

    def greet(step, carry):
        _, to_group, to_seq = peer(step)
        pl.semaphore_signal(
            barrier, inc=1, device_id={"batch": to_group, "seq": to_seq}, device_id_type=MESH
        )
        return carry

    over_peers(greet, count, half_seqs * groups)
    for copy in loads[2:]:
        copy.start()

    def transfer(source, target, kind, to_group, to_seq):
        return pltpu.make_async_remote_copy(
            src_ref=source,
            dst_ref=target,
            send_sem=send_sems.at[kind],
            recv_sem=recv_sems.at[kind],
            device_id={"batch": to_group, "seq": to_seq},
            device_id_type=MESH,
        )

    def all_of(buffer, blocks, kind):
        _, to_group, to_seq = peer(0)
        view = buffer.at[pl.ds(0, blocks)]
        return transfer(view, view, kind, to_group, to_seq)

    loads[GRAD].wait()
    grad_out_buf[...] = grad_ref[...].astype(F32).T.reshape(count, own, rows)
    loads[TAPS].wait()
    tap_out_buf[...] = tap_ref[...].T.reshape(count, own, rows)
    pl.semaphore_wait(barrier, count - 1)

    def send_taps(step, carry):
        to_seq = seq_at(step)
        place = group * seqs + to_seq
        transfer(tap_out_buf.at[place], tap_in.at[seq], TAPS, group, to_seq).start()
        return carry

    def send_grads(step, carry):
        place, to_group, to_seq = peer(step)
        transfer(grad_out_buf.at[place], grad_in.at[me], GRAD, to_group, to_seq).start()
        return carry

    def send_signals(step, carry):
        place, to_group, to_seq = peer(step)
        transfer(signal_out_buf.at[place], signal_in.at[me], SIGNAL, to_group, to_seq).start()
        return carry

    over_peers(send_taps, seqs, half_seqs)
    over_peers(send_grads, count, half_seqs * groups)
    loads[SIGNAL].wait()
    signal_out_buf[...] = signal_ref[...].astype(F32).T.reshape(count, own, rows)
    over_peers(send_signals, count, half_seqs * groups)
    grad_in[me] = grad_out_buf[me]
    tap_in[seq] = tap_out_buf[me]
    signal_in[me] = signal_out_buf[me]

    def spread(blocks, target, first_row):
        place = pl.ds(first_row, own)
        for k, (real, imag) in enumerate(coarse_forward(blocks)):
            real, imag = turn(real, imag, cos_ref[k], sin_ref[k])
            target[k, place, re] = real
            target[k, place, im] = imag

    def fine(source, target):
        lines = source.shape[0] * source.shape[1]
        value = source[...].reshape(lines, 2 * rows)
        high = value.astype(BF16)
        low = (value - high.astype(F32)).astype(BF16)
        product = functools.partial(jnp.dot, preferred_element_type=F32)
        total = product(high, high_ref[...]) + product(low, high_ref[...]) + product(high, low_ref[...])
        target[...] = total.reshape(target.shape)

    def collect(source, first_row):
        place = pl.ds(first_row, own)
        terms = [
            turn(source[k, place, re], source[k, place, im], cos_ref[k], sin_ref[k])
            for k in range(coarse)
        ]
        return coarse_inverse(terms, scale)

    def row_of(index):
        return pl.multiple_of(index * own, own)

    for copy in loads[3:]:
        copy.wait()
    all_of(tap_in, seqs - 1, TAPS).wait_recv()
    spread([tap_in[s] for s in range(seqs)], tap_rows, 0)
    fine(tap_rows, tap_spec)
    all_of(grad_in, count - 1, GRAD).wait_recv()

    def group_at(index):
        return lax.rem(2 * pair + index, groups)

    def input_part(first):
        source, spectrum, lines = grad_rows.at[first], grad_spec.at[first], input_rows.at[first]

        def spread_grad(index, carry):
            here = group_at(2 * first + index)
            spread([grad_in[here * seqs + s] for s in range(seqs)], source, row_of(index))
            return carry

        lax.fori_loop(0, 2, spread_grad, 0)
        fine(source, spectrum)

        def multiply_taps(index, carry):
            place = pl.ds(row_of(index), own)
            for k in range(coarse):
                grad_re, grad_im = spectrum[k, place, re], spectrum[k, place, im]
                tap_re, tap_im = tap_spec[k, :, re], tap_spec[k, :, im]
                lines[k, place, re] = grad_re * tap_re + grad_im * tap_im
                lines[k, place, im] = grad_re * tap_im - grad_im * tap_re
            return carry

        lax.fori_loop(0, 2, multiply_taps, 0)
        fine(lines, lines)

        def collect_input(index, carry):
            here = group_at(2 * first + index)
            for s, block in enumerate(collect(lines, row_of(index))):
                input_out[here * seqs + s] = block
            return carry

        lax.fori_loop(0, 2, collect_input, 0)

        def send_inputs(step, carry):
            to_seq = seq_at(lax.div(step, 2))
            to_group = group_at(2 * first + lax.rem(parity + step, 2))
            place = to_group * seqs + to_seq
            transfer(input_out.at[place], input_in.at[me], INPUT, to_group, to_seq).start()
            return carry

        if first == 0:
            over_peers(send_inputs, 2 * seqs, 2 * half_seqs)
        else:
            lax.fori_loop(0, 2 * seqs, send_inputs, 0)

    for first in reversed(range(half_groups)):
        input_part(first)
    input_in[me] = input_out[me]

    all_of(signal_in, count - 1, SIGNAL).wait_recv()

    def spread_signal(index, carry):
        here = group_at(index)
        spread([signal_in[here * seqs + s] for s in range(seqs)], signal_rows, row_of(index))
        return carry

    lax.fori_loop(0, groups, spread_signal, 0)
    fine(signal_rows, signal_spec)
    for k in range(coarse):
        real, imag = None, None
        for index in range(groups):
            place = pl.ds(index * own, own)
            which, local = index // 2, pl.ds(index % 2 * own, own)
            grad_re, grad_im = grad_spec[which, k, local, re], grad_spec[which, k, local, im]
            signal_re, signal_im = signal_spec[k, place, re], signal_spec[k, place, im]
            real = added(real, grad_re * signal_re + grad_im * signal_im)
            imag = added(imag, grad_re * signal_im - grad_im * signal_re)
        filter_rows[k, :, re] = real
        filter_rows[k, :, im] = imag
    fine(filter_rows, filter_spec)
    for s, block in enumerate(collect(filter_spec, 0)):
        filter_out[s] = block

    def send_filters(step, carry):
        to_seq = seq_at(lax.div(step, half_groups))
        to_group = 2 * lax.rem(pair + step, half_groups) + parity
        place = pair * seqs + seq
        transfer(
            filter_out.at[to_seq], filter_in.at[parity, place], FILTER, to_group, to_seq
        ).start()
        return carry

    over_peers(send_filters, seqs * half_groups, half_seqs * half_groups)
    filter_in[parity, pair * seqs + seq] = filter_out[seq]

    half = count // 2
    skip_term_ref[...] = skip_ref[...] * grad_ref[...].astype(F32)
    all_of(input_in, count - 1, INPUT).wait_recv()
    all_of(filter_in.at[0], half - 1, FILTER).wait_recv()
    mine = filter_in.at[parity]
    partner = 2 * pair + 1 - parity
    forward = transfer(mine, mine, FORWARD, partner, seq)
    forward.start()
    forward.wait_recv()
    for kind, buffer in ((GRAD, grad_in), (SIGNAL, signal_in), (INPUT, input_in)):
        all_of(buffer, count - 1, kind).wait_send()
    all_of(filter_in.at[0], half - 1, FILTER).wait_send()
    forward.wait_send()
    all_of(tap_in, seqs - 1, TAPS).wait_send()


def finish_kernel(
    groups, seqs, input_in, filter_in, skip_term_ref, input_hbm, filter_hbm, input_ref, filter_ref, sems
):
    own, rows = input_in.shape[1:]
    channels = input_in.shape[0] * own
    gradient = input_in[...].reshape(channels, rows).T + skip_term_ref[...]
    input_ref[...] = gradient.astype(BF16)
    input_store = pltpu.make_async_copy(input_ref, input_hbm, sems.at[0])
    input_store.start()
    parts = [
        filter_in[which, first * seqs : (first + 1) * seqs].reshape(seqs * own, rows)
        for first in range(groups // 2)
        for which in range(2)
    ]
    filter_ref[...] = jnp.concatenate(parts, axis=0).T
    filter_store = pltpu.make_async_copy(filter_ref, filter_hbm, sems.at[1])
    filter_store.start()
    input_store.wait()
    filter_store.wait()


def fine_tables(rows):
    grid = np.arange(rows)
    angle = 2.0 * np.pi / rows * (np.outer(grid, grid) % rows)
    table = np.block([[np.cos(angle), -np.sin(angle)], [np.sin(angle), np.cos(angle)]]).astype(np.float32)
    high = table.astype(BF16)
    return high, (table - high.astype(np.float32)).astype(BF16)


def turn_tables(seqs, rows, lines):
    angle = np.pi / (seqs * rows) * np.outer(np.arange(seqs + 1), np.arange(rows))
    wide = np.broadcast_to(angle[:, None, :], (seqs + 1, lines, rows))
    return np.cos(wide).astype(np.float32), np.sin(wide).astype(np.float32)


def fused_shards(groups, seqs, signal, grad_out, filter_taps, skip_gain):
    rows, channels = filter_taps.shape
    count, coarse = groups * seqs, seqs + 1
    own = channels // count
    high, low = fine_tables(rows)
    cos_turn, sin_turn = turn_tables(seqs, rows, own)
    blocks = pltpu.VMEM((count, own, rows), F32)
    few = pltpu.VMEM((seqs, own, rows), F32)
    lines = lambda number: pltpu.VMEM((coarse, number * own, 2 * rows), F32)
    pairs = pltpu.VMEM((groups // 2, coarse, 2 * own, 2 * rows), F32)
    hbm = pl.BlockSpec(memory_space=pltpu.HBM)
    turns = pltpu.VMEM((coarse, own, rows), F32)
    table = pltpu.VMEM((2 * rows, 2 * rows), BF16)
    vmem = pl.BlockSpec(memory_space=pltpu.VMEM)
    gathered = pl.pallas_call(
        functools.partial(fused_kernel, groups, seqs),
        out_shape=(
            pltpu.VMEM((count, own, rows), F32),
            pltpu.VMEM((2, count // 2, own, rows), F32),
            pltpu.VMEM((rows, channels), F32),
        ),
        in_specs=[hbm] * 8,
        out_specs=(vmem, vmem, vmem),
        scratch_shapes=[
            pltpu.VMEM((rows, channels), BF16), pltpu.VMEM((rows, channels), BF16),
            pltpu.VMEM((rows, channels), F32), pltpu.VMEM((1, channels), F32),
            table, table, turns, turns,
            blocks, blocks, blocks, blocks, blocks, few,
            blocks, few,
            lines(1), lines(1), pairs, pairs, lines(groups), lines(groups),
            pairs, lines(1), lines(1),
            pltpu.SemaphoreType.DMA((6,)),
            pltpu.SemaphoreType.DMA((6,)),
            pltpu.SemaphoreType.DMA((8,)),
        ],
        compiler_params=pltpu.CompilerParams(
            collective_id=0, has_side_effects=True, vmem_limit_bytes=24 << 20
        ),
    )(
        *(
            pltpu.with_memory_space_constraint(array, pltpu.HBM)
            for array in (
                signal[0], grad_out[0], filter_taps, skip_gain[None, :],
                jnp.asarray(high), jnp.asarray(low), jnp.asarray(cos_turn), jnp.asarray(sin_turn),
            )
        )
    )
    input_grad, filter_grad = pl.pallas_call(
        functools.partial(finish_kernel, groups, seqs),
        out_shape=(
            jax.ShapeDtypeStruct((rows, channels), BF16),
            jax.ShapeDtypeStruct((rows, channels), F32),
        ),
        in_specs=[vmem] * 3,
        out_specs=(hbm, hbm),
        scratch_shapes=[
            pltpu.VMEM((rows, channels), BF16), pltpu.VMEM((rows, channels), F32),
            pltpu.SemaphoreType.DMA((2,)),
        ],
        compiler_params=pltpu.CompilerParams(vmem_limit_bytes=24 << 20),
    )(*gathered)
    return input_grad[None], filter_grad


def fits_fused(groups, seqs, signal, filter_taps):
    rows, channels = filter_taps.shape
    return (
        signal.shape[0] == 1
        and seqs % 2 == 0
        and groups % 2 == 0
        and rows % 128 == 0
        and channels % (8 * groups * seqs) == 0
    )


def angle_table(height, width, period):
    product = lax.broadcasted_iota(jnp.int32, (height, width), 0) * lax.broadcasted_iota(
        jnp.int32, (height, width), 1
    )
    return 2.0 * jnp.pi / period * (product % period).astype(jnp.float32)


def angle_of(product, period):
    return 2.0 * jnp.pi / period * (product % period).astype(jnp.float32)


def coarse_order(slot, seq_count):
    pair_index = slot // 2
    odd_slot = slot % 2
    return jnp.where(
        pair_index == 0,
        odd_slot * seq_count,
        jnp.where(odd_slot == 0, pair_index, 2 * seq_count - pair_index),
    )


def contract(form, table, operand):
    return jnp.einsum(form, table, operand, precision=lax.Precision.HIGHEST)


def forward_spectra(columns):
    seq_count = lax.axis_size("seq")
    row_count = columns.shape[0]
    part_rows = row_count // seq_count
    period_len = 2 * row_count * seq_count
    spread = lax.all_to_all(
        columns.reshape(1, row_count, columns.shape[1]),
        "seq",
        split_axis=1,
        concat_axis=0,
        tiled=True,
    )
    slot_grid = lax.broadcasted_iota(jnp.int32, (2 * seq_count, seq_count), 0)
    source_grid = lax.broadcasted_iota(jnp.int32, (2 * seq_count, seq_count), 1)
    first_table = angle_of(coarse_order(slot_grid, seq_count) * source_grid, 2 * seq_count)
    cos_first = jnp.cos(first_table)
    sin_first = jnp.sin(first_table)
    half_width = spread.shape[2] // 2
    real_in = spread[:, :, :half_width]
    imag_in = spread[:, :, half_width:]
    real_part = contract("ks,srw->krw", cos_first, real_in) + contract(
        "ks,srw->krw", sin_first, imag_in
    )
    imag_part = contract("ks,srw->krw", cos_first, imag_in) - contract(
        "ks,srw->krw", sin_first, real_in
    )
    global_row = lax.axis_index("seq") * part_rows + lax.broadcasted_iota(
        jnp.int32, (2 * seq_count, part_rows), 1
    )
    coarse = coarse_order(lax.broadcasted_iota(jnp.int32, (2 * seq_count, part_rows), 0), seq_count)
    phases = angle_of(global_row * coarse, period_len)
    cos_turn = jnp.cos(phases)[:, :, None]
    sin_turn = jnp.sin(phases)[:, :, None]
    rotated = jnp.stack(
        [real_part * cos_turn + imag_part * sin_turn, imag_part * cos_turn - real_part * sin_turn]
    )
    inner_table = angle_table(row_count, row_count, row_count)
    cos_inner = jnp.cos(inner_table)
    sin_inner = jnp.sin(inner_table)
    pieces = lax.all_to_all(rotated, "seq", split_axis=1, concat_axis=2, tiled=True)
    real_sum = contract("qr,krw->kqw", cos_inner, pieces[0]) + contract(
        "qr,krw->kqw", sin_inner, pieces[1]
    )
    imag_sum = contract("qr,krw->kqw", cos_inner, pieces[1]) - contract(
        "qr,krw->kqw", sin_inner, pieces[0]
    )
    return jnp.stack([real_sum, imag_sum])


def split_pairs(packed):
    reversed_q = packed[:, :, ::-1]
    zero_row = jnp.roll(reversed_q[:, 0], 1, axis=1)
    own_pair = jnp.stack([zero_row, reversed_q[:, 1]], axis=1)
    partner = jnp.where(lax.axis_index("seq") == 0, own_pair, reversed_q[:, ::-1])
    first = jnp.stack([0.5 * (packed[0] + partner[0]), 0.5 * (packed[1] - partner[1])])
    second = jnp.stack([0.5 * (packed[1] + partner[1]), 0.5 * (partner[0] - packed[0])])
    return (first, second)


def inverse_rows(spectra):
    seq_count = lax.axis_size("seq")
    row_count = spectra.shape[2]
    period_len = 2 * row_count * seq_count
    inner_table = angle_table(row_count, row_count, row_count)
    cos_inner = jnp.cos(inner_table)
    sin_inner = jnp.sin(inner_table)
    real_sum = contract("qr,krw->kqw", cos_inner, spectra[0]) - contract(
        "qr,krw->kqw", sin_inner, spectra[1]
    )
    imag_sum = contract("qr,krw->kqw", cos_inner, spectra[1]) + contract(
        "qr,krw->kqw", sin_inner, spectra[0]
    )
    coarse = coarse_order(
        2 * lax.axis_index("seq") + lax.broadcasted_iota(jnp.int32, (2, row_count), 0), seq_count
    )
    position = lax.broadcasted_iota(jnp.int32, (2, row_count), 1)
    phases = angle_of(position * coarse, period_len)
    cos_turn = jnp.cos(phases)[:, :, None]
    sin_turn = jnp.sin(phases)[:, :, None]
    rotated = jnp.stack(
        [real_sum * cos_turn - imag_sum * sin_turn, real_sum * sin_turn + imag_sum * cos_turn]
    )
    target_grid = lax.broadcasted_iota(jnp.int32, (seq_count, 2 * seq_count), 0)
    slot_grid = lax.broadcasted_iota(jnp.int32, (seq_count, 2 * seq_count), 1)
    last_table = angle_of(target_grid * coarse_order(slot_grid, seq_count), 2 * seq_count)
    cos_last = jnp.cos(last_table)
    sin_last = jnp.sin(last_table)
    pieces = lax.all_to_all(rotated, "seq", split_axis=2, concat_axis=1, tiled=True)
    value = contract("sk,krw->srw", cos_last, pieces[0]) - contract(
        "sk,krw->srw", sin_last, pieces[1]
    )
    other = contract("sk,krw->srw", sin_last, pieces[0]) + contract(
        "sk,krw->srw", cos_last, pieces[1]
    )
    gathered = (value / period_len, other / period_len)
    gathered = jnp.concatenate([gathered[0], gathered[1]], axis=2)
    home_rows = lax.all_to_all(gathered, "seq", split_axis=0, concat_axis=1, tiled=True)
    return home_rows.reshape(row_count, home_rows.shape[2])


def invert_all(spectra):
    half_width = spectra.shape[3] // 2
    joined = jnp.stack(
        [
            spectra[0, :, :, :half_width] - spectra[1, :, :, half_width:],
            spectra[1, :, :, :half_width] + spectra[0, :, :, half_width:],
        ]
    )
    return inverse_rows(joined)


def shards(signal, grad_out, filter_taps, skip_gain):
    channels = filter_taps.shape[1]
    signal_rows = signal[0].astype(jnp.float32)
    grad_rows = grad_out[0].astype(jnp.float32)
    tap_half = filter_taps.shape[1] // 2
    columns = jnp.concatenate(
        [signal_rows, filter_taps[:, :tap_half], grad_rows, filter_taps[:, tap_half:]], axis=1
    )
    first, second = split_pairs(forward_spectra(columns))
    signal_spec = first[:, :, :, :channels]
    grad_spec = second[:, :, :, :channels]
    own_spec = jnp.concatenate([first[:, :, :, channels:], second[:, :, :, channels:]], axis=3)
    input_spec = jnp.stack(
        [
            grad_spec[0] * own_spec[0] + grad_spec[1] * own_spec[1],
            grad_spec[1] * own_spec[0] - grad_spec[0] * own_spec[1],
        ]
    )
    filter_terms = jnp.stack(
        [
            grad_spec[0] * signal_spec[0] + grad_spec[1] * signal_spec[1],
            grad_spec[1] * signal_spec[0] - grad_spec[0] * signal_spec[1],
        ]
    )
    summed = lax.psum(filter_terms, "batch")
    rows_back = invert_all(jnp.concatenate([input_spec, summed], axis=3))
    filter_grad = rows_back[:, channels:]
    input_grad = (rows_back[:, :channels] + skip_gain[None, :] * grad_rows).astype(jnp.bfloat16)
    return (input_grad[None], filter_grad)


def solution(mesh):
    groups, seqs = mesh.shape["batch"], mesh.shape["seq"]

    def either(signal, grad_out, filter_taps, skip_gain):
        if fits_fused(groups, seqs, signal, filter_taps):
            return fused_shards(groups, seqs, signal, grad_out, filter_taps, skip_gain)
        return shards(signal, grad_out, filter_taps, skip_gain)

    return jax.shard_map(
        either,
        mesh=mesh,
        in_specs=(P("batch", "seq", None), P("batch", "seq", None), P("seq", None), P()),
        out_specs=(P("batch", "seq", None), P("seq", None)),
        check_vma=False,
    )
```

```python
import functools
import math

import jax
import jax.numpy as jnp
import numpy as np
from jax import lax
from jax.experimental import pallas as pl
from jax.experimental.pallas import tpu as pltpu
from jax.sharding import PartitionSpec as P

MESH = pl.DeviceIdType.MESH
F32 = jnp.float32
BF16 = jnp.bfloat16
GRAD, TAPS, SIGNAL, INPUT, FILTER, FORWARD = range(6)


def weighted(terms):
    total = None
    for factor, array in terms:
        if array is None or abs(factor) < 1e-12:
            continue
        if total is None:
            if abs(factor - 1.0) < 1e-12:
                total = array
            else:
                total = array * factor
        elif abs(factor - 1.0) < 1e-12:
            total = total + array
        elif abs(factor + 1.0) < 1e-12:
            total = total - array
        else:
            total = total + array * factor
    return total


def added(left, right):
    return weighted([(1.0, left), (1.0, right)])


def subtracted(left, right):
    return weighted([(1.0, left), (-1.0, right)])


def turn(real, imag, cos_turn, sin_turn):
    if imag is None:
        return real * cos_turn, -(real * sin_turn)
    return real * cos_turn + imag * sin_turn, imag * cos_turn - real * sin_turn


def coarse_forward(blocks):
    count = len(blocks)
    result = [None] * (count + 1)
    for k in range(count // 2 + 1):
        sums = []
        for parity in (0, 1):
            angles = [(math.pi * ((s * k) % (2 * count)) / count, s) for s in range(parity, count, 2)]
            sums.append(
                (
                    weighted([(math.cos(a), blocks[s]) for a, s in angles]),
                    weighted([(-math.sin(a), blocks[s]) for a, s in angles]),
                )
            )
        (even_re, even_im), (odd_re, odd_im) = sums
        result[k] = (added(even_re, odd_re), added(even_im, odd_im))
        if k != count - k:
            result[count - k] = (subtracted(even_re, odd_re), subtracted(odd_im, even_im))
    return result


def coarse_inverse(terms, scale):
    count = len(terms) - 1
    pairs = []
    for k in range(count // 2 + 1):
        weight = scale if k == 0 else 2.0 * scale
        real, imag = terms[k]
        if k == count - k:
            pairs.append((weight, real, imag, real, imag))
        else:
            other_re, other_im = terms[count - k]
            pairs.append((weight, real + other_re, imag - other_im, real - other_re, imag + other_im))
    blocks = []
    for s in range(count):
        parts = []
        for k, (weight, even_re, even_im, odd_re, odd_im) in enumerate(pairs):
            angle = math.pi * ((s * k) % (2 * count)) / count
            parts.append((weight * math.cos(angle) * (1 if abs(math.cos(angle)) > 1e-9 else 0), odd_re if s % 2 else even_re))
            parts.append((weight * math.sin(angle) * (1 if abs(math.sin(angle)) > 1e-9 else 0), odd_im if s % 2 else even_im))
        blocks.append(weighted(parts))
    return blocks


def fused_kernel(
    groups, seqs,
    signal_hbm, grad_hbm, tap_hbm, skip_hbm, high_hbm, low_hbm, cos_hbm, sin_hbm,
    input_in, filter_in, skip_term_ref,
    signal_ref, grad_ref, tap_ref, skip_ref, high_ref, low_ref, cos_ref, sin_ref,
    grad_out_buf, signal_out_buf, tap_out_buf, grad_in, signal_in, tap_in,
    input_out, filter_out,
    tap_rows, tap_spec, grad_rows, grad_spec, signal_rows, signal_spec, input_rows, filter_rows, filter_spec,
    send_sems, recv_sems, load_sems, ready_sems,
):
    count = groups * seqs
    coarse = seqs + 1
    own, rows = grad_in.shape[1:]
    channels = count * own
    group, seq = lax.axis_index("batch"), lax.axis_index("seq")
    me = group * seqs + seq
    scale = 1.0 / (2 * seqs * rows)
    re, im = pl.ds(0, rows), pl.ds(rows, rows)

    parity, pair = lax.rem(group, 2), lax.div(group, 2)
    half_seqs, half_groups = seqs // 2, groups // 2
    rank = seq * groups + group

    def load(index, source, target):
        return pltpu.make_async_copy(source, target, load_sems.at[index])

    loads = [
        load(index, source, target)
        for index, (source, target) in enumerate(
            (
                (grad_hbm, grad_ref), (tap_hbm, tap_ref), (signal_hbm, signal_ref),
                (cos_hbm, cos_ref), (sin_hbm, sin_ref), (high_hbm, high_ref),
                (low_hbm, low_ref), (skip_hbm, skip_ref),
            )
        )
    ]
    loads[GRAD].start()
    loads[TAPS].start()

    def seq_at(step):
        return lax.bitwise_xor(seq, lax.rem(step + half_seqs, seqs))

    def over_seqs(body):
        lax.fori_loop(0, half_seqs, body, 0)
        lax.fori_loop(half_seqs + 1, seqs, body, 0)

    def groups_of(to_seq):
        for flip in range(groups):
            to_group = lax.bitwise_xor(group, flip)
            yield flip, to_group, to_seq * groups + to_group

    def signal(semaphore, to_group, to_seq):
        pl.semaphore_signal(
            semaphore, inc=1, device_id={"batch": to_group, "seq": to_seq}, device_id_type=MESH
        )

    barrier = pltpu.get_barrier_semaphore()

    def greet(step, carry):
        for _, to_group, to_rank in groups_of(seq_at(step)):
            pl.when(to_rank > rank)(lambda: signal(barrier, to_group, seq_at(step)))
        return carry

    lax.fori_loop(0, seqs, greet, 0)
    for copy in loads[2:]:
        copy.start()

    def transfer(source, target, kind, to_group, to_seq):
        return pltpu.make_async_remote_copy(
            src_ref=source,
            dst_ref=target,
            send_sem=send_sems.at[kind],
            recv_sem=recv_sems.at[kind],
            device_id={"batch": to_group, "seq": to_seq},
            device_id_type=MESH,
        )

    def all_of(buffer, blocks, kind):
        view = buffer.at[pl.ds(0, blocks)]
        return transfer(view, view, kind, group, seq_at(0))

    loads[GRAD].wait()
    grad_out_buf[...] = grad_ref[...].astype(F32).T.reshape(count, own, rows)
    loads[TAPS].wait()
    tap_out_buf[...] = tap_ref[...].T.reshape(count, own, rows)
    pl.when(rank > 0)(lambda: pl.semaphore_wait(barrier, rank))

    def answer(step, carry):
        for _, to_group, to_rank in groups_of(seq_at(step)):
            pl.when(to_rank < rank)(lambda: signal(ready_sems.at[seq], to_group, seq_at(step)))
        return carry

    lax.fori_loop(0, seqs, answer, 0)

    def send_first(flip, to_group, to_seq):
        place = to_group * seqs + to_seq
        if flip == 0:
            transfer(tap_out_buf.at[place], tap_in.at[seq], TAPS, to_group, to_seq).start()
        transfer(grad_out_buf.at[place], grad_in.at[me], GRAD, to_group, to_seq).start()

    def send_lower(step, carry):
        to_seq = seq_at(step)
        for flip, to_group, to_rank in groups_of(to_seq):
            pl.when(to_rank < rank)(lambda: send_first(flip, to_group, to_seq))
        return carry

    def send_higher(step, carry):
        to_seq = lax.bitwise_xor(step, lax.rem(seq, 2))

        @pl.when((to_seq == seq) & (group < groups - 1))
        def _():
            pl.semaphore_wait(ready_sems.at[seq], groups - 1 - group)

        @pl.when(to_seq > seq)
        def _():
            pl.semaphore_wait(ready_sems.at[to_seq], groups)

        for flip, to_group, to_rank in groups_of(to_seq):
            pl.when(to_rank > rank)(lambda: send_first(flip, to_group, to_seq))
        return carry

    lax.fori_loop(0, seqs, send_lower, 0)
    lax.fori_loop(0, seqs, send_higher, 0)
    loads[SIGNAL].wait()
    signal_out_buf[...] = signal_ref[...].astype(F32).T.reshape(count, own, rows)

    def send_signal(to_group, to_seq):
        place = to_group * seqs + to_seq
        transfer(signal_out_buf.at[place], signal_in.at[me], SIGNAL, to_group, to_seq).start()

    def send_signals(step, carry):
        for _, to_group, _ in groups_of(seq_at(step)):
            send_signal(to_group, seq_at(step))
        return carry

    over_seqs(send_signals)
    for flip in range(1, groups):
        send_signal(lax.bitwise_xor(group, flip), seq)
    grad_in[me] = grad_out_buf[me]
    tap_in[seq] = tap_out_buf[me]
    signal_in[me] = signal_out_buf[me]

    def spread(blocks, target, first_row):
        place = pl.ds(first_row, own)
        for k, (real, imag) in enumerate(coarse_forward(blocks)):
            real, imag = turn(real, imag, cos_ref[k], sin_ref[k])
            target[k, place, re] = real
            target[k, place, im] = imag

    def fine(source, target):
        lines = source.shape[0] * source.shape[1]
        value = source[...].reshape(lines, 2 * rows)
        high = value.astype(BF16)
        low = (value - high.astype(F32)).astype(BF16)
        product = functools.partial(jnp.dot, preferred_element_type=F32)
        total = product(high, high_ref[...]) + product(low, high_ref[...]) + product(high, low_ref[...])
        target[...] = total.reshape(target.shape)

    def collect(source, first_row):
        place = pl.ds(first_row, own)
        terms = [
            turn(source[k, place, re], source[k, place, im], cos_ref[k], sin_ref[k])
            for k in range(coarse)
        ]
        return coarse_inverse(terms, scale)

    def row_of(index):
        return pl.multiple_of(index * own, own)

    for copy in loads[3:]:
        copy.wait()
    all_of(tap_in, seqs - 1, TAPS).wait_recv()
    spread([tap_in[s] for s in range(seqs)], tap_rows, 0)
    fine(tap_rows, tap_spec)
    all_of(grad_in, count - 1, GRAD).wait_recv()

    def group_at(index):
        return lax.rem(2 * pair + index, groups)

    def input_part(first):
        source, spectrum, lines = grad_rows.at[first], grad_spec.at[first], input_rows.at[first]

        def spread_grad(index, carry):
            here = group_at(2 * first + index)
            spread([grad_in[here * seqs + s] for s in range(seqs)], source, row_of(index))
            return carry

        lax.fori_loop(0, 2, spread_grad, 0)
        fine(source, spectrum)

        def multiply_taps(index, carry):
            place = pl.ds(row_of(index), own)
            for k in range(coarse):
                grad_re, grad_im = spectrum[k, place, re], spectrum[k, place, im]
                tap_re, tap_im = tap_spec[k, :, re], tap_spec[k, :, im]
                lines[k, place, re] = grad_re * tap_re + grad_im * tap_im
                lines[k, place, im] = grad_re * tap_im - grad_im * tap_re
            return carry

        lax.fori_loop(0, 2, multiply_taps, 0)
        fine(lines, lines)

        def collect_input(index, carry):
            here = group_at(2 * first + index)
            for s, block in enumerate(collect(lines, row_of(index))):
                input_out[here * seqs + s] = block
            return carry

        lax.fori_loop(0, 2, collect_input, 0)

        if first == 0:
            partner = lax.bitwise_xor(group, 1)
            lax.fori_loop(0, seqs, lambda step, carry: send_input(partner, seq_at(step)), 0)
        else:

            def send_inputs(step, carry):
                for index in range(2):
                    send_input(group_at(2 * first + lax.bitwise_xor(parity, index)), seq_at(step))
                return carry

            lax.fori_loop(0, seqs, send_inputs, 0)

    def send_input(to_group, to_seq):
        place = to_group * seqs + to_seq
        transfer(input_out.at[place], input_in.at[me], INPUT, to_group, to_seq).start()
        return 0

    for first in reversed(range(half_groups)):
        input_part(first)
    input_in[me] = input_out[me]

    all_of(signal_in, count - 1, SIGNAL).wait_recv()

    def spread_signal(index, carry):
        here = group_at(index)
        spread([signal_in[here * seqs + s] for s in range(seqs)], signal_rows, row_of(index))
        return carry

    lax.fori_loop(0, groups, spread_signal, 0)
    fine(signal_rows, signal_spec)
    for k in range(coarse):
        real, imag = None, None
        for index in range(groups):
            place = pl.ds(index * own, own)
            which, local = index // 2, pl.ds(index % 2 * own, own)
            grad_re, grad_im = grad_spec[which, k, local, re], grad_spec[which, k, local, im]
            signal_re, signal_im = signal_spec[k, place, re], signal_spec[k, place, im]
            real = added(real, grad_re * signal_re + grad_im * signal_im)
            imag = added(imag, grad_re * signal_im - grad_im * signal_re)
        filter_rows[k, :, re] = real
        filter_rows[k, :, im] = imag
    fine(filter_rows, filter_spec)
    for s, block in enumerate(collect(filter_spec, 0)):
        filter_out[s] = block

    def send_filter(turned, to_seq):
        to_group = 2 * lax.rem(pair + turned, half_groups) + parity
        place = pair * seqs + seq
        transfer(
            filter_out.at[to_seq], filter_in.at[parity, place], FILTER, to_group, to_seq
        ).start()

    def send_filters(step, carry):
        for turned in range(half_groups):
            send_filter(turned, seq_at(step))
        return carry

    over_seqs(send_filters)
    for turned in range(1, half_groups):
        send_filter(turned, seq)
    over_seqs(lambda step, carry: send_input(group, seq_at(step)))
    filter_in[parity, pair * seqs + seq] = filter_out[seq]

    half = count // 2
    skip_term_ref[...] = skip_ref[...] * grad_ref[...].astype(F32)
    all_of(input_in, count - 1, INPUT).wait_recv()
    all_of(filter_in.at[0], half - 1, FILTER).wait_recv()
    mine = filter_in.at[parity]
    partner = 2 * pair + 1 - parity
    forward = transfer(mine, mine, FORWARD, partner, seq)
    forward.start()
    forward.wait_recv()
    for kind, buffer in ((GRAD, grad_in), (SIGNAL, signal_in), (INPUT, input_in)):
        all_of(buffer, count - 1, kind).wait_send()
    all_of(filter_in.at[0], half - 1, FILTER).wait_send()
    forward.wait_send()
    all_of(tap_in, seqs - 1, TAPS).wait_send()


def finish_kernel(
    groups, seqs, input_in, filter_in, skip_term_ref, input_hbm, filter_hbm, input_ref, filter_ref, sems
):
    own, rows = input_in.shape[1:]
    channels = input_in.shape[0] * own
    gradient = input_in[...].reshape(channels, rows).T + skip_term_ref[...]
    input_ref[...] = gradient.astype(BF16)
    input_store = pltpu.make_async_copy(input_ref, input_hbm, sems.at[0])
    input_store.start()
    parts = [
        filter_in[which, first * seqs : (first + 1) * seqs].reshape(seqs * own, rows)
        for first in range(groups // 2)
        for which in range(2)
    ]
    filter_ref[...] = jnp.concatenate(parts, axis=0).T
    filter_store = pltpu.make_async_copy(filter_ref, filter_hbm, sems.at[1])
    filter_store.start()
    input_store.wait()
    filter_store.wait()


def fine_tables(rows):
    grid = np.arange(rows)
    angle = 2.0 * np.pi / rows * (np.outer(grid, grid) % rows)
    table = np.block([[np.cos(angle), -np.sin(angle)], [np.sin(angle), np.cos(angle)]]).astype(np.float32)
    high = table.astype(BF16)
    return high, (table - high.astype(np.float32)).astype(BF16)


def turn_tables(seqs, rows, lines):
    angle = np.pi / (seqs * rows) * np.outer(np.arange(seqs + 1), np.arange(rows))
    wide = np.broadcast_to(angle[:, None, :], (seqs + 1, lines, rows))
    return np.cos(wide).astype(np.float32), np.sin(wide).astype(np.float32)


def fused_shards(groups, seqs, signal, grad_out, filter_taps, skip_gain):
    rows, channels = filter_taps.shape
    count, coarse = groups * seqs, seqs + 1
    own = channels // count
    high, low = fine_tables(rows)
    cos_turn, sin_turn = turn_tables(seqs, rows, own)
    blocks = pltpu.VMEM((count, own, rows), F32)
    few = pltpu.VMEM((seqs, own, rows), F32)
    lines = lambda number: pltpu.VMEM((coarse, number * own, 2 * rows), F32)
    pairs = pltpu.VMEM((groups // 2, coarse, 2 * own, 2 * rows), F32)
    hbm = pl.BlockSpec(memory_space=pltpu.HBM)
    turns = pltpu.VMEM((coarse, own, rows), F32)
    table = pltpu.VMEM((2 * rows, 2 * rows), BF16)
    vmem = pl.BlockSpec(memory_space=pltpu.VMEM)
    gathered = pl.pallas_call(
        functools.partial(fused_kernel, groups, seqs),
        out_shape=(
            pltpu.VMEM((count, own, rows), F32),
            pltpu.VMEM((2, count // 2, own, rows), F32),
            pltpu.VMEM((rows, channels), F32),
        ),
        in_specs=[hbm] * 8,
        out_specs=(vmem, vmem, vmem),
        scratch_shapes=[
            pltpu.VMEM((rows, channels), BF16), pltpu.VMEM((rows, channels), BF16),
            pltpu.VMEM((rows, channels), F32), pltpu.VMEM((1, channels), F32),
            table, table, turns, turns,
            blocks, blocks, blocks, blocks, blocks, few,
            blocks, few,
            lines(1), lines(1), pairs, pairs, lines(groups), lines(groups),
            pairs, lines(1), lines(1),
            pltpu.SemaphoreType.DMA((6,)),
            pltpu.SemaphoreType.DMA((6,)),
            pltpu.SemaphoreType.DMA((8,)),
            pltpu.SemaphoreType.REGULAR((seqs,)),
        ],
        compiler_params=pltpu.CompilerParams(
            collective_id=0, has_side_effects=True, vmem_limit_bytes=24 << 20
        ),
    )(
        *(
            pltpu.with_memory_space_constraint(array, pltpu.HBM)
            for array in (
                signal[0], grad_out[0], filter_taps, skip_gain[None, :],
                jnp.asarray(high), jnp.asarray(low), jnp.asarray(cos_turn), jnp.asarray(sin_turn),
            )
        )
    )
    input_grad, filter_grad = pl.pallas_call(
        functools.partial(finish_kernel, groups, seqs),
        out_shape=(
            jax.ShapeDtypeStruct((rows, channels), BF16),
            jax.ShapeDtypeStruct((rows, channels), F32),
        ),
        in_specs=[vmem] * 3,
        out_specs=(hbm, hbm),
        scratch_shapes=[
            pltpu.VMEM((rows, channels), BF16), pltpu.VMEM((rows, channels), F32),
            pltpu.SemaphoreType.DMA((2,)),
        ],
        compiler_params=pltpu.CompilerParams(vmem_limit_bytes=24 << 20),
    )(*gathered)
    return input_grad[None], filter_grad


def fits_fused(groups, seqs, signal, filter_taps):
    rows, channels = filter_taps.shape
    return (
        signal.shape[0] == 1
        and seqs % 2 == 0
        and groups % 2 == 0
        and rows % 128 == 0
        and channels % (8 * groups * seqs) == 0
        and groups & (groups - 1) == 0
        and seqs & (seqs - 1) == 0
    )


def angle_table(height, width, period):
    product = lax.broadcasted_iota(jnp.int32, (height, width), 0) * lax.broadcasted_iota(
        jnp.int32, (height, width), 1
    )
    return 2.0 * jnp.pi / period * (product % period).astype(jnp.float32)


def angle_of(product, period):
    return 2.0 * jnp.pi / period * (product % period).astype(jnp.float32)


def coarse_order(slot, seq_count):
    pair_index = slot // 2
    odd_slot = slot % 2
    return jnp.where(
        pair_index == 0,
        odd_slot * seq_count,
        jnp.where(odd_slot == 0, pair_index, 2 * seq_count - pair_index),
    )


def contract(form, table, operand):
    return jnp.einsum(form, table, operand, precision=lax.Precision.HIGHEST)


def forward_spectra(columns):
    seq_count = lax.axis_size("seq")
    row_count = columns.shape[0]
    part_rows = row_count // seq_count
    period_len = 2 * row_count * seq_count
    spread = lax.all_to_all(
        columns.reshape(1, row_count, columns.shape[1]),
        "seq",
        split_axis=1,
        concat_axis=0,
        tiled=True,
    )
    slot_grid = lax.broadcasted_iota(jnp.int32, (2 * seq_count, seq_count), 0)
    source_grid = lax.broadcasted_iota(jnp.int32, (2 * seq_count, seq_count), 1)
    first_table = angle_of(coarse_order(slot_grid, seq_count) * source_grid, 2 * seq_count)
    cos_first = jnp.cos(first_table)
    sin_first = jnp.sin(first_table)
    half_width = spread.shape[2] // 2
    real_in = spread[:, :, :half_width]
    imag_in = spread[:, :, half_width:]
    real_part = contract("ks,srw->krw", cos_first, real_in) + contract(
        "ks,srw->krw", sin_first, imag_in
    )
    imag_part = contract("ks,srw->krw", cos_first, imag_in) - contract(
        "ks,srw->krw", sin_first, real_in
    )
    global_row = lax.axis_index("seq") * part_rows + lax.broadcasted_iota(
        jnp.int32, (2 * seq_count, part_rows), 1
    )
    coarse = coarse_order(lax.broadcasted_iota(jnp.int32, (2 * seq_count, part_rows), 0), seq_count)
    phases = angle_of(global_row * coarse, period_len)
    cos_turn = jnp.cos(phases)[:, :, None]
    sin_turn = jnp.sin(phases)[:, :, None]
    rotated = jnp.stack(
        [real_part * cos_turn + imag_part * sin_turn, imag_part * cos_turn - real_part * sin_turn]
    )
    inner_table = angle_table(row_count, row_count, row_count)
    cos_inner = jnp.cos(inner_table)
    sin_inner = jnp.sin(inner_table)
    pieces = lax.all_to_all(rotated, "seq", split_axis=1, concat_axis=2, tiled=True)
    real_sum = contract("qr,krw->kqw", cos_inner, pieces[0]) + contract(
        "qr,krw->kqw", sin_inner, pieces[1]
    )
    imag_sum = contract("qr,krw->kqw", cos_inner, pieces[1]) - contract(
        "qr,krw->kqw", sin_inner, pieces[0]
    )
    return jnp.stack([real_sum, imag_sum])


def split_pairs(packed):
    reversed_q = packed[:, :, ::-1]
    zero_row = jnp.roll(reversed_q[:, 0], 1, axis=1)
    own_pair = jnp.stack([zero_row, reversed_q[:, 1]], axis=1)
    partner = jnp.where(lax.axis_index("seq") == 0, own_pair, reversed_q[:, ::-1])
    first = jnp.stack([0.5 * (packed[0] + partner[0]), 0.5 * (packed[1] - partner[1])])
    second = jnp.stack([0.5 * (packed[1] + partner[1]), 0.5 * (partner[0] - packed[0])])
    return (first, second)


def inverse_rows(spectra):
    seq_count = lax.axis_size("seq")
    row_count = spectra.shape[2]
    period_len = 2 * row_count * seq_count
    inner_table = angle_table(row_count, row_count, row_count)
    cos_inner = jnp.cos(inner_table)
    sin_inner = jnp.sin(inner_table)
    real_sum = contract("qr,krw->kqw", cos_inner, spectra[0]) - contract(
        "qr,krw->kqw", sin_inner, spectra[1]
    )
    imag_sum = contract("qr,krw->kqw", cos_inner, spectra[1]) + contract(
        "qr,krw->kqw", sin_inner, spectra[0]
    )
    coarse = coarse_order(
        2 * lax.axis_index("seq") + lax.broadcasted_iota(jnp.int32, (2, row_count), 0), seq_count
    )
    position = lax.broadcasted_iota(jnp.int32, (2, row_count), 1)
    phases = angle_of(position * coarse, period_len)
    cos_turn = jnp.cos(phases)[:, :, None]
    sin_turn = jnp.sin(phases)[:, :, None]
    rotated = jnp.stack(
        [real_sum * cos_turn - imag_sum * sin_turn, real_sum * sin_turn + imag_sum * cos_turn]
    )
    target_grid = lax.broadcasted_iota(jnp.int32, (seq_count, 2 * seq_count), 0)
    slot_grid = lax.broadcasted_iota(jnp.int32, (seq_count, 2 * seq_count), 1)
    last_table = angle_of(target_grid * coarse_order(slot_grid, seq_count), 2 * seq_count)
    cos_last = jnp.cos(last_table)
    sin_last = jnp.sin(last_table)
    pieces = lax.all_to_all(rotated, "seq", split_axis=2, concat_axis=1, tiled=True)
    value = contract("sk,krw->srw", cos_last, pieces[0]) - contract(
        "sk,krw->srw", sin_last, pieces[1]
    )
    other = contract("sk,krw->srw", sin_last, pieces[0]) + contract(
        "sk,krw->srw", cos_last, pieces[1]
    )
    gathered = (value / period_len, other / period_len)
    gathered = jnp.concatenate([gathered[0], gathered[1]], axis=2)
    home_rows = lax.all_to_all(gathered, "seq", split_axis=0, concat_axis=1, tiled=True)
    return home_rows.reshape(row_count, home_rows.shape[2])


def invert_all(spectra):
    half_width = spectra.shape[3] // 2
    joined = jnp.stack(
        [
            spectra[0, :, :, :half_width] - spectra[1, :, :, half_width:],
            spectra[1, :, :, :half_width] + spectra[0, :, :, half_width:],
        ]
    )
    return inverse_rows(joined)


def shards(signal, grad_out, filter_taps, skip_gain):
    channels = filter_taps.shape[1]
    signal_rows = signal[0].astype(jnp.float32)
    grad_rows = grad_out[0].astype(jnp.float32)
    tap_half = filter_taps.shape[1] // 2
    columns = jnp.concatenate(
        [signal_rows, filter_taps[:, :tap_half], grad_rows, filter_taps[:, tap_half:]], axis=1
    )
    first, second = split_pairs(forward_spectra(columns))
    signal_spec = first[:, :, :, :channels]
    grad_spec = second[:, :, :, :channels]
    own_spec = jnp.concatenate([first[:, :, :, channels:], second[:, :, :, channels:]], axis=3)
    input_spec = jnp.stack(
        [
            grad_spec[0] * own_spec[0] + grad_spec[1] * own_spec[1],
            grad_spec[1] * own_spec[0] - grad_spec[0] * own_spec[1],
        ]
    )
    filter_terms = jnp.stack(
        [
            grad_spec[0] * signal_spec[0] + grad_spec[1] * signal_spec[1],
            grad_spec[1] * signal_spec[0] - grad_spec[0] * signal_spec[1],
        ]
    )
    summed = lax.psum(filter_terms, "batch")
    rows_back = invert_all(jnp.concatenate([input_spec, summed], axis=3))
    filter_grad = rows_back[:, channels:]
    input_grad = (rows_back[:, :channels] + skip_gain[None, :] * grad_rows).astype(jnp.bfloat16)
    return (input_grad[None], filter_grad)


def solution(mesh):
    groups, seqs = mesh.shape["batch"], mesh.shape["seq"]

    def either(signal, grad_out, filter_taps, skip_gain):
        if fits_fused(groups, seqs, signal, filter_taps):
            return fused_shards(groups, seqs, signal, grad_out, filter_taps, skip_gain)
        return shards(signal, grad_out, filter_taps, skip_gain)

    return jax.shard_map(
        either,
        mesh=mesh,
        in_specs=(P("batch", "seq", None), P("batch", "seq", None), P("seq", None), P()),
        out_specs=(P("batch", "seq", None), P("seq", None)),
        check_vma=False,
    )
```

```python
import functools
import math

import jax
import jax.numpy as jnp
import numpy as np
from jax import lax
from jax.experimental import pallas as pl
from jax.experimental.pallas import tpu as pltpu
from jax.sharding import PartitionSpec as P

MESH = pl.DeviceIdType.MESH
F32 = jnp.float32
BF16 = jnp.bfloat16
GRAD, TAPS, SIGNAL, INPUT, FILTER, FORWARD = range(6)


def weighted(terms):
    total = None
    for factor, array in terms:
        if array is None or abs(factor) < 1e-12:
            continue
        if total is None:
            if abs(factor - 1.0) < 1e-12:
                total = array
            else:
                total = array * factor
        elif abs(factor - 1.0) < 1e-12:
            total = total + array
        elif abs(factor + 1.0) < 1e-12:
            total = total - array
        else:
            total = total + array * factor
    return total


def added(left, right):
    return weighted([(1.0, left), (1.0, right)])


def subtracted(left, right):
    return weighted([(1.0, left), (-1.0, right)])


def turn(real, imag, cos_turn, sin_turn):
    if imag is None:
        return real * cos_turn, -(real * sin_turn)
    return real * cos_turn + imag * sin_turn, imag * cos_turn - real * sin_turn


def coarse_forward(blocks):
    count = len(blocks)
    result = [None] * (count + 1)
    for k in range(count // 2 + 1):
        sums = []
        for parity in (0, 1):
            angles = [(math.pi * ((s * k) % (2 * count)) / count, s) for s in range(parity, count, 2)]
            sums.append(
                (
                    weighted([(math.cos(a), blocks[s]) for a, s in angles]),
                    weighted([(-math.sin(a), blocks[s]) for a, s in angles]),
                )
            )
        (even_re, even_im), (odd_re, odd_im) = sums
        result[k] = (added(even_re, odd_re), added(even_im, odd_im))
        if k != count - k:
            result[count - k] = (subtracted(even_re, odd_re), subtracted(odd_im, even_im))
    return result


def coarse_inverse(terms, scale):
    count = len(terms) - 1
    pairs = []
    for k in range(count // 2 + 1):
        weight = scale if k == 0 else 2.0 * scale
        real, imag = terms[k]
        if k == count - k:
            pairs.append((weight, real, imag, real, imag))
        else:
            other_re, other_im = terms[count - k]
            pairs.append((weight, real + other_re, imag - other_im, real - other_re, imag + other_im))
    blocks = []
    for s in range(count):
        parts = []
        for k, (weight, even_re, even_im, odd_re, odd_im) in enumerate(pairs):
            angle = math.pi * ((s * k) % (2 * count)) / count
            parts.append((weight * math.cos(angle) * (1 if abs(math.cos(angle)) > 1e-9 else 0), odd_re if s % 2 else even_re))
            parts.append((weight * math.sin(angle) * (1 if abs(math.sin(angle)) > 1e-9 else 0), odd_im if s % 2 else even_im))
        blocks.append(weighted(parts))
    return blocks


def fused_kernel(
    groups, seqs,
    signal_hbm, grad_hbm, tap_hbm, skip_hbm, high_hbm, low_hbm, cos_hbm, sin_hbm,
    input_ref, filter_in,
    signal_ref, grad_ref, tap_ref, skip_ref, high_ref, low_ref, cos_ref, sin_ref,
    grad_out_buf, signal_out_buf, tap_out_buf, grad_in, signal_in, tap_in,
    input_out, filter_out, input_in,
    tap_rows, tap_spec, grad_rows, grad_spec, signal_rows, signal_spec, input_rows, filter_rows, filter_spec,
    send_sems, recv_sems, load_sems,
):
    count = groups * seqs
    coarse = seqs + 1
    own, rows = grad_in.shape[1:]
    channels = count * own
    group, seq = lax.axis_index("batch"), lax.axis_index("seq")
    me = group * seqs + seq
    scale = 1.0 / (2 * seqs * rows)
    re, im = pl.ds(0, rows), pl.ds(rows, rows)

    parity, pair = lax.rem(group, 2), lax.div(group, 2)
    half_seqs, half_groups = seqs // 2, groups // 2
    upper, inner = lax.div(seq, half_seqs), lax.rem(seq, half_seqs)

    def load(index, source, target):
        return pltpu.make_async_copy(source, target, load_sems.at[index])

    loads = [
        load(index, source, target)
        for index, (source, target) in enumerate(
            (
                (grad_hbm, grad_ref), (tap_hbm, tap_ref), (signal_hbm, signal_ref),
                (cos_hbm, cos_ref), (sin_hbm, sin_ref), (high_hbm, high_ref),
                (low_hbm, low_ref), (skip_hbm, skip_ref),
            )
        )
    ]
    loads[GRAD].start()
    loads[TAPS].start()

    rank = seq * groups + group
    turns = [(half_seqs + seqs - step) % seqs for step in range(seqs)]

    def turned_seq(offset):
        return lax.rem(seq + offset, seqs) if offset else seq

    def over_peers(body):
        for shift in (half_groups, *range(half_groups - 1, -1, -1), *range(half_groups + 1, groups)):
            to_group = lax.rem(group + shift, groups) if shift else group
            for offset in reversed(range(seqs)):
                if shift or offset:
                    body(to_group, turned_seq(offset), shift == 0)

    def compare(to_group, to_seq):
        return to_seq * groups + to_group - rank

    def signal(semaphore, to_group, to_seq):
        pl.semaphore_signal(
            semaphore, inc=1, device_id={"batch": to_group, "seq": to_seq}, device_id_type=MESH
        )

    barrier = pltpu.get_barrier_semaphore()

    def greet(to_group, to_seq, same):
        signal(barrier, to_group, to_seq)

    over_peers(greet)
    for copy in loads[2:]:
        copy.start()

    def transfer(source, target, kind, to_group, to_seq):
        return pltpu.make_async_remote_copy(
            src_ref=source,
            dst_ref=target,
            send_sem=send_sems.at[kind],
            recv_sem=recv_sems.at[kind],
            device_id={"batch": to_group, "seq": to_seq},
            device_id_type=MESH,
        )

    def all_of(buffer, blocks, kind):
        view = buffer.at[pl.ds(0, blocks)]
        return transfer(view, view, kind, group, turned_seq(1))

    loads[GRAD].wait()
    grad_out_buf[...] = grad_ref[...].astype(F32).T.reshape(count, own, rows)
    loads[TAPS].wait()
    tap_out_buf[...] = tap_ref[...].T.reshape(count, own, rows)

    def send_grad(to_group, to_seq, same):
        place = to_group * seqs + to_seq
        if same:
            transfer(tap_out_buf.at[place], tap_in.at[seq], TAPS, to_group, to_seq).start()
        transfer(grad_out_buf.at[place], grad_in.at[me], GRAD, to_group, to_seq).start()

    def send_signal(to_group, to_seq, same):
        place = to_group * seqs + to_seq
        transfer(signal_out_buf.at[place], signal_in.at[me], SIGNAL, to_group, to_seq).start()

    pl.semaphore_wait(barrier, count - 1)
    over_peers(send_grad)
    loads[SIGNAL].wait()
    signal_out_buf[...] = signal_ref[...].astype(F32).T.reshape(count, own, rows)
    over_peers(send_signal)
    grad_in[me] = grad_out_buf[me]
    tap_in[seq] = tap_out_buf[me]
    signal_in[me] = signal_out_buf[me]

    def spread(blocks, target, first_row):
        place = pl.ds(first_row, own)
        for k, (real, imag) in enumerate(coarse_forward(blocks)):
            real, imag = turn(real, imag, cos_ref[k], sin_ref[k])
            target[k, place, re] = real
            target[k, place, im] = imag

    def fine(source, target):
        lines = source.shape[0] * source.shape[1]
        value = source[...].reshape(lines, 2 * rows)
        high = value.astype(BF16)
        low = (value - high.astype(F32)).astype(BF16)
        product = functools.partial(jnp.dot, preferred_element_type=F32)
        total = product(high, high_ref[...]) + product(low, high_ref[...]) + product(high, low_ref[...])
        target[...] = total.reshape(target.shape)

    def collect(source, first_row):
        place = pl.ds(first_row, own)
        terms = [
            turn(source[k, place, re], source[k, place, im], cos_ref[k], sin_ref[k])
            for k in range(coarse)
        ]
        return coarse_inverse(terms, scale)

    def row_of(index):
        return pl.multiple_of(index * own, own)

    for copy in loads[3:]:
        copy.wait()
    all_of(tap_in, seqs - 1, TAPS).wait_recv()
    spread([tap_in[s] for s in range(seqs)], tap_rows, 0)
    fine(tap_rows, tap_spec)
    all_of(grad_in, count - 1, GRAD).wait_recv()

    def group_at(index):
        return lax.rem(2 * pair + index, groups)

    def input_part(first):
        source, spectrum, lines = grad_rows.at[first], grad_spec.at[first], input_rows.at[first]

        def spread_grad(index, carry):
            here = group_at(2 * first + index)
            spread([grad_in[here * seqs + s] for s in range(seqs)], source, row_of(index))
            return carry

        lax.fori_loop(0, 2, spread_grad, 0)
        fine(source, spectrum)

        def multiply_taps(index, carry):
            place = pl.ds(row_of(index), own)
            for k in range(coarse):
                grad_re, grad_im = spectrum[k, place, re], spectrum[k, place, im]
                tap_re, tap_im = tap_spec[k, :, re], tap_spec[k, :, im]
                lines[k, place, re] = grad_re * tap_re + grad_im * tap_im
                lines[k, place, im] = grad_re * tap_im - grad_im * tap_re
            return carry

        lax.fori_loop(0, 2, multiply_taps, 0)
        fine(lines, lines)

        def collect_input(index, carry):
            here = group_at(2 * first + index)
            for s, block in enumerate(collect(lines, row_of(index))):
                input_out[here * seqs + s] = block
            return carry

        lax.fori_loop(0, 2, collect_input, 0)

        for offset in turns:
            for flip in range(2):
                if first or offset or flip:
                    to_group = group_at(2 * first + lax.rem(parity + flip, 2))
                    to_seq = turned_seq(offset)
                    place = to_group * seqs + to_seq
                    transfer(input_out.at[place], input_in.at[me], INPUT, to_group, to_seq).start()

    for first in reversed(range(half_groups)):
        input_part(first)
    input_in[me] = input_out[me]

    all_of(signal_in, count - 1, SIGNAL).wait_recv()

    def spread_signal(index, carry):
        here = group_at(index)
        spread([signal_in[here * seqs + s] for s in range(seqs)], signal_rows, row_of(index))
        return carry

    lax.fori_loop(0, groups, spread_signal, 0)
    fine(signal_rows, signal_spec)
    for k in range(coarse):
        real, imag = None, None
        for index in range(groups):
            place = pl.ds(index * own, own)
            which, local = index // 2, pl.ds(index % 2 * own, own)
            grad_re, grad_im = grad_spec[which, k, local, re], grad_spec[which, k, local, im]
            signal_re, signal_im = signal_spec[k, place, re], signal_spec[k, place, im]
            real = added(real, grad_re * signal_re + grad_im * signal_im)
            imag = added(imag, grad_re * signal_im - grad_im * signal_re)
        filter_rows[k, :, re] = real
        filter_rows[k, :, im] = imag
    fine(filter_rows, filter_spec)
    for s, block in enumerate(collect(filter_spec, 0)):
        filter_out[s] = block

    for offset in turns:
        for flip in range(half_groups):
            if offset or flip:
                to_group = 2 * lax.rem(pair + flip, half_groups) + parity
                to_seq = turned_seq(offset)
                transfer(
                    filter_out.at[to_seq], filter_in.at[parity, pair * seqs + seq], FILTER, to_group, to_seq
                ).start()
    filter_in[parity, pair * seqs + seq] = filter_out[seq]

    half = count // 2
    all_of(input_in, count - 1, INPUT).wait_recv()
    gradient = input_in[...].reshape(channels, rows).T + skip_ref[...] * grad_ref[...].astype(F32)
    input_ref[...] = gradient.astype(BF16)
    all_of(filter_in.at[0], half - 1, FILTER).wait_recv()
    mine = filter_in.at[parity]
    partner = 2 * pair + 1 - parity
    forward = transfer(mine, mine, FORWARD, partner, seq)
    forward.start()
    forward.wait_recv()
    for kind, buffer in ((GRAD, grad_in), (SIGNAL, signal_in), (INPUT, input_in)):
        all_of(buffer, count - 1, kind).wait_send()
    all_of(filter_in.at[0], half - 1, FILTER).wait_send()
    forward.wait_send()
    all_of(tap_in, seqs - 1, TAPS).wait_send()


def finish_kernel(groups, seqs, input_ref, filter_in, input_hbm, filter_hbm, filter_ref, sems):
    own, rows = filter_in.shape[2:]
    input_store = pltpu.make_async_copy(input_ref, input_hbm, sems.at[0])
    input_store.start()
    parts = [
        filter_in[which, first * seqs : (first + 1) * seqs].reshape(seqs * own, rows)
        for first in range(groups // 2)
        for which in range(2)
    ]
    filter_ref[...] = jnp.concatenate(parts, axis=0).T
    filter_store = pltpu.make_async_copy(filter_ref, filter_hbm, sems.at[1])
    filter_store.start()
    input_store.wait()
    filter_store.wait()


def fine_tables(rows):
    grid = np.arange(rows)
    angle = 2.0 * np.pi / rows * (np.outer(grid, grid) % rows)
    table = np.block([[np.cos(angle), -np.sin(angle)], [np.sin(angle), np.cos(angle)]]).astype(np.float32)
    high = table.astype(BF16)
    return high, (table - high.astype(np.float32)).astype(BF16)


def turn_tables(seqs, rows, lines):
    angle = np.pi / (seqs * rows) * np.outer(np.arange(seqs + 1), np.arange(rows))
    wide = np.broadcast_to(angle[:, None, :], (seqs + 1, lines, rows))
    return np.cos(wide).astype(np.float32), np.sin(wide).astype(np.float32)


def fused_shards(groups, seqs, signal, grad_out, filter_taps, skip_gain):
    rows, channels = filter_taps.shape
    count, coarse = groups * seqs, seqs + 1
    own = channels // count
    high, low = fine_tables(rows)
    cos_turn, sin_turn = turn_tables(seqs, rows, own)
    blocks = pltpu.VMEM((count, own, rows), F32)
    few = pltpu.VMEM((seqs, own, rows), F32)
    lines = lambda number: pltpu.VMEM((coarse, number * own, 2 * rows), F32)
    pairs = pltpu.VMEM((groups // 2, coarse, 2 * own, 2 * rows), F32)
    hbm = pl.BlockSpec(memory_space=pltpu.HBM)
    turns = pltpu.VMEM((coarse, own, rows), F32)
    table = pltpu.VMEM((2 * rows, 2 * rows), BF16)
    vmem = pl.BlockSpec(memory_space=pltpu.VMEM)
    gathered = pl.pallas_call(
        functools.partial(fused_kernel, groups, seqs),
        out_shape=(
            pltpu.VMEM((rows, channels), BF16),
            pltpu.VMEM((2, count // 2, own, rows), F32),
        ),
        in_specs=[hbm] * 8,
        out_specs=(vmem, vmem),
        scratch_shapes=[
            pltpu.VMEM((rows, channels), BF16), pltpu.VMEM((rows, channels), BF16),
            pltpu.VMEM((rows, channels), F32), pltpu.VMEM((1, channels), F32),
            table, table, turns, turns,
            blocks, blocks, blocks, blocks, blocks, few,
            blocks, few, blocks,
            lines(1), lines(1), pairs, pairs, lines(groups), lines(groups),
            pairs, lines(1), lines(1),
            pltpu.SemaphoreType.DMA((6,)),
            pltpu.SemaphoreType.DMA((6,)),
            pltpu.SemaphoreType.DMA((8,)),
        ],
        compiler_params=pltpu.CompilerParams(
            collective_id=0, has_side_effects=True, vmem_limit_bytes=24 << 20
        ),
    )(
        *(
            pltpu.with_memory_space_constraint(array, pltpu.HBM)
            for array in (
                signal[0], grad_out[0], filter_taps, skip_gain[None, :],
                jnp.asarray(high), jnp.asarray(low), jnp.asarray(cos_turn), jnp.asarray(sin_turn),
            )
        )
    )
    input_grad, filter_grad = pl.pallas_call(
        functools.partial(finish_kernel, groups, seqs),
        out_shape=(
            jax.ShapeDtypeStruct((rows, channels), BF16),
            jax.ShapeDtypeStruct((rows, channels), F32),
        ),
        in_specs=[vmem] * 2,
        out_specs=(hbm, hbm),
        scratch_shapes=[
            pltpu.VMEM((rows, channels), F32),
            pltpu.SemaphoreType.DMA((2,)),
        ],
        compiler_params=pltpu.CompilerParams(vmem_limit_bytes=24 << 20),
    )(*gathered)
    return input_grad[None], filter_grad


def fits_fused(groups, seqs, signal, filter_taps):
    rows, channels = filter_taps.shape
    return (
        signal.shape[0] == 1
        and seqs % 2 == 0
        and groups % 2 == 0
        and rows % 128 == 0
        and channels % (8 * groups * seqs) == 0
    )


def angle_table(height, width, period):
    product = lax.broadcasted_iota(jnp.int32, (height, width), 0) * lax.broadcasted_iota(
        jnp.int32, (height, width), 1
    )
    return 2.0 * jnp.pi / period * (product % period).astype(jnp.float32)


def angle_of(product, period):
    return 2.0 * jnp.pi / period * (product % period).astype(jnp.float32)


def coarse_order(slot, seq_count):
    pair_index = slot // 2
    odd_slot = slot % 2
    return jnp.where(
        pair_index == 0,
        odd_slot * seq_count,
        jnp.where(odd_slot == 0, pair_index, 2 * seq_count - pair_index),
    )


def contract(form, table, operand):
    return jnp.einsum(form, table, operand, precision=lax.Precision.HIGHEST)


def forward_spectra(columns):
    seq_count = lax.axis_size("seq")
    row_count = columns.shape[0]
    part_rows = row_count // seq_count
    period_len = 2 * row_count * seq_count
    spread = lax.all_to_all(
        columns.reshape(1, row_count, columns.shape[1]),
        "seq",
        split_axis=1,
        concat_axis=0,
        tiled=True,
    )
    slot_grid = lax.broadcasted_iota(jnp.int32, (2 * seq_count, seq_count), 0)
    source_grid = lax.broadcasted_iota(jnp.int32, (2 * seq_count, seq_count), 1)
    first_table = angle_of(coarse_order(slot_grid, seq_count) * source_grid, 2 * seq_count)
    cos_first = jnp.cos(first_table)
    sin_first = jnp.sin(first_table)
    half_width = spread.shape[2] // 2
    real_in = spread[:, :, :half_width]
    imag_in = spread[:, :, half_width:]
    real_part = contract("ks,srw->krw", cos_first, real_in) + contract(
        "ks,srw->krw", sin_first, imag_in
    )
    imag_part = contract("ks,srw->krw", cos_first, imag_in) - contract(
        "ks,srw->krw", sin_first, real_in
    )
    global_row = lax.axis_index("seq") * part_rows + lax.broadcasted_iota(
        jnp.int32, (2 * seq_count, part_rows), 1
    )
    coarse = coarse_order(lax.broadcasted_iota(jnp.int32, (2 * seq_count, part_rows), 0), seq_count)
    phases = angle_of(global_row * coarse, period_len)
    cos_turn = jnp.cos(phases)[:, :, None]
    sin_turn = jnp.sin(phases)[:, :, None]
    rotated = jnp.stack(
        [real_part * cos_turn + imag_part * sin_turn, imag_part * cos_turn - real_part * sin_turn]
    )
    inner_table = angle_table(row_count, row_count, row_count)
    cos_inner = jnp.cos(inner_table)
    sin_inner = jnp.sin(inner_table)
    pieces = lax.all_to_all(rotated, "seq", split_axis=1, concat_axis=2, tiled=True)
    real_sum = contract("qr,krw->kqw", cos_inner, pieces[0]) + contract(
        "qr,krw->kqw", sin_inner, pieces[1]
    )
    imag_sum = contract("qr,krw->kqw", cos_inner, pieces[1]) - contract(
        "qr,krw->kqw", sin_inner, pieces[0]
    )
    return jnp.stack([real_sum, imag_sum])


def split_pairs(packed):
    reversed_q = packed[:, :, ::-1]
    zero_row = jnp.roll(reversed_q[:, 0], 1, axis=1)
    own_pair = jnp.stack([zero_row, reversed_q[:, 1]], axis=1)
    partner = jnp.where(lax.axis_index("seq") == 0, own_pair, reversed_q[:, ::-1])
    first = jnp.stack([0.5 * (packed[0] + partner[0]), 0.5 * (packed[1] - partner[1])])
    second = jnp.stack([0.5 * (packed[1] + partner[1]), 0.5 * (partner[0] - packed[0])])
    return (first, second)


def inverse_rows(spectra):
    seq_count = lax.axis_size("seq")
    row_count = spectra.shape[2]
    period_len = 2 * row_count * seq_count
    inner_table = angle_table(row_count, row_count, row_count)
    cos_inner = jnp.cos(inner_table)
    sin_inner = jnp.sin(inner_table)
    real_sum = contract("qr,krw->kqw", cos_inner, spectra[0]) - contract(
        "qr,krw->kqw", sin_inner, spectra[1]
    )
    imag_sum = contract("qr,krw->kqw", cos_inner, spectra[1]) + contract(
        "qr,krw->kqw", sin_inner, spectra[0]
    )
    coarse = coarse_order(
        2 * lax.axis_index("seq") + lax.broadcasted_iota(jnp.int32, (2, row_count), 0), seq_count
    )
    position = lax.broadcasted_iota(jnp.int32, (2, row_count), 1)
    phases = angle_of(position * coarse, period_len)
    cos_turn = jnp.cos(phases)[:, :, None]
    sin_turn = jnp.sin(phases)[:, :, None]
    rotated = jnp.stack(
        [real_sum * cos_turn - imag_sum * sin_turn, real_sum * sin_turn + imag_sum * cos_turn]
    )
    target_grid = lax.broadcasted_iota(jnp.int32, (seq_count, 2 * seq_count), 0)
    slot_grid = lax.broadcasted_iota(jnp.int32, (seq_count, 2 * seq_count), 1)
    last_table = angle_of(target_grid * coarse_order(slot_grid, seq_count), 2 * seq_count)
    cos_last = jnp.cos(last_table)
    sin_last = jnp.sin(last_table)
    pieces = lax.all_to_all(rotated, "seq", split_axis=2, concat_axis=1, tiled=True)
    value = contract("sk,krw->srw", cos_last, pieces[0]) - contract(
        "sk,krw->srw", sin_last, pieces[1]
    )
    other = contract("sk,krw->srw", sin_last, pieces[0]) + contract(
        "sk,krw->srw", cos_last, pieces[1]
    )
    gathered = (value / period_len, other / period_len)
    gathered = jnp.concatenate([gathered[0], gathered[1]], axis=2)
    home_rows = lax.all_to_all(gathered, "seq", split_axis=0, concat_axis=1, tiled=True)
    return home_rows.reshape(row_count, home_rows.shape[2])


def invert_all(spectra):
    half_width = spectra.shape[3] // 2
    joined = jnp.stack(
        [
            spectra[0, :, :, :half_width] - spectra[1, :, :, half_width:],
            spectra[1, :, :, :half_width] + spectra[0, :, :, half_width:],
        ]
    )
    return inverse_rows(joined)


def shards(signal, grad_out, filter_taps, skip_gain):
    channels = filter_taps.shape[1]
    signal_rows = signal[0].astype(jnp.float32)
    grad_rows = grad_out[0].astype(jnp.float32)
    tap_half = filter_taps.shape[1] // 2
    columns = jnp.concatenate(
        [signal_rows, filter_taps[:, :tap_half], grad_rows, filter_taps[:, tap_half:]], axis=1
    )
    first, second = split_pairs(forward_spectra(columns))
    signal_spec = first[:, :, :, :channels]
    grad_spec = second[:, :, :, :channels]
    own_spec = jnp.concatenate([first[:, :, :, channels:], second[:, :, :, channels:]], axis=3)
    input_spec = jnp.stack(
        [
            grad_spec[0] * own_spec[0] + grad_spec[1] * own_spec[1],
            grad_spec[1] * own_spec[0] - grad_spec[0] * own_spec[1],
        ]
    )
    filter_terms = jnp.stack(
        [
            grad_spec[0] * signal_spec[0] + grad_spec[1] * signal_spec[1],
            grad_spec[1] * signal_spec[0] - grad_spec[0] * signal_spec[1],
        ]
    )
    summed = lax.psum(filter_terms, "batch")
    rows_back = invert_all(jnp.concatenate([input_spec, summed], axis=3))
    filter_grad = rows_back[:, channels:]
    input_grad = (rows_back[:, :channels] + skip_gain[None, :] * grad_rows).astype(jnp.bfloat16)
    return (input_grad[None], filter_grad)


def solution(mesh):
    groups, seqs = mesh.shape["batch"], mesh.shape["seq"]

    def either(signal, grad_out, filter_taps, skip_gain):
        if fits_fused(groups, seqs, signal, filter_taps):
            return fused_shards(groups, seqs, signal, grad_out, filter_taps, skip_gain)
        return shards(signal, grad_out, filter_taps, skip_gain)

    return jax.shard_map(
        either,
        mesh=mesh,
        in_specs=(P("batch", "seq", None), P("batch", "seq", None), P("seq", None), P()),
        out_specs=(P("batch", "seq", None), P("seq", None)),
        check_vma=False,
    )
```

```python
import functools
import math

import jax
import jax.numpy as jnp
import numpy as np
from jax import lax
from jax.experimental import pallas as pl
from jax.experimental.pallas import tpu as pltpu
from jax.sharding import PartitionSpec as P

MESH = pl.DeviceIdType.MESH
F32 = jnp.float32
BF16 = jnp.bfloat16
GRAD, TAPS, SIGNAL, INPUT, FILTER, FORWARD, CROSS, NEAR_GRAD, NEAR_SIGNAL, NEAR_TAPS, PART, NEAR_INPUT = range(12)


def weighted(terms):
    total = None
    for factor, array in terms:
        if array is None or abs(factor) < 1e-12:
            continue
        if total is None:
            if abs(factor - 1.0) < 1e-12:
                total = array
            else:
                total = array * factor
        elif abs(factor - 1.0) < 1e-12:
            total = total + array
        elif abs(factor + 1.0) < 1e-12:
            total = total - array
        else:
            total = total + array * factor
    return total


def added(left, right):
    return weighted([(1.0, left), (1.0, right)])


def subtracted(left, right):
    return weighted([(1.0, left), (-1.0, right)])


def turn(real, imag, cos_turn, sin_turn):
    if imag is None:
        return real * cos_turn, -(real * sin_turn)
    return real * cos_turn + imag * sin_turn, imag * cos_turn - real * sin_turn


def coarse_forward(blocks):
    count = len(blocks)
    result = [None] * (count + 1)
    for k in range(count // 2 + 1):
        sums = []
        for parity in (0, 1):
            angles = [(math.pi * ((s * k) % (2 * count)) / count, s) for s in range(parity, count, 2)]
            sums.append(
                (
                    weighted([(math.cos(a), blocks[s]) for a, s in angles]),
                    weighted([(-math.sin(a), blocks[s]) for a, s in angles]),
                )
            )
        (even_re, even_im), (odd_re, odd_im) = sums
        result[k] = (added(even_re, odd_re), added(even_im, odd_im))
        if k != count - k:
            result[count - k] = (subtracted(even_re, odd_re), subtracted(odd_im, even_im))
    return result


def coarse_inverse(terms, scale):
    count = len(terms) - 1
    pairs = []
    for k in range(count // 2 + 1):
        weight = scale if k == 0 else 2.0 * scale
        real, imag = terms[k]
        if k == count - k:
            pairs.append((weight, real, imag, real, imag))
        else:
            other_re, other_im = terms[count - k]
            pairs.append((weight, real + other_re, imag - other_im, real - other_re, imag + other_im))
    blocks = []
    for s in range(count):
        parts = []
        for k, (weight, even_re, even_im, odd_re, odd_im) in enumerate(pairs):
            angle = math.pi * ((s * k) % (2 * count)) / count
            parts.append((weight * math.cos(angle) * (1 if abs(math.cos(angle)) > 1e-9 else 0), odd_re if s % 2 else even_re))
            parts.append((weight * math.sin(angle) * (1 if abs(math.sin(angle)) > 1e-9 else 0), odd_im if s % 2 else even_im))
        blocks.append(weighted(parts))
    return blocks


def fused_kernel(
    groups, seqs,
    signal_hbm, grad_hbm, tap_hbm, skip_hbm, high_hbm, low_hbm, cos_hbm, sin_hbm,
    input_ref, filter_in,
    signal_ref, grad_ref, tap_ref, skip_ref, high_ref, low_ref, cos_ref, sin_ref,
    grad_out_buf, signal_out_buf, tap_out_buf, grad_in, signal_in, tap_in,
    input_out, filter_out, input_in,
    tap_rows, tap_spec, grad_rows, grad_spec, signal_rows, signal_spec, input_rows, filter_rows, filter_spec,
    near_grad_in, near_signal_in, near_tap_in, near_input_out, near_input_in, near_filter_out, part_in,
    near_grad, near_signal, near_tap, near_lines, near_filter,
    send_sems, recv_sems, load_sems,
):
    count = groups * seqs
    coarse = seqs + 1
    own, rows = grad_in.shape[1:]
    channels = count * own
    group, seq = lax.axis_index("batch"), lax.axis_index("seq")
    me = group * seqs + seq
    re, im = pl.ds(0, rows), pl.ds(rows, rows)

    parity, pair = lax.rem(group, 2), lax.div(group, 2)
    half_seqs, half_groups = seqs // 2, groups // 2
    upper, inner = lax.div(seq, half_seqs), lax.rem(seq, half_seqs)

    def load(index, source, target):
        return pltpu.make_async_copy(source, target, load_sems.at[index])

    loads = [
        load(index, source, target)
        for index, (source, target) in enumerate(
            (
                (grad_hbm, grad_ref), (tap_hbm, tap_ref), (signal_hbm, signal_ref),
                (cos_hbm, cos_ref), (sin_hbm, sin_ref), (high_hbm, high_ref),
                (low_hbm, low_ref), (skip_hbm, skip_ref),
            )
        )
    ]
    loads[GRAD].start()
    loads[TAPS].start()

    slot, near_count = group * half_seqs + inner, groups * half_seqs
    mate = lax.rem(seq + half_seqs, seqs)
    turns = [(half_seqs + seqs - step) % seqs for step in range(seqs)]

    def turned_seq(offset):
        return lax.rem(seq + offset, seqs) if offset else seq

    shifts = (half_groups, *range(half_groups - 1, -1, -1), *range(half_groups + 1, groups))

    def over_peers(body):
        for shift in shifts:
            to_group = lax.rem(group + shift, groups) if shift else group
            for offset in reversed(range(seqs)):
                if shift or offset:
                    body(to_group, turned_seq(offset), shift == 0)

    def signal(semaphore, to_group, to_seq):
        pl.semaphore_signal(
            semaphore, inc=1, device_id={"batch": to_group, "seq": to_seq}, device_id_type=MESH
        )

    barrier = pltpu.get_barrier_semaphore()

    def greet(to_group, to_seq, same):
        signal(barrier, to_group, to_seq)

    over_peers(greet)
    for copy in loads[2:]:
        copy.start()

    def transfer(source, target, kind, to_group, to_seq):
        return pltpu.make_async_remote_copy(
            src_ref=source,
            dst_ref=target,
            send_sem=send_sems.at[kind],
            recv_sem=recv_sems.at[kind],
            device_id={"batch": to_group, "seq": to_seq},
            device_id_type=MESH,
        )

    def all_of(buffer, blocks, kind):
        view = buffer.at[pl.ds(0, blocks)]
        return transfer(view, view, kind, group, turned_seq(1))

    @pl.when(upper == 0)
    def _():
        for where in range(groups):
            signal_in[where * seqs + half_seqs : (where + 1) * seqs] = jnp.zeros((half_seqs, own, rows), F32)

    @pl.when(upper == 1)
    def _():
        for where in range(groups):
            grad_in[where * seqs : where * seqs + half_seqs] = jnp.zeros((half_seqs, own, rows), F32)

    loads[GRAD].wait()
    grad_out_buf[...] = grad_ref[...].astype(F32).T.reshape(count, own, rows)
    loads[TAPS].wait()
    tap_out_buf[...] = tap_ref[...].T.reshape(count, own, rows)
    loads[SIGNAL].wait()
    signal_out_buf[...] = signal_ref[...].astype(F32).T.reshape(count, own, rows)
    pl.semaphore_wait(barrier, count - 1)

    def near_seq(ring):
        return upper * half_seqs + ring

    def far_seq(ring):
        return (1 - upper) * half_seqs + ring

    def far_block(shift, to_group, ring):
        to_seq = far_seq(ring)
        place = to_group * seqs + to_seq

        @pl.when(upper == 0)
        def _():
            transfer(signal_out_buf.at[place], signal_in.at[me], CROSS, to_group, to_seq).start()

        @pl.when(upper == 1)
        def _():
            transfer(grad_out_buf.at[place], grad_in.at[me], CROSS, to_group, to_seq).start()

    def far_taps(shift, to_group, ring):
        if shift == 0:
            place = group * seqs + far_seq(ring)
            transfer(tap_out_buf.at[place], tap_in.at[seq], TAPS, group, far_seq(ring)).start()

    def near_taps(shift, to_group, ring):
        if shift == 0:
            place = group * seqs + near_seq(ring)
            transfer(tap_out_buf.at[place], tap_in.at[seq], TAPS, group, near_seq(ring)).start()

    def near_grad_block(shift, to_group, ring):
        place = to_group * seqs + near_seq(ring)
        transfer(grad_out_buf.at[place], grad_in.at[me], GRAD, to_group, near_seq(ring)).start()

    def near_signal_block(shift, to_group, ring):
        place = to_group * seqs + near_seq(ring)
        transfer(signal_out_buf.at[place], signal_in.at[me], SIGNAL, to_group, near_seq(ring)).start()

    def mate_blocks(shift, to_group, ring):
        place, to_seq = to_group * seqs + far_seq(ring), near_seq(ring)
        transfer(grad_out_buf.at[place], near_grad_in.at[slot], NEAR_GRAD, to_group, to_seq).start()
        transfer(signal_out_buf.at[place], near_signal_in.at[slot], NEAR_SIGNAL, to_group, to_seq).start()

    def mate_taps(shift, to_group, ring):
        place, to_seq = group * seqs + far_seq(ring), near_seq(ring)
        if shift == 0:

            @pl.when(upper == 0)
            def _():
                transfer(tap_out_buf.at[place], near_tap_in.at[inner], NEAR_TAPS, group, to_seq).start()

    def in_turn(*sends):
        for shift in shifts:
            to_group = lax.rem(group + shift, groups) if shift else group
            for offset in reversed(range(half_seqs)):
                ring = lax.rem(inner + offset, half_seqs) if offset else inner
                for send in sends:
                    if shift or offset or send in (far_block, far_taps):
                        send(shift, to_group, ring)

    in_turn(far_taps, near_taps, mate_taps)
    in_turn(mate_blocks)
    in_turn(far_block, near_grad_block)
    in_turn(near_signal_block)
    grad_in[me] = grad_out_buf[me]
    tap_in[seq] = tap_out_buf[me]
    signal_in[me] = signal_out_buf[me]
    near_grad_in[slot] = grad_out_buf[group * seqs + mate]
    near_signal_in[slot] = signal_out_buf[group * seqs + mate]
    near_tap_in[inner] = tap_out_buf[group * seqs + mate]

    def spread(blocks, target, first_row):
        place = pl.ds(first_row, own)
        for k, (real, imag) in enumerate(coarse_forward(blocks)):
            row = k * (seqs // len(blocks))
            real, imag = turn(real, imag, cos_ref[row], sin_ref[row])
            target[k, place, re] = real
            target[k, place, im] = imag

    def fine(source, target):
        lines = source.shape[0] * source.shape[1]
        value = source[...].reshape(lines, 2 * rows)
        high = value.astype(BF16)
        low = (value - high.astype(F32)).astype(BF16)
        product = functools.partial(jnp.dot, preferred_element_type=F32)
        total = product(high, high_ref[...]) + product(low, high_ref[...]) + product(high, low_ref[...])
        target[...] = total.reshape(target.shape)

    def collect(source, first_row, pieces):
        place, stride = pl.ds(first_row, own), seqs // pieces
        terms = [
            turn(source[k, place, re], source[k, place, im], cos_ref[k * stride], sin_ref[k * stride])
            for k in range(pieces + 1)
        ]
        return coarse_inverse(terms, 1.0 / (2 * pieces * rows))

    def row_of(index):
        return pl.multiple_of(index * own, own)

    for copy in loads[3:]:
        copy.wait()
    all_of(near_grad_in, near_count - 1, NEAR_GRAD).wait_recv()
    all_of(near_signal_in, near_count - 1, NEAR_SIGNAL).wait_recv()

    def spread_near(index, carry):
        for source, target in ((near_grad_in, near_grad), (near_signal_in, near_signal)):
            spread([source[index * half_seqs + s] for s in range(half_seqs)], target, row_of(index))
        return carry

    lax.fori_loop(0, groups, spread_near, 0)
    fine(near_grad, near_grad)
    fine(near_signal, near_signal)
    for k in range(half_seqs + 1):
        real, imag = None, None
        for index in range(groups):
            place = pl.ds(index * own, own)
            grad_re, grad_im = near_grad[k, place, re], near_grad[k, place, im]
            signal_re, signal_im = near_signal[k, place, re], near_signal[k, place, im]
            real = added(real, grad_re * signal_re + grad_im * signal_im)
            imag = added(imag, grad_re * signal_im - grad_im * signal_re)
        near_filter[k, :, re] = real
        near_filter[k, :, im] = imag
    fine(near_filter, near_filter)
    for s, block in enumerate(collect(near_filter, 0, half_seqs)):
        near_filter_out[s] = block
    transfer(near_filter_out, part_in, PART, group, mate).start()

    @pl.when(upper == 0)
    def _():
        all_of(near_tap_in, half_seqs - 1, NEAR_TAPS).wait_recv()
        spread([near_tap_in[s] for s in range(half_seqs)], near_tap, 0)
        fine(near_tap, near_tap)

        def multiply_near(index, carry):
            place = pl.ds(row_of(index), own)
            for k in range(half_seqs + 1):
                grad_re, grad_im = near_grad[k, place, re], near_grad[k, place, im]
                tap_re, tap_im = near_tap[k, :, re], near_tap[k, :, im]
                near_lines[k, place, re] = grad_re * tap_re + grad_im * tap_im
                near_lines[k, place, im] = grad_re * tap_im - grad_im * tap_re
            return carry

        lax.fori_loop(0, groups, multiply_near, 0)
        fine(near_lines, near_lines)

        def collect_near(index, carry):
            for s, block in enumerate(collect(near_lines, row_of(index), half_seqs)):
                near_input_out[index * half_seqs + s] = block
            return carry

        lax.fori_loop(0, groups, collect_near, 0)
        for shift in shifts:
            to_group = lax.rem(group + shift, groups) if shift else group
            for offset in reversed(range(half_seqs)):
                if shift or offset:
                    ring = lax.rem(inner + offset, half_seqs)
                    transfer(
                        near_input_out.at[to_group * half_seqs + ring], near_input_in.at[slot],
                        NEAR_INPUT, to_group, ring,
                    ).start()
        near_input_in[slot] = near_input_out[slot]

    all_of(tap_in, seqs - 1, TAPS).wait_recv()
    spread([tap_in[s] for s in range(seqs)], tap_rows, 0)
    fine(tap_rows, tap_spec)
    all_of(grad_in, near_count - 1, GRAD).wait_recv()
    pl.when(upper == 0)(lambda: all_of(grad_in, near_count, CROSS).wait_recv())

    def group_at(index):
        return lax.rem(2 * pair + index, groups)

    def input_part(first):
        source, spectrum, lines = grad_rows.at[first], grad_spec.at[first], input_rows.at[first]

        def spread_grad(index, carry):
            here = group_at(2 * first + index)
            spread([grad_in[here * seqs + s] for s in range(seqs)], source, row_of(index))
            return carry

        lax.fori_loop(0, 2, spread_grad, 0)
        fine(source, spectrum)

        def multiply_taps(index, carry):
            place = pl.ds(row_of(index), own)
            for k in range(coarse):
                grad_re, grad_im = spectrum[k, place, re], spectrum[k, place, im]
                tap_re, tap_im = tap_spec[k, :, re], tap_spec[k, :, im]
                lines[k, place, re] = grad_re * tap_re + grad_im * tap_im
                lines[k, place, im] = grad_re * tap_im - grad_im * tap_re
            return carry

        lax.fori_loop(0, 2, multiply_taps, 0)
        fine(lines, lines)

        def collect_input(index, carry):
            here = group_at(2 * first + index)
            for s, block in enumerate(collect(lines, row_of(index), seqs)):
                input_out[here * seqs + s] = block
            return carry

        lax.fori_loop(0, 2, collect_input, 0)

        for offset in turns:
            for flip in range(2):
                if first or offset or flip:
                    to_group = group_at(2 * first + lax.rem(parity + flip, 2))
                    to_seq = turned_seq(offset)
                    place = to_group * seqs + to_seq
                    transfer(input_out.at[place], input_in.at[me], INPUT, to_group, to_seq).start()

    for first in reversed(range(half_groups)):
        input_part(first)
    input_in[me] = input_out[me]

    all_of(signal_in, near_count - 1, SIGNAL).wait_recv()
    pl.when(upper == 1)(lambda: all_of(signal_in, near_count, CROSS).wait_recv())

    def spread_signal(index, carry):
        here = group_at(index)
        spread([signal_in[here * seqs + s] for s in range(seqs)], signal_rows, row_of(index))
        return carry

    lax.fori_loop(0, groups, spread_signal, 0)
    fine(signal_rows, signal_spec)
    for k in range(coarse):
        real, imag = None, None
        for index in range(groups):
            place = pl.ds(index * own, own)
            which, local = index // 2, pl.ds(index % 2 * own, own)
            grad_re, grad_im = grad_spec[which, k, local, re], grad_spec[which, k, local, im]
            signal_re, signal_im = signal_spec[k, place, re], signal_spec[k, place, im]
            real = added(real, grad_re * signal_re + grad_im * signal_im)
            imag = added(imag, grad_re * signal_im - grad_im * signal_re)
        filter_rows[k, :, re] = real
        filter_rows[k, :, im] = imag
    fine(filter_rows, filter_spec)
    all_of(part_in, half_seqs, PART).wait_recv()
    for s, block in enumerate(collect(filter_spec, 0, seqs)):
        filter_out[s] = block + part_in[s] if s < half_seqs else block

    for offset in turns:
        for flip in range(half_groups):
            if offset or flip:
                to_group = 2 * lax.rem(pair + flip, half_groups) + parity
                to_seq = turned_seq(offset)
                transfer(
                    filter_out.at[to_seq], filter_in.at[parity, pair * seqs + seq], FILTER, to_group, to_seq
                ).start()
    filter_in[parity, pair * seqs + seq] = filter_out[seq]

    half = count // 2
    all_of(input_in, count - 1, INPUT).wait_recv()

    @pl.when(upper == 0)
    def _():
        all_of(near_input_in, near_count - 1, NEAR_INPUT).wait_recv()
        for where in range(groups):
            far = slice(where * seqs + half_seqs, (where + 1) * seqs)
            input_in[far] = input_in[far] + near_input_in[where * half_seqs : (where + 1) * half_seqs]

    gradient = input_in[...].reshape(channels, rows).T + skip_ref[...] * grad_ref[...].astype(F32)
    input_ref[...] = gradient.astype(BF16)
    all_of(filter_in.at[0], half - 1, FILTER).wait_recv()
    mine = filter_in.at[parity]
    partner = 2 * pair + 1 - parity
    forward = transfer(mine, mine, FORWARD, partner, seq)
    forward.start()
    forward.wait_recv()
    for kind in (GRAD, SIGNAL, NEAR_GRAD, NEAR_SIGNAL):
        all_of(grad_in, near_count - 1, kind).wait_send()
    all_of(grad_in, near_count, CROSS).wait_send()
    all_of(part_in, half_seqs, PART).wait_send()

    @pl.when(upper == 0)
    def _():
        all_of(grad_in, near_count - 1, NEAR_INPUT).wait_send()
        all_of(tap_in, half_seqs - 1, NEAR_TAPS).wait_send()

    all_of(input_in, count - 1, INPUT).wait_send()
    all_of(filter_in.at[0], half - 1, FILTER).wait_send()
    forward.wait_send()
    all_of(tap_in, seqs - 1, TAPS).wait_send()


def finish_kernel(groups, seqs, input_ref, filter_in, input_hbm, filter_hbm, filter_ref, sems):
    own, rows = filter_in.shape[2:]
    input_store = pltpu.make_async_copy(input_ref, input_hbm, sems.at[0])
    input_store.start()
    parts = [
        filter_in[which, first * seqs : (first + 1) * seqs].reshape(seqs * own, rows)
        for first in range(groups // 2)
        for which in range(2)
    ]
    filter_ref[...] = jnp.concatenate(parts, axis=0).T
    filter_store = pltpu.make_async_copy(filter_ref, filter_hbm, sems.at[1])
    filter_store.start()
    input_store.wait()
    filter_store.wait()


def fine_tables(rows):
    grid = np.arange(rows)
    angle = 2.0 * np.pi / rows * (np.outer(grid, grid) % rows)
    table = np.block([[np.cos(angle), -np.sin(angle)], [np.sin(angle), np.cos(angle)]]).astype(np.float32)
    high = table.astype(BF16)
    return high, (table - high.astype(np.float32)).astype(BF16)


def turn_tables(seqs, rows, lines):
    angle = np.pi / (seqs * rows) * np.outer(np.arange(seqs + 1), np.arange(rows))
    wide = np.broadcast_to(angle[:, None, :], (seqs + 1, lines, rows))
    return np.cos(wide).astype(np.float32), np.sin(wide).astype(np.float32)


def fused_shards(groups, seqs, signal, grad_out, filter_taps, skip_gain):
    rows, channels = filter_taps.shape
    count, coarse = groups * seqs, seqs + 1
    own = channels // count
    high, low = fine_tables(rows)
    cos_turn, sin_turn = turn_tables(seqs, rows, own)
    blocks = pltpu.VMEM((count, own, rows), F32)
    few = pltpu.VMEM((seqs, own, rows), F32)
    half_blocks = pltpu.VMEM((count // 2, own, rows), F32)
    half_few = pltpu.VMEM((seqs // 2, own, rows), F32)
    near = lambda number: pltpu.VMEM((seqs // 2 + 1, number * own, 2 * rows), F32)
    lines = lambda number: pltpu.VMEM((coarse, number * own, 2 * rows), F32)
    pairs = pltpu.VMEM((groups // 2, coarse, 2 * own, 2 * rows), F32)
    hbm = pl.BlockSpec(memory_space=pltpu.HBM)
    turns = pltpu.VMEM((coarse, own, rows), F32)
    table = pltpu.VMEM((2 * rows, 2 * rows), BF16)
    vmem = pl.BlockSpec(memory_space=pltpu.VMEM)
    gathered = pl.pallas_call(
        functools.partial(fused_kernel, groups, seqs),
        out_shape=(
            pltpu.VMEM((rows, channels), BF16),
            pltpu.VMEM((2, count // 2, own, rows), F32),
        ),
        in_specs=[hbm] * 8,
        out_specs=(vmem, vmem),
        scratch_shapes=[
            pltpu.VMEM((rows, channels), BF16), pltpu.VMEM((rows, channels), BF16),
            pltpu.VMEM((rows, channels), F32), pltpu.VMEM((1, channels), F32),
            table, table, turns, turns,
            blocks, blocks, blocks, blocks, blocks, few,
            blocks, few, blocks,
            lines(1), lines(1), pairs, pairs, lines(groups), lines(groups),
            pairs, lines(1), lines(1),
            half_blocks, half_blocks, half_few, half_blocks, half_blocks, half_few, half_few,
            near(groups), near(groups), near(1), near(groups), near(1),
            pltpu.SemaphoreType.DMA((12,)),
            pltpu.SemaphoreType.DMA((12,)),
            pltpu.SemaphoreType.DMA((8,)),
        ],
        compiler_params=pltpu.CompilerParams(
            collective_id=0, has_side_effects=True, vmem_limit_bytes=24 << 20
        ),
    )(
        *(
            pltpu.with_memory_space_constraint(array, pltpu.HBM)
            for array in (
                signal[0], grad_out[0], filter_taps, skip_gain[None, :],
                jnp.asarray(high), jnp.asarray(low), jnp.asarray(cos_turn), jnp.asarray(sin_turn),
            )
        )
    )
    input_grad, filter_grad = pl.pallas_call(
        functools.partial(finish_kernel, groups, seqs),
        out_shape=(
            jax.ShapeDtypeStruct((rows, channels), BF16),
            jax.ShapeDtypeStruct((rows, channels), F32),
        ),
        in_specs=[vmem] * 2,
        out_specs=(hbm, hbm),
        scratch_shapes=[
            pltpu.VMEM((rows, channels), F32),
            pltpu.SemaphoreType.DMA((2,)),
        ],
        compiler_params=pltpu.CompilerParams(vmem_limit_bytes=24 << 20),
    )(*gathered)
    return input_grad[None], filter_grad


def fits_fused(groups, seqs, signal, filter_taps):
    rows, channels = filter_taps.shape
    return (
        signal.shape[0] == 1
        and seqs % 4 == 0
        and groups % 2 == 0
        and rows % 128 == 0
        and channels % (8 * groups * seqs) == 0
    )


def angle_table(height, width, period):
    product = lax.broadcasted_iota(jnp.int32, (height, width), 0) * lax.broadcasted_iota(
        jnp.int32, (height, width), 1
    )
    return 2.0 * jnp.pi / period * (product % period).astype(jnp.float32)


def angle_of(product, period):
    return 2.0 * jnp.pi / period * (product % period).astype(jnp.float32)


def coarse_order(slot, seq_count):
    pair_index = slot // 2
    odd_slot = slot % 2
    return jnp.where(
        pair_index == 0,
        odd_slot * seq_count,
        jnp.where(odd_slot == 0, pair_index, 2 * seq_count - pair_index),
    )


def contract(form, table, operand):
    return jnp.einsum(form, table, operand, precision=lax.Precision.HIGHEST)


def forward_spectra(columns):
    seq_count = lax.axis_size("seq")
    row_count = columns.shape[0]
    part_rows = row_count // seq_count
    period_len = 2 * row_count * seq_count
    spread = lax.all_to_all(
        columns.reshape(1, row_count, columns.shape[1]),
        "seq",
        split_axis=1,
        concat_axis=0,
        tiled=True,
    )
    slot_grid = lax.broadcasted_iota(jnp.int32, (2 * seq_count, seq_count), 0)
    source_grid = lax.broadcasted_iota(jnp.int32, (2 * seq_count, seq_count), 1)
    first_table = angle_of(coarse_order(slot_grid, seq_count) * source_grid, 2 * seq_count)
    cos_first = jnp.cos(first_table)
    sin_first = jnp.sin(first_table)
    half_width = spread.shape[2] // 2
    real_in = spread[:, :, :half_width]
    imag_in = spread[:, :, half_width:]
    real_part = contract("ks,srw->krw", cos_first, real_in) + contract(
        "ks,srw->krw", sin_first, imag_in
    )
    imag_part = contract("ks,srw->krw", cos_first, imag_in) - contract(
        "ks,srw->krw", sin_first, real_in
    )
    global_row = lax.axis_index("seq") * part_rows + lax.broadcasted_iota(
        jnp.int32, (2 * seq_count, part_rows), 1
    )
    coarse = coarse_order(lax.broadcasted_iota(jnp.int32, (2 * seq_count, part_rows), 0), seq_count)
    phases = angle_of(global_row * coarse, period_len)
    cos_turn = jnp.cos(phases)[:, :, None]
    sin_turn = jnp.sin(phases)[:, :, None]
    rotated = jnp.stack(
        [real_part * cos_turn + imag_part * sin_turn, imag_part * cos_turn - real_part * sin_turn]
    )
    inner_table = angle_table(row_count, row_count, row_count)
    cos_inner = jnp.cos(inner_table)
    sin_inner = jnp.sin(inner_table)
    pieces = lax.all_to_all(rotated, "seq", split_axis=1, concat_axis=2, tiled=True)
    real_sum = contract("qr,krw->kqw", cos_inner, pieces[0]) + contract(
        "qr,krw->kqw", sin_inner, pieces[1]
    )
    imag_sum = contract("qr,krw->kqw", cos_inner, pieces[1]) - contract(
        "qr,krw->kqw", sin_inner, pieces[0]
    )
    return jnp.stack([real_sum, imag_sum])


def split_pairs(packed):
    reversed_q = packed[:, :, ::-1]
    zero_row = jnp.roll(reversed_q[:, 0], 1, axis=1)
    own_pair = jnp.stack([zero_row, reversed_q[:, 1]], axis=1)
    partner = jnp.where(lax.axis_index("seq") == 0, own_pair, reversed_q[:, ::-1])
    first = jnp.stack([0.5 * (packed[0] + partner[0]), 0.5 * (packed[1] - partner[1])])
    second = jnp.stack([0.5 * (packed[1] + partner[1]), 0.5 * (partner[0] - packed[0])])
    return (first, second)


def inverse_rows(spectra):
    seq_count = lax.axis_size("seq")
    row_count = spectra.shape[2]
    period_len = 2 * row_count * seq_count
    inner_table = angle_table(row_count, row_count, row_count)
    cos_inner = jnp.cos(inner_table)
    sin_inner = jnp.sin(inner_table)
    real_sum = contract("qr,krw->kqw", cos_inner, spectra[0]) - contract(
        "qr,krw->kqw", sin_inner, spectra[1]
    )
    imag_sum = contract("qr,krw->kqw", cos_inner, spectra[1]) + contract(
        "qr,krw->kqw", sin_inner, spectra[0]
    )
    coarse = coarse_order(
        2 * lax.axis_index("seq") + lax.broadcasted_iota(jnp.int32, (2, row_count), 0), seq_count
    )
    position = lax.broadcasted_iota(jnp.int32, (2, row_count), 1)
    phases = angle_of(position * coarse, period_len)
    cos_turn = jnp.cos(phases)[:, :, None]
    sin_turn = jnp.sin(phases)[:, :, None]
    rotated = jnp.stack(
        [real_sum * cos_turn - imag_sum * sin_turn, real_sum * sin_turn + imag_sum * cos_turn]
    )
    target_grid = lax.broadcasted_iota(jnp.int32, (seq_count, 2 * seq_count), 0)
    slot_grid = lax.broadcasted_iota(jnp.int32, (seq_count, 2 * seq_count), 1)
    last_table = angle_of(target_grid * coarse_order(slot_grid, seq_count), 2 * seq_count)
    cos_last = jnp.cos(last_table)
    sin_last = jnp.sin(last_table)
    pieces = lax.all_to_all(rotated, "seq", split_axis=2, concat_axis=1, tiled=True)
    value = contract("sk,krw->srw", cos_last, pieces[0]) - contract(
        "sk,krw->srw", sin_last, pieces[1]
    )
    other = contract("sk,krw->srw", sin_last, pieces[0]) + contract(
        "sk,krw->srw", cos_last, pieces[1]
    )
    gathered = (value / period_len, other / period_len)
    gathered = jnp.concatenate([gathered[0], gathered[1]], axis=2)
    home_rows = lax.all_to_all(gathered, "seq", split_axis=0, concat_axis=1, tiled=True)
    return home_rows.reshape(row_count, home_rows.shape[2])


def invert_all(spectra):
    half_width = spectra.shape[3] // 2
    joined = jnp.stack(
        [
            spectra[0, :, :, :half_width] - spectra[1, :, :, half_width:],
            spectra[1, :, :, :half_width] + spectra[0, :, :, half_width:],
        ]
    )
    return inverse_rows(joined)


def shards(signal, grad_out, filter_taps, skip_gain):
    channels = filter_taps.shape[1]
    signal_rows = signal[0].astype(jnp.float32)
    grad_rows = grad_out[0].astype(jnp.float32)
    tap_half = filter_taps.shape[1] // 2
    columns = jnp.concatenate(
        [signal_rows, filter_taps[:, :tap_half], grad_rows, filter_taps[:, tap_half:]], axis=1
    )
    first, second = split_pairs(forward_spectra(columns))
    signal_spec = first[:, :, :, :channels]
    grad_spec = second[:, :, :, :channels]
    own_spec = jnp.concatenate([first[:, :, :, channels:], second[:, :, :, channels:]], axis=3)
    input_spec = jnp.stack(
        [
            grad_spec[0] * own_spec[0] + grad_spec[1] * own_spec[1],
            grad_spec[1] * own_spec[0] - grad_spec[0] * own_spec[1],
        ]
    )
    filter_terms = jnp.stack(
        [
            grad_spec[0] * signal_spec[0] + grad_spec[1] * signal_spec[1],
            grad_spec[1] * signal_spec[0] - grad_spec[0] * signal_spec[1],
        ]
    )
    summed = lax.psum(filter_terms, "batch")
    rows_back = invert_all(jnp.concatenate([input_spec, summed], axis=3))
    filter_grad = rows_back[:, channels:]
    input_grad = (rows_back[:, :channels] + skip_gain[None, :] * grad_rows).astype(jnp.bfloat16)
    return (input_grad[None], filter_grad)


def solution(mesh):
    groups, seqs = mesh.shape["batch"], mesh.shape["seq"]

    def either(signal, grad_out, filter_taps, skip_gain):
        if fits_fused(groups, seqs, signal, filter_taps):
            return fused_shards(groups, seqs, signal, grad_out, filter_taps, skip_gain)
        return shards(signal, grad_out, filter_taps, skip_gain)

    return jax.shard_map(
        either,
        mesh=mesh,
        in_specs=(P("batch", "seq", None), P("batch", "seq", None), P("seq", None), P()),
        out_specs=(P("batch", "seq", None), P("seq", None)),
        check_vma=False,
    )
```

```python
import functools
import math

import jax
import jax.numpy as jnp
import numpy as np
from jax import lax
from jax.experimental import pallas as pl
from jax.experimental.pallas import tpu as pltpu
from jax.sharding import PartitionSpec as P

MESH = pl.DeviceIdType.MESH
F32 = jnp.float32
BF16 = jnp.bfloat16
GRAD, TAPS, SIGNAL, INPUT, FILTER, FORWARD, CROSS, NEAR_GRAD, NEAR_SIGNAL, NEAR_TAPS, PART, NEAR_INPUT = range(12)


def weighted(terms):
    total = None
    for factor, array in terms:
        if array is None or abs(factor) < 1e-12:
            continue
        if total is None:
            if abs(factor - 1.0) < 1e-12:
                total = array
            else:
                total = array * factor
        elif abs(factor - 1.0) < 1e-12:
            total = total + array
        elif abs(factor + 1.0) < 1e-12:
            total = total - array
        else:
            total = total + array * factor
    return total


def added(left, right):
    return weighted([(1.0, left), (1.0, right)])


def subtracted(left, right):
    return weighted([(1.0, left), (-1.0, right)])


def turn(real, imag, cos_turn, sin_turn):
    if imag is None:
        return real * cos_turn, -(real * sin_turn)
    return real * cos_turn + imag * sin_turn, imag * cos_turn - real * sin_turn


def coarse_forward(blocks):
    count = len(blocks)
    result = [None] * (count + 1)
    for k in range(count // 2 + 1):
        sums = []
        for parity in (0, 1):
            angles = [(math.pi * ((s * k) % (2 * count)) / count, s) for s in range(parity, count, 2)]
            sums.append(
                (
                    weighted([(math.cos(a), blocks[s]) for a, s in angles]),
                    weighted([(-math.sin(a), blocks[s]) for a, s in angles]),
                )
            )
        (even_re, even_im), (odd_re, odd_im) = sums
        result[k] = (added(even_re, odd_re), added(even_im, odd_im))
        if k != count - k:
            result[count - k] = (subtracted(even_re, odd_re), subtracted(odd_im, even_im))
    return result


def coarse_inverse(terms, scale):
    count = len(terms) - 1
    pairs = []
    for k in range(count // 2 + 1):
        weight = scale if k == 0 else 2.0 * scale
        real, imag = terms[k]
        if k == count - k:
            pairs.append((weight, real, imag, real, imag))
        else:
            other_re, other_im = terms[count - k]
            pairs.append((weight, real + other_re, imag - other_im, real - other_re, imag + other_im))
    blocks = []
    for s in range(count):
        parts = []
        for k, (weight, even_re, even_im, odd_re, odd_im) in enumerate(pairs):
            angle = math.pi * ((s * k) % (2 * count)) / count
            parts.append((weight * math.cos(angle) * (1 if abs(math.cos(angle)) > 1e-9 else 0), odd_re if s % 2 else even_re))
            parts.append((weight * math.sin(angle) * (1 if abs(math.sin(angle)) > 1e-9 else 0), odd_im if s % 2 else even_im))
        blocks.append(weighted(parts))
    return blocks


def fused_kernel(
    groups, seqs,
    signal_hbm, grad_hbm, tap_hbm, skip_hbm, high_hbm, low_hbm, cos_hbm, sin_hbm,
    input_ref, filter_in,
    signal_ref, grad_ref, tap_ref, skip_ref, high_ref, low_ref, cos_ref, sin_ref,
    grad_out_buf, signal_out_buf, tap_out_buf, grad_in, signal_in, tap_in,
    input_out, filter_out, input_in,
    tap_rows, tap_spec, grad_rows, grad_spec, signal_rows, signal_spec, input_rows, filter_rows, filter_spec,
    near_grad_in, near_signal_in, near_tap_in, near_input_out, near_input_in, near_filter_out, part_in,
    near_grad, near_signal, near_tap, near_lines, near_filter,
    send_sems, recv_sems, load_sems,
):
    count = groups * seqs
    coarse = seqs + 1
    own, rows = grad_in.shape[1:]
    channels = count * own
    group, seq = lax.axis_index("batch"), lax.axis_index("seq")
    me = group * seqs + seq
    re, im = pl.ds(0, rows), pl.ds(rows, rows)

    parity, pair = lax.rem(group, 2), lax.div(group, 2)
    half_seqs, half_groups = seqs // 2, groups // 2
    upper, inner = lax.div(seq, half_seqs), lax.rem(seq, half_seqs)

    def load(index, source, target):
        return pltpu.make_async_copy(source, target, load_sems.at[index])

    loads = [
        load(index, source, target)
        for index, (source, target) in enumerate(
            (
                (grad_hbm, grad_ref), (tap_hbm, tap_ref), (signal_hbm, signal_ref),
                (cos_hbm, cos_ref), (sin_hbm, sin_ref), (high_hbm, high_ref),
                (low_hbm, low_ref), (skip_hbm, skip_ref),
            )
        )
    ]
    loads[GRAD].start()
    loads[TAPS].start()

    slot, near_count = group * half_seqs + inner, groups * half_seqs
    mate = lax.rem(seq + half_seqs, seqs)
    turns = [(half_seqs + seqs - step) % seqs for step in range(seqs)]

    def turned_seq(offset):
        return lax.rem(seq + offset, seqs) if offset else seq

    shifts = (half_groups, *range(half_groups - 1, -1, -1), *range(half_groups + 1, groups))

    def over_peers(body):
        for shift in shifts:
            to_group = lax.rem(group + shift, groups) if shift else group
            for offset in reversed(range(seqs)):
                if shift or offset:
                    body(to_group, turned_seq(offset), shift == 0)

    def signal(semaphore, to_group, to_seq):
        pl.semaphore_signal(
            semaphore, inc=1, device_id={"batch": to_group, "seq": to_seq}, device_id_type=MESH
        )

    barrier = pltpu.get_barrier_semaphore()

    def greet(to_group, to_seq, same):
        signal(barrier, to_group, to_seq)

    over_peers(greet)
    for copy in loads[2:]:
        copy.start()

    def transfer(source, target, kind, to_group, to_seq):
        return pltpu.make_async_remote_copy(
            src_ref=source,
            dst_ref=target,
            send_sem=send_sems.at[kind],
            recv_sem=recv_sems.at[kind],
            device_id={"batch": to_group, "seq": to_seq},
            device_id_type=MESH,
        )

    def all_of(buffer, blocks, kind):
        view = buffer.at[pl.ds(0, blocks)]
        return transfer(view, view, kind, group, turned_seq(1))

    @pl.when(upper == 0)
    def _():
        for where in range(groups):
            signal_in[where * seqs + half_seqs : (where + 1) * seqs] = jnp.zeros((half_seqs, own, rows), F32)

    @pl.when(upper == 1)
    def _():
        for where in range(groups):
            grad_in[where * seqs : where * seqs + half_seqs] = jnp.zeros((half_seqs, own, rows), F32)

    loads[GRAD].wait()
    grad_out_buf[...] = grad_ref[...].astype(F32).T.reshape(count, own, rows)
    loads[TAPS].wait()
    tap_out_buf[...] = tap_ref[...].T.reshape(count, own, rows)
    loads[SIGNAL].wait()
    signal_out_buf[...] = signal_ref[...].astype(F32).T.reshape(count, own, rows)
    pl.semaphore_wait(barrier, count - 1)

    def near_seq(ring):
        return upper * half_seqs + ring

    def far_seq(ring):
        return (1 - upper) * half_seqs + ring

    def far_block(shift, to_group, ring):
        to_seq = far_seq(ring)
        place = to_group * seqs + to_seq

        @pl.when(upper == 0)
        def _():
            transfer(signal_out_buf.at[place], signal_in.at[me], CROSS, to_group, to_seq).start()

        @pl.when(upper == 1)
        def _():
            transfer(grad_out_buf.at[place], grad_in.at[me], CROSS, to_group, to_seq).start()

    def far_taps(shift, to_group, ring):
        if shift == 0:
            place = group * seqs + far_seq(ring)
            transfer(tap_out_buf.at[place], tap_in.at[seq], TAPS, group, far_seq(ring)).start()

    def near_taps(shift, to_group, ring):
        if shift == 0:
            place = group * seqs + near_seq(ring)
            transfer(tap_out_buf.at[place], tap_in.at[seq], TAPS, group, near_seq(ring)).start()

    def near_grad_block(shift, to_group, ring):
        place = to_group * seqs + near_seq(ring)
        transfer(grad_out_buf.at[place], grad_in.at[me], GRAD, to_group, near_seq(ring)).start()

    def near_signal_block(shift, to_group, ring):
        place = to_group * seqs + near_seq(ring)
        transfer(signal_out_buf.at[place], signal_in.at[me], SIGNAL, to_group, near_seq(ring)).start()

    def mate_blocks(shift, to_group, ring):
        place, to_seq = to_group * seqs + far_seq(ring), near_seq(ring)
        transfer(grad_out_buf.at[place], near_grad_in.at[slot], NEAR_GRAD, to_group, to_seq).start()
        transfer(signal_out_buf.at[place], near_signal_in.at[slot], NEAR_SIGNAL, to_group, to_seq).start()

    def mate_taps(shift, to_group, ring):
        place, to_seq = group * seqs + far_seq(ring), near_seq(ring)
        if shift == 0:

            @pl.when(upper == 0)
            def _():
                transfer(tap_out_buf.at[place], near_tap_in.at[inner], NEAR_TAPS, group, to_seq).start()

    def in_turn(*sends):
        for shift in shifts:
            to_group = lax.rem(group + shift, groups) if shift else group
            for offset in reversed(range(half_seqs)):
                ring = lax.rem(inner + offset, half_seqs) if offset else inner
                for send in sends:
                    if shift or offset or send in (far_block, far_taps):
                        send(shift, to_group, ring)

    in_turn(far_taps, near_taps, mate_taps)
    in_turn(mate_blocks)
    in_turn(far_block, near_grad_block)
    in_turn(near_signal_block)
    grad_in[me] = grad_out_buf[me]
    tap_in[seq] = tap_out_buf[me]
    signal_in[me] = signal_out_buf[me]
    near_grad_in[slot] = grad_out_buf[group * seqs + mate]
    near_signal_in[slot] = signal_out_buf[group * seqs + mate]
    near_tap_in[inner] = tap_out_buf[group * seqs + mate]

    def spread(blocks, target, first_row):
        place = pl.ds(first_row, own)
        for k, (real, imag) in enumerate(coarse_forward(blocks)):
            row = k * (seqs // len(blocks))
            real, imag = turn(real, imag, cos_ref[row], sin_ref[row])
            target[k, place, re] = real
            target[k, place, im] = imag

    def fine(source, target):
        lines = source.shape[0] * source.shape[1]
        value = source[...].reshape(lines, 2 * rows)
        high = value.astype(BF16)
        low = (value - high.astype(F32)).astype(BF16)
        product = functools.partial(jnp.dot, preferred_element_type=F32)
        total = product(high, high_ref[...]) + product(low, high_ref[...]) + product(high, low_ref[...])
        target[...] = total.reshape(target.shape)

    def collect(source, first_row, pieces):
        place, stride = pl.ds(first_row, own), seqs // pieces
        terms = [
            turn(source[k, place, re], source[k, place, im], cos_ref[k * stride], sin_ref[k * stride])
            for k in range(pieces + 1)
        ]
        return coarse_inverse(terms, 1.0 / (2 * pieces * rows))

    def row_of(index):
        return pl.multiple_of(index * own, own)

    for copy in loads[3:]:
        copy.wait()
    all_of(tap_in, seqs - 1, TAPS).wait_recv()
    spread([tap_in[s] for s in range(seqs)], tap_rows, 0)
    fine(tap_rows, tap_spec)

    @pl.when(upper == 0)
    def _():
        all_of(near_tap_in, half_seqs - 1, NEAR_TAPS).wait_recv()
        spread([near_tap_in[s] for s in range(half_seqs)], near_tap, 0)
        fine(near_tap, near_tap)

    all_of(near_grad_in, near_count - 1, NEAR_GRAD).wait_recv()
    all_of(near_signal_in, near_count - 1, NEAR_SIGNAL).wait_recv()

    def spread_near(index, carry):
        for source, target in ((near_grad_in, near_grad), (near_signal_in, near_signal)):
            spread([source[index * half_seqs + s] for s in range(half_seqs)], target, row_of(index))
        return carry

    lax.fori_loop(0, groups, spread_near, 0)
    fine(near_grad, near_grad)
    fine(near_signal, near_signal)
    for k in range(half_seqs + 1):
        real, imag = None, None
        for index in range(groups):
            place = pl.ds(index * own, own)
            grad_re, grad_im = near_grad[k, place, re], near_grad[k, place, im]
            signal_re, signal_im = near_signal[k, place, re], near_signal[k, place, im]
            real = added(real, grad_re * signal_re + grad_im * signal_im)
            imag = added(imag, grad_re * signal_im - grad_im * signal_re)
        near_filter[k, :, re] = real
        near_filter[k, :, im] = imag
    fine(near_filter, near_filter)
    for s, block in enumerate(collect(near_filter, 0, half_seqs)):
        near_filter_out[s] = block
    transfer(near_filter_out, part_in, PART, group, mate).start()

    @pl.when(upper == 0)
    def _():
        def multiply_near(index, carry):
            place = pl.ds(row_of(index), own)
            for k in range(half_seqs + 1):
                grad_re, grad_im = near_grad[k, place, re], near_grad[k, place, im]
                tap_re, tap_im = near_tap[k, :, re], near_tap[k, :, im]
                near_lines[k, place, re] = grad_re * tap_re + grad_im * tap_im
                near_lines[k, place, im] = grad_re * tap_im - grad_im * tap_re
            return carry

        lax.fori_loop(0, groups, multiply_near, 0)
        fine(near_lines, near_lines)

        def collect_near(index, carry):
            for s, block in enumerate(collect(near_lines, row_of(index), half_seqs)):
                near_input_out[index * half_seqs + s] = block
            return carry

        lax.fori_loop(0, groups, collect_near, 0)
        for shift in shifts:
            to_group = lax.rem(group + shift, groups) if shift else group
            for offset in reversed(range(half_seqs)):
                if shift or offset:
                    ring = lax.rem(inner + offset, half_seqs)
                    transfer(
                        near_input_out.at[to_group * half_seqs + ring], near_input_in.at[slot],
                        NEAR_INPUT, to_group, ring,
                    ).start()
        near_input_in[slot] = near_input_out[slot]

    all_of(grad_in, near_count - 1, GRAD).wait_recv()
    pl.when(upper == 0)(lambda: all_of(grad_in, near_count, CROSS).wait_recv())

    def group_at(index):
        return lax.rem(2 * pair + index, groups)

    def input_part(first):
        source, spectrum, lines = grad_rows.at[first], grad_spec.at[first], input_rows.at[first]

        def spread_grad(index, carry):
            here = group_at(2 * first + index)
            spread([grad_in[here * seqs + s] for s in range(seqs)], source, row_of(index))
            return carry

        def transform():
            lax.fori_loop(0, 2, spread_grad, 0)
            fine(source, spectrum)

        def multiply_taps(index, carry):
            place = pl.ds(row_of(index), own)
            for k in range(coarse):
                grad_re, grad_im = spectrum[k, place, re], spectrum[k, place, im]
                tap_re, tap_im = tap_spec[k, :, re], tap_spec[k, :, im]
                lines[k, place, re] = grad_re * tap_re + grad_im * tap_im
                lines[k, place, im] = grad_re * tap_im - grad_im * tap_re
            return carry

        def collect_input(index, carry):
            here = group_at(2 * first + index)
            for s, block in enumerate(collect(lines, row_of(index), seqs)):
                input_out[here * seqs + s] = block
            return carry

        def finish():
            lax.fori_loop(0, 2, multiply_taps, 0)
            fine(lines, lines)
            lax.fori_loop(0, 2, collect_input, 0)

            for offset in turns:
                for flip in range(2):
                    if first or offset or flip:
                        to_group = group_at(2 * first + lax.rem(parity + flip, 2))
                        to_seq = turned_seq(offset)
                        place = to_group * seqs + to_seq
                        transfer(input_out.at[place], input_in.at[me], INPUT, to_group, to_seq).start()

        return transform, finish

    parts = [input_part(first) for first in reversed(range(half_groups))]
    parts[0][0]()
    parts[0][1]()
    for transform, _ in parts[1:]:
        transform()

    all_of(signal_in, near_count - 1, SIGNAL).wait_recv()
    pl.when(upper == 1)(lambda: all_of(signal_in, near_count, CROSS).wait_recv())

    def spread_signal(index, carry):
        here = group_at(index)
        spread([signal_in[here * seqs + s] for s in range(seqs)], signal_rows, row_of(index))
        return carry

    lax.fori_loop(0, groups, spread_signal, 0)
    fine(signal_rows, signal_spec)
    for k in range(coarse):
        real, imag = None, None
        for index in range(groups):
            place = pl.ds(index * own, own)
            which, local = index // 2, pl.ds(index % 2 * own, own)
            grad_re, grad_im = grad_spec[which, k, local, re], grad_spec[which, k, local, im]
            signal_re, signal_im = signal_spec[k, place, re], signal_spec[k, place, im]
            real = added(real, grad_re * signal_re + grad_im * signal_im)
            imag = added(imag, grad_re * signal_im - grad_im * signal_re)
        filter_rows[k, :, re] = real
        filter_rows[k, :, im] = imag
    fine(filter_rows, filter_spec)
    all_of(part_in, half_seqs, PART).wait_recv()
    for s, block in enumerate(collect(filter_spec, 0, seqs)):
        filter_out[s] = block + part_in[s] if s < half_seqs else block

    for offset in turns:
        for flip in range(half_groups):
            if offset or flip:
                to_group = 2 * lax.rem(pair + flip, half_groups) + parity
                to_seq = turned_seq(offset)
                transfer(
                    filter_out.at[to_seq], filter_in.at[parity, pair * seqs + seq], FILTER, to_group, to_seq
                ).start()
    for _, finish in parts[1:]:
        finish()
    input_in[me] = input_out[me]
    filter_in[parity, pair * seqs + seq] = filter_out[seq]

    half = count // 2
    all_of(filter_in.at[0], half - 1, FILTER).wait_recv()
    mine = filter_in.at[parity]
    partner = 2 * pair + 1 - parity
    forward = transfer(mine, mine, FORWARD, partner, seq)
    forward.start()
    all_of(input_in, count - 1, INPUT).wait_recv()

    @pl.when(upper == 0)
    def _():
        all_of(near_input_in, near_count - 1, NEAR_INPUT).wait_recv()
        for where in range(groups):
            far = slice(where * seqs + half_seqs, (where + 1) * seqs)
            input_in[far] = input_in[far] + near_input_in[where * half_seqs : (where + 1) * half_seqs]

    gradient = input_in[...].reshape(channels, rows).T + skip_ref[...] * grad_ref[...].astype(F32)
    input_ref[...] = gradient.astype(BF16)
    forward.wait_recv()
    for kind in (GRAD, SIGNAL, NEAR_GRAD, NEAR_SIGNAL):
        all_of(grad_in, near_count - 1, kind).wait_send()
    all_of(grad_in, near_count, CROSS).wait_send()
    all_of(part_in, half_seqs, PART).wait_send()

    @pl.when(upper == 0)
    def _():
        all_of(grad_in, near_count - 1, NEAR_INPUT).wait_send()
        all_of(tap_in, half_seqs - 1, NEAR_TAPS).wait_send()

    all_of(input_in, count - 1, INPUT).wait_send()
    all_of(filter_in.at[0], half - 1, FILTER).wait_send()
    forward.wait_send()
    all_of(tap_in, seqs - 1, TAPS).wait_send()


def finish_kernel(groups, seqs, input_ref, filter_in, input_hbm, filter_hbm, filter_ref, sems):
    own, rows = filter_in.shape[2:]
    input_store = pltpu.make_async_copy(input_ref, input_hbm, sems.at[0])
    input_store.start()
    parts = [
        filter_in[which, first * seqs : (first + 1) * seqs].reshape(seqs * own, rows)
        for first in range(groups // 2)
        for which in range(2)
    ]
    filter_ref[...] = jnp.concatenate(parts, axis=0).T
    filter_store = pltpu.make_async_copy(filter_ref, filter_hbm, sems.at[1])
    filter_store.start()
    input_store.wait()
    filter_store.wait()


def fine_tables(rows):
    grid = np.arange(rows)
    angle = 2.0 * np.pi / rows * (np.outer(grid, grid) % rows)
    table = np.block([[np.cos(angle), -np.sin(angle)], [np.sin(angle), np.cos(angle)]]).astype(np.float32)
    high = table.astype(BF16)
    return high, (table - high.astype(np.float32)).astype(BF16)


def turn_tables(seqs, rows, lines):
    angle = np.pi / (seqs * rows) * np.outer(np.arange(seqs + 1), np.arange(rows))
    wide = np.broadcast_to(angle[:, None, :], (seqs + 1, lines, rows))
    return np.cos(wide).astype(np.float32), np.sin(wide).astype(np.float32)


def fused_shards(groups, seqs, signal, grad_out, filter_taps, skip_gain):
    rows, channels = filter_taps.shape
    count, coarse = groups * seqs, seqs + 1
    own = channels // count
    high, low = fine_tables(rows)
    cos_turn, sin_turn = turn_tables(seqs, rows, own)
    blocks = pltpu.VMEM((count, own, rows), F32)
    few = pltpu.VMEM((seqs, own, rows), F32)
    half_blocks = pltpu.VMEM((count // 2, own, rows), F32)
    half_few = pltpu.VMEM((seqs // 2, own, rows), F32)
    near = lambda number: pltpu.VMEM((seqs // 2 + 1, number * own, 2 * rows), F32)
    lines = lambda number: pltpu.VMEM((coarse, number * own, 2 * rows), F32)
    pairs = pltpu.VMEM((groups // 2, coarse, 2 * own, 2 * rows), F32)
    hbm = pl.BlockSpec(memory_space=pltpu.HBM)
    turns = pltpu.VMEM((coarse, own, rows), F32)
    table = pltpu.VMEM((2 * rows, 2 * rows), BF16)
    vmem = pl.BlockSpec(memory_space=pltpu.VMEM)
    gathered = pl.pallas_call(
        functools.partial(fused_kernel, groups, seqs),
        out_shape=(
            pltpu.VMEM((rows, channels), BF16),
            pltpu.VMEM((2, count // 2, own, rows), F32),
        ),
        in_specs=[hbm] * 8,
        out_specs=(vmem, vmem),
        scratch_shapes=[
            pltpu.VMEM((rows, channels), BF16), pltpu.VMEM((rows, channels), BF16),
            pltpu.VMEM((rows, channels), F32), pltpu.VMEM((1, channels), F32),
            table, table, turns, turns,
            blocks, blocks, blocks, blocks, blocks, few,
            blocks, few, blocks,
            lines(1), lines(1), pairs, pairs, lines(groups), lines(groups),
            pairs, lines(1), lines(1),
            half_blocks, half_blocks, half_few, half_blocks, half_blocks, half_few, half_few,
            near(groups), near(groups), near(1), near(groups), near(1),
            pltpu.SemaphoreType.DMA((12,)),
            pltpu.SemaphoreType.DMA((12,)),
            pltpu.SemaphoreType.DMA((8,)),
        ],
        compiler_params=pltpu.CompilerParams(
            collective_id=0, has_side_effects=True, vmem_limit_bytes=24 << 20
        ),
    )(
        *(
            pltpu.with_memory_space_constraint(array, pltpu.HBM)
            for array in (
                signal[0], grad_out[0], filter_taps, skip_gain[None, :],
                jnp.asarray(high), jnp.asarray(low), jnp.asarray(cos_turn), jnp.asarray(sin_turn),
            )
        )
    )
    input_grad, filter_grad = pl.pallas_call(
        functools.partial(finish_kernel, groups, seqs),
        out_shape=(
            jax.ShapeDtypeStruct((rows, channels), BF16),
            jax.ShapeDtypeStruct((rows, channels), F32),
        ),
        in_specs=[vmem] * 2,
        out_specs=(hbm, hbm),
        scratch_shapes=[
            pltpu.VMEM((rows, channels), F32),
            pltpu.SemaphoreType.DMA((2,)),
        ],
        compiler_params=pltpu.CompilerParams(vmem_limit_bytes=24 << 20),
    )(*gathered)
    return input_grad[None], filter_grad


def fits_fused(groups, seqs, signal, filter_taps):
    rows, channels = filter_taps.shape
    return (
        signal.shape[0] == 1
        and seqs % 4 == 0
        and groups % 2 == 0
        and rows % 128 == 0
        and channels % (8 * groups * seqs) == 0
    )


def angle_table(height, width, period):
    product = lax.broadcasted_iota(jnp.int32, (height, width), 0) * lax.broadcasted_iota(
        jnp.int32, (height, width), 1
    )
    return 2.0 * jnp.pi / period * (product % period).astype(jnp.float32)


def angle_of(product, period):
    return 2.0 * jnp.pi / period * (product % period).astype(jnp.float32)


def coarse_order(slot, seq_count):
    pair_index = slot // 2
    odd_slot = slot % 2
    return jnp.where(
        pair_index == 0,
        odd_slot * seq_count,
        jnp.where(odd_slot == 0, pair_index, 2 * seq_count - pair_index),
    )


def contract(form, table, operand):
    return jnp.einsum(form, table, operand, precision=lax.Precision.HIGHEST)


def forward_spectra(columns):
    seq_count = lax.axis_size("seq")
    row_count = columns.shape[0]
    part_rows = row_count // seq_count
    period_len = 2 * row_count * seq_count
    spread = lax.all_to_all(
        columns.reshape(1, row_count, columns.shape[1]),
        "seq",
        split_axis=1,
        concat_axis=0,
        tiled=True,
    )
    slot_grid = lax.broadcasted_iota(jnp.int32, (2 * seq_count, seq_count), 0)
    source_grid = lax.broadcasted_iota(jnp.int32, (2 * seq_count, seq_count), 1)
    first_table = angle_of(coarse_order(slot_grid, seq_count) * source_grid, 2 * seq_count)
    cos_first = jnp.cos(first_table)
    sin_first = jnp.sin(first_table)
    half_width = spread.shape[2] // 2
    real_in = spread[:, :, :half_width]
    imag_in = spread[:, :, half_width:]
    real_part = contract("ks,srw->krw", cos_first, real_in) + contract(
        "ks,srw->krw", sin_first, imag_in
    )
    imag_part = contract("ks,srw->krw", cos_first, imag_in) - contract(
        "ks,srw->krw", sin_first, real_in
    )
    global_row = lax.axis_index("seq") * part_rows + lax.broadcasted_iota(
        jnp.int32, (2 * seq_count, part_rows), 1
    )
    coarse = coarse_order(lax.broadcasted_iota(jnp.int32, (2 * seq_count, part_rows), 0), seq_count)
    phases = angle_of(global_row * coarse, period_len)
    cos_turn = jnp.cos(phases)[:, :, None]
    sin_turn = jnp.sin(phases)[:, :, None]
    rotated = jnp.stack(
        [real_part * cos_turn + imag_part * sin_turn, imag_part * cos_turn - real_part * sin_turn]
    )
    inner_table = angle_table(row_count, row_count, row_count)
    cos_inner = jnp.cos(inner_table)
    sin_inner = jnp.sin(inner_table)
    pieces = lax.all_to_all(rotated, "seq", split_axis=1, concat_axis=2, tiled=True)
    real_sum = contract("qr,krw->kqw", cos_inner, pieces[0]) + contract(
        "qr,krw->kqw", sin_inner, pieces[1]
    )
    imag_sum = contract("qr,krw->kqw", cos_inner, pieces[1]) - contract(
        "qr,krw->kqw", sin_inner, pieces[0]
    )
    return jnp.stack([real_sum, imag_sum])


def split_pairs(packed):
    reversed_q = packed[:, :, ::-1]
    zero_row = jnp.roll(reversed_q[:, 0], 1, axis=1)
    own_pair = jnp.stack([zero_row, reversed_q[:, 1]], axis=1)
    partner = jnp.where(lax.axis_index("seq") == 0, own_pair, reversed_q[:, ::-1])
    first = jnp.stack([0.5 * (packed[0] + partner[0]), 0.5 * (packed[1] - partner[1])])
    second = jnp.stack([0.5 * (packed[1] + partner[1]), 0.5 * (partner[0] - packed[0])])
    return (first, second)


def inverse_rows(spectra):
    seq_count = lax.axis_size("seq")
    row_count = spectra.shape[2]
    period_len = 2 * row_count * seq_count
    inner_table = angle_table(row_count, row_count, row_count)
    cos_inner = jnp.cos(inner_table)
    sin_inner = jnp.sin(inner_table)
    real_sum = contract("qr,krw->kqw", cos_inner, spectra[0]) - contract(
        "qr,krw->kqw", sin_inner, spectra[1]
    )
    imag_sum = contract("qr,krw->kqw", cos_inner, spectra[1]) + contract(
        "qr,krw->kqw", sin_inner, spectra[0]
    )
    coarse = coarse_order(
        2 * lax.axis_index("seq") + lax.broadcasted_iota(jnp.int32, (2, row_count), 0), seq_count
    )
    position = lax.broadcasted_iota(jnp.int32, (2, row_count), 1)
    phases = angle_of(position * coarse, period_len)
    cos_turn = jnp.cos(phases)[:, :, None]
    sin_turn = jnp.sin(phases)[:, :, None]
    rotated = jnp.stack(
        [real_sum * cos_turn - imag_sum * sin_turn, real_sum * sin_turn + imag_sum * cos_turn]
    )
    target_grid = lax.broadcasted_iota(jnp.int32, (seq_count, 2 * seq_count), 0)
    slot_grid = lax.broadcasted_iota(jnp.int32, (seq_count, 2 * seq_count), 1)
    last_table = angle_of(target_grid * coarse_order(slot_grid, seq_count), 2 * seq_count)
    cos_last = jnp.cos(last_table)
    sin_last = jnp.sin(last_table)
    pieces = lax.all_to_all(rotated, "seq", split_axis=2, concat_axis=1, tiled=True)
    value = contract("sk,krw->srw", cos_last, pieces[0]) - contract(
        "sk,krw->srw", sin_last, pieces[1]
    )
    other = contract("sk,krw->srw", sin_last, pieces[0]) + contract(
        "sk,krw->srw", cos_last, pieces[1]
    )
    gathered = (value / period_len, other / period_len)
    gathered = jnp.concatenate([gathered[0], gathered[1]], axis=2)
    home_rows = lax.all_to_all(gathered, "seq", split_axis=0, concat_axis=1, tiled=True)
    return home_rows.reshape(row_count, home_rows.shape[2])


def invert_all(spectra):
    half_width = spectra.shape[3] // 2
    joined = jnp.stack(
        [
            spectra[0, :, :, :half_width] - spectra[1, :, :, half_width:],
            spectra[1, :, :, :half_width] + spectra[0, :, :, half_width:],
        ]
    )
    return inverse_rows(joined)


def shards(signal, grad_out, filter_taps, skip_gain):
    channels = filter_taps.shape[1]
    signal_rows = signal[0].astype(jnp.float32)
    grad_rows = grad_out[0].astype(jnp.float32)
    tap_half = filter_taps.shape[1] // 2
    columns = jnp.concatenate(
        [signal_rows, filter_taps[:, :tap_half], grad_rows, filter_taps[:, tap_half:]], axis=1
    )
    first, second = split_pairs(forward_spectra(columns))
    signal_spec = first[:, :, :, :channels]
    grad_spec = second[:, :, :, :channels]
    own_spec = jnp.concatenate([first[:, :, :, channels:], second[:, :, :, channels:]], axis=3)
    input_spec = jnp.stack(
        [
            grad_spec[0] * own_spec[0] + grad_spec[1] * own_spec[1],
            grad_spec[1] * own_spec[0] - grad_spec[0] * own_spec[1],
        ]
    )
    filter_terms = jnp.stack(
        [
            grad_spec[0] * signal_spec[0] + grad_spec[1] * signal_spec[1],
            grad_spec[1] * signal_spec[0] - grad_spec[0] * signal_spec[1],
        ]
    )
    summed = lax.psum(filter_terms, "batch")
    rows_back = invert_all(jnp.concatenate([input_spec, summed], axis=3))
    filter_grad = rows_back[:, channels:]
    input_grad = (rows_back[:, :channels] + skip_gain[None, :] * grad_rows).astype(jnp.bfloat16)
    return (input_grad[None], filter_grad)


def solution(mesh):
    groups, seqs = mesh.shape["batch"], mesh.shape["seq"]

    def either(signal, grad_out, filter_taps, skip_gain):
        if fits_fused(groups, seqs, signal, filter_taps):
            return fused_shards(groups, seqs, signal, grad_out, filter_taps, skip_gain)
        return shards(signal, grad_out, filter_taps, skip_gain)

    return jax.shard_map(
        either,
        mesh=mesh,
        in_specs=(P("batch", "seq", None), P("batch", "seq", None), P("seq", None), P()),
        out_specs=(P("batch", "seq", None), P("seq", None)),
        check_vma=False,
    )
```

```python
import functools
import math

import jax
import jax.numpy as jnp
import numpy as np
from jax import lax
from jax.experimental import pallas as pl
from jax.experimental.pallas import tpu as pltpu
from jax.sharding import PartitionSpec as P

MESH = pl.DeviceIdType.MESH
F32 = jnp.float32
BF16 = jnp.bfloat16
GRAD, TAPS, SIGNAL, INPUT, FILTER, FORWARD, CROSS, NEAR_GRAD, NEAR_SIGNAL, NEAR_TAPS, PART, NEAR_INPUT, CROSS_OWN = range(13)


def weighted(terms):
    total = None
    for factor, array in terms:
        if array is None or abs(factor) < 1e-12:
            continue
        if total is None:
            if abs(factor - 1.0) < 1e-12:
                total = array
            else:
                total = array * factor
        elif abs(factor - 1.0) < 1e-12:
            total = total + array
        elif abs(factor + 1.0) < 1e-12:
            total = total - array
        else:
            total = total + array * factor
    return total


def added(left, right):
    return weighted([(1.0, left), (1.0, right)])


def subtracted(left, right):
    return weighted([(1.0, left), (-1.0, right)])


def turn(real, imag, cos_turn, sin_turn):
    if imag is None:
        return real * cos_turn, -(real * sin_turn)
    return real * cos_turn + imag * sin_turn, imag * cos_turn - real * sin_turn


def coarse_forward(blocks):
    count = len(blocks)
    result = [None] * (count + 1)
    for k in range(count // 2 + 1):
        sums = []
        for parity in (0, 1):
            angles = [(math.pi * ((s * k) % (2 * count)) / count, s) for s in range(parity, count, 2)]
            sums.append(
                (
                    weighted([(math.cos(a), blocks[s]) for a, s in angles]),
                    weighted([(-math.sin(a), blocks[s]) for a, s in angles]),
                )
            )
        (even_re, even_im), (odd_re, odd_im) = sums
        result[k] = (added(even_re, odd_re), added(even_im, odd_im))
        if k != count - k:
            result[count - k] = (subtracted(even_re, odd_re), subtracted(odd_im, even_im))
    return result


def coarse_inverse(terms, scale):
    count = len(terms) - 1
    pairs = []
    for k in range(count // 2 + 1):
        weight = scale if k == 0 else 2.0 * scale
        real, imag = terms[k]
        if k == count - k:
            pairs.append((weight, real, imag, real, imag))
        else:
            other_re, other_im = terms[count - k]
            pairs.append((weight, real + other_re, imag - other_im, real - other_re, imag + other_im))
    blocks = []
    for s in range(count):
        parts = []
        for k, (weight, even_re, even_im, odd_re, odd_im) in enumerate(pairs):
            angle = math.pi * ((s * k) % (2 * count)) / count
            parts.append((weight * math.cos(angle) * (1 if abs(math.cos(angle)) > 1e-9 else 0), odd_re if s % 2 else even_re))
            parts.append((weight * math.sin(angle) * (1 if abs(math.sin(angle)) > 1e-9 else 0), odd_im if s % 2 else even_im))
        blocks.append(weighted(parts))
    return blocks


def fused_kernel(
    groups, seqs,
    signal_hbm, grad_hbm, tap_hbm, skip_hbm, high_hbm, low_hbm, cos_hbm, sin_hbm,
    input_ref, filter_in,
    signal_ref, grad_ref, tap_ref, skip_ref, high_ref, low_ref, cos_ref, sin_ref,
    grad_out_buf, signal_out_buf, tap_out_buf, grad_in, signal_in, tap_in,
    input_out, filter_out, input_in,
    tap_rows, tap_spec, grad_rows, grad_spec, signal_rows, signal_spec, input_rows, filter_rows, filter_spec,
    near_grad_in, near_signal_in, near_tap_in, near_input_out, near_input_in, near_filter_out, part_in,
    near_grad, near_signal, near_tap, near_lines, near_filter,
    send_sems, recv_sems, load_sems,
):
    count = groups * seqs
    coarse = seqs + 1
    own, rows = grad_in.shape[1:]
    channels = count * own
    group, seq = lax.axis_index("batch"), lax.axis_index("seq")
    me = group * seqs + seq
    re, im = pl.ds(0, rows), pl.ds(rows, rows)

    parity, pair = lax.rem(group, 2), lax.div(group, 2)
    half_seqs, half_groups = seqs // 2, groups // 2
    upper, inner = lax.div(seq, half_seqs), lax.rem(seq, half_seqs)

    def load(index, source, target):
        return pltpu.make_async_copy(source, target, load_sems.at[index])

    loads = [
        load(index, source, target)
        for index, (source, target) in enumerate(
            (
                (grad_hbm, grad_ref), (tap_hbm, tap_ref), (signal_hbm, signal_ref),
                (cos_hbm, cos_ref), (sin_hbm, sin_ref), (high_hbm, high_ref),
                (low_hbm, low_ref), (skip_hbm, skip_ref),
            )
        )
    ]
    loads[GRAD].start()
    loads[TAPS].start()

    slot, near_count = group * half_seqs + inner, groups * half_seqs
    mate = lax.rem(seq + half_seqs, seqs)
    turns = [(half_seqs + seqs - step) % seqs for step in range(seqs)]

    def turned_seq(offset):
        return lax.rem(seq + offset, seqs) if offset else seq

    shifts = (half_groups, *range(half_groups - 1, -1, -1), *range(half_groups + 1, groups))

    def over_peers(body):
        for shift in shifts:
            to_group = lax.rem(group + shift, groups) if shift else group
            for offset in reversed(range(seqs)):
                if shift or offset:
                    body(to_group, turned_seq(offset), shift == 0)

    def signal(semaphore, to_group, to_seq):
        pl.semaphore_signal(
            semaphore, inc=1, device_id={"batch": to_group, "seq": to_seq}, device_id_type=MESH
        )

    barrier = pltpu.get_barrier_semaphore()

    def greet(to_group, to_seq, same):
        signal(barrier, to_group, to_seq)

    over_peers(greet)
    for copy in loads[2:]:
        copy.start()

    def transfer(source, target, kind, to_group, to_seq):
        return pltpu.make_async_remote_copy(
            src_ref=source,
            dst_ref=target,
            send_sem=send_sems.at[kind],
            recv_sem=recv_sems.at[kind],
            device_id={"batch": to_group, "seq": to_seq},
            device_id_type=MESH,
        )

    def all_of(buffer, blocks, kind):
        view = buffer.at[pl.ds(0, blocks)]
        return transfer(view, view, kind, group, turned_seq(1))

    @pl.when(upper == 0)
    def _():
        for where in range(groups):
            signal_in[where * seqs + half_seqs : (where + 1) * seqs] = jnp.zeros((half_seqs, own, rows), F32)

    @pl.when(upper == 1)
    def _():
        for where in range(groups):
            grad_in[where * seqs : where * seqs + half_seqs] = jnp.zeros((half_seqs, own, rows), F32)

    loads[GRAD].wait()
    grad_out_buf[...] = grad_ref[...].astype(F32).T.reshape(count, own, rows)
    loads[TAPS].wait()
    tap_out_buf[...] = tap_ref[...].T.reshape(count, own, rows)
    loads[SIGNAL].wait()
    signal_out_buf[...] = signal_ref[...].astype(F32).T.reshape(count, own, rows)
    pl.semaphore_wait(barrier, count - 1)

    def near_seq(ring):
        return upper * half_seqs + ring

    def far_seq(ring):
        return (1 - upper) * half_seqs + ring

    def far_block(shift, to_group, ring):
        to_seq, kind = far_seq(ring), CROSS if shift >= 2 else CROSS_OWN
        place = to_group * seqs + to_seq

        @pl.when(upper == 0)
        def _():
            transfer(signal_out_buf.at[place], signal_in.at[me], kind, to_group, to_seq).start()

        @pl.when(upper == 1)
        def _():
            transfer(grad_out_buf.at[place], grad_in.at[me], kind, to_group, to_seq).start()

    def far_taps(shift, to_group, ring):
        if shift == 0:
            place = group * seqs + far_seq(ring)
            transfer(tap_out_buf.at[place], tap_in.at[seq], TAPS, group, far_seq(ring)).start()

    def near_taps(shift, to_group, ring):
        if shift == 0:
            place = group * seqs + near_seq(ring)
            transfer(tap_out_buf.at[place], tap_in.at[seq], TAPS, group, near_seq(ring)).start()

    def near_grad_block(shift, to_group, ring):
        place = to_group * seqs + near_seq(ring)
        transfer(grad_out_buf.at[place], grad_in.at[me], GRAD, to_group, near_seq(ring)).start()

    def near_signal_block(shift, to_group, ring):
        place = to_group * seqs + near_seq(ring)
        transfer(signal_out_buf.at[place], signal_in.at[me], SIGNAL, to_group, near_seq(ring)).start()

    def mate_blocks(shift, to_group, ring):
        place, to_seq = to_group * seqs + far_seq(ring), near_seq(ring)
        transfer(grad_out_buf.at[place], near_grad_in.at[slot], NEAR_GRAD, to_group, to_seq).start()
        transfer(signal_out_buf.at[place], near_signal_in.at[slot], NEAR_SIGNAL, to_group, to_seq).start()

    def mate_taps(shift, to_group, ring):
        place, to_seq = group * seqs + far_seq(ring), near_seq(ring)
        if shift == 0:

            @pl.when(upper == 0)
            def _():
                transfer(tap_out_buf.at[place], near_tap_in.at[inner], NEAR_TAPS, group, to_seq).start()

    def in_turn(*sends):
        for shift in (*range(2, groups), 1, 0):
            to_group = 2 * lax.rem(pair + shift // 2, half_groups) + lax.rem(parity + shift, 2)
            for offset in reversed(range(half_seqs)):
                ring = lax.rem(inner + offset, half_seqs) if offset else inner
                for send in sends:
                    if shift or offset or send in (far_block, far_taps):
                        send(shift, to_group, ring)

    in_turn(far_taps, near_taps, mate_taps)
    in_turn(mate_blocks)
    in_turn(far_block, near_grad_block)
    in_turn(near_signal_block)
    grad_in[me] = grad_out_buf[me]
    tap_in[seq] = tap_out_buf[me]
    signal_in[me] = signal_out_buf[me]
    near_grad_in[slot] = grad_out_buf[group * seqs + mate]
    near_signal_in[slot] = signal_out_buf[group * seqs + mate]
    near_tap_in[inner] = tap_out_buf[group * seqs + mate]

    def spread(blocks, target, first_row):
        place = pl.ds(first_row, own)
        for k, (real, imag) in enumerate(coarse_forward(blocks)):
            row = k * (seqs // len(blocks))
            real, imag = turn(real, imag, cos_ref[row], sin_ref[row])
            target[k, place, re] = real
            target[k, place, im] = imag

    def fine(source, target):
        lines = source.shape[0] * source.shape[1]
        value = source[...].reshape(lines, 2 * rows)
        high = value.astype(BF16)
        low = (value - high.astype(F32)).astype(BF16)
        product = functools.partial(jnp.dot, preferred_element_type=F32)
        total = product(high, high_ref[...]) + product(low, high_ref[...]) + product(high, low_ref[...])
        target[...] = total.reshape(target.shape)

    def collect(source, first_row, pieces):
        place, stride = pl.ds(first_row, own), seqs // pieces
        terms = [
            turn(source[k, place, re], source[k, place, im], cos_ref[k * stride], sin_ref[k * stride])
            for k in range(pieces + 1)
        ]
        return coarse_inverse(terms, 1.0 / (2 * pieces * rows))

    def row_of(index):
        return pl.multiple_of(index * own, own)

    for copy in loads[3:]:
        copy.wait()
    all_of(tap_in, seqs - 1, TAPS).wait_recv()
    spread([tap_in[s] for s in range(seqs)], tap_rows, 0)
    fine(tap_rows, tap_spec)

    @pl.when(upper == 0)
    def _():
        all_of(near_tap_in, half_seqs - 1, NEAR_TAPS).wait_recv()
        spread([near_tap_in[s] for s in range(half_seqs)], near_tap, 0)
        fine(near_tap, near_tap)

    all_of(near_grad_in, near_count - 1, NEAR_GRAD).wait_recv()
    all_of(near_signal_in, near_count - 1, NEAR_SIGNAL).wait_recv()

    def spread_near(index, carry):
        for source, target in ((near_grad_in, near_grad), (near_signal_in, near_signal)):
            spread([source[index * half_seqs + s] for s in range(half_seqs)], target, row_of(index))
        return carry

    lax.fori_loop(0, groups, spread_near, 0)
    fine(near_grad, near_grad)
    fine(near_signal, near_signal)
    for k in range(half_seqs + 1):
        real, imag = None, None
        for index in range(groups):
            place = pl.ds(index * own, own)
            grad_re, grad_im = near_grad[k, place, re], near_grad[k, place, im]
            signal_re, signal_im = near_signal[k, place, re], near_signal[k, place, im]
            real = added(real, grad_re * signal_re + grad_im * signal_im)
            imag = added(imag, grad_re * signal_im - grad_im * signal_re)
        near_filter[k, :, re] = real
        near_filter[k, :, im] = imag
    fine(near_filter, near_filter)
    for s, block in enumerate(collect(near_filter, 0, half_seqs)):
        near_filter_out[s] = block
    transfer(near_filter_out, part_in, PART, group, mate).start()

    @pl.when(upper == 0)
    def _():
        def multiply_near(index, carry):
            place = pl.ds(row_of(index), own)
            for k in range(half_seqs + 1):
                grad_re, grad_im = near_grad[k, place, re], near_grad[k, place, im]
                tap_re, tap_im = near_tap[k, :, re], near_tap[k, :, im]
                near_lines[k, place, re] = grad_re * tap_re + grad_im * tap_im
                near_lines[k, place, im] = grad_re * tap_im - grad_im * tap_re
            return carry

        lax.fori_loop(0, groups, multiply_near, 0)
        fine(near_lines, near_lines)

        def collect_near(index, carry):
            for s, block in enumerate(collect(near_lines, row_of(index), half_seqs)):
                near_input_out[index * half_seqs + s] = block
            return carry

        lax.fori_loop(0, groups, collect_near, 0)
        for shift in shifts:
            to_group = lax.rem(group + shift, groups) if shift else group
            for offset in reversed(range(half_seqs)):
                if shift or offset:
                    ring = lax.rem(inner + offset, half_seqs)
                    transfer(
                        near_input_out.at[to_group * half_seqs + ring], near_input_in.at[slot],
                        NEAR_INPUT, to_group, ring,
                    ).start()
        near_input_in[slot] = near_input_out[slot]

    all_of(grad_in, near_count - 1, GRAD).wait_recv()
    own_far = 2 * half_seqs
    other_far = near_count - own_far
    pl.when(upper == 0)(lambda: all_of(grad_in, other_far, CROSS).wait_recv())

    def group_at(index):
        return lax.rem(2 * pair + index, groups)

    def input_part(first):
        source, spectrum, lines = grad_rows.at[first], grad_spec.at[first], input_rows.at[first]

        def spread_grad(index, carry):
            here = group_at(2 * first + index)
            spread([grad_in[here * seqs + s] for s in range(seqs)], source, row_of(index))
            return carry

        def transform():
            lax.fori_loop(0, 2, spread_grad, 0)
            fine(source, spectrum)

        def multiply_taps(index, carry):
            place = pl.ds(row_of(index), own)
            for k in range(coarse):
                grad_re, grad_im = spectrum[k, place, re], spectrum[k, place, im]
                tap_re, tap_im = tap_spec[k, :, re], tap_spec[k, :, im]
                lines[k, place, re] = grad_re * tap_re + grad_im * tap_im
                lines[k, place, im] = grad_re * tap_im - grad_im * tap_re
            return carry

        def collect_input(index, carry):
            here = group_at(2 * first + index)
            for s, block in enumerate(collect(lines, row_of(index), seqs)):
                input_out[here * seqs + s] = block
            return carry

        def finish():
            lax.fori_loop(0, 2, multiply_taps, 0)
            fine(lines, lines)
            lax.fori_loop(0, 2, collect_input, 0)

            for offset in turns:
                for flip in range(2):
                    if first or offset or flip:
                        to_group = group_at(2 * first + lax.rem(parity + flip, 2))
                        to_seq = turned_seq(offset)
                        place = to_group * seqs + to_seq
                        transfer(input_out.at[place], input_in.at[me], INPUT, to_group, to_seq).start()

        return transform, finish

    parts = [input_part(first) for first in reversed(range(half_groups))]
    parts[0][0]()
    parts[0][1]()
    pl.when(upper == 0)(lambda: all_of(grad_in, own_far, CROSS_OWN).wait_recv())
    for transform, _ in parts[1:]:
        transform()

    all_of(signal_in, near_count - 1, SIGNAL).wait_recv()

    @pl.when(upper == 1)
    def _():
        all_of(signal_in, other_far, CROSS).wait_recv()
        all_of(signal_in, own_far, CROSS_OWN).wait_recv()


    def spread_signal(index, carry):
        here = group_at(index)
        spread([signal_in[here * seqs + s] for s in range(seqs)], signal_rows, row_of(index))
        return carry

    lax.fori_loop(0, groups, spread_signal, 0)
    fine(signal_rows, signal_spec)
    for k in range(coarse):
        real, imag = None, None
        for index in range(groups):
            place = pl.ds(index * own, own)
            which, local = index // 2, pl.ds(index % 2 * own, own)
            grad_re, grad_im = grad_spec[which, k, local, re], grad_spec[which, k, local, im]
            signal_re, signal_im = signal_spec[k, place, re], signal_spec[k, place, im]
            real = added(real, grad_re * signal_re + grad_im * signal_im)
            imag = added(imag, grad_re * signal_im - grad_im * signal_re)
        filter_rows[k, :, re] = real
        filter_rows[k, :, im] = imag
    fine(filter_rows, filter_spec)
    all_of(part_in, half_seqs, PART).wait_recv()
    for s, block in enumerate(collect(filter_spec, 0, seqs)):
        filter_out[s] = block + part_in[s] if s < half_seqs else block

    for offset in turns:
        for flip in range(half_groups):
            if offset or flip:
                to_group = 2 * lax.rem(pair + flip, half_groups) + parity
                to_seq = turned_seq(offset)
                transfer(
                    filter_out.at[to_seq], filter_in.at[parity, pair * seqs + seq], FILTER, to_group, to_seq
                ).start()
    for _, finish in parts[1:]:
        finish()
    input_in[me] = input_out[me]
    filter_in[parity, pair * seqs + seq] = filter_out[seq]

    half = count // 2
    all_of(filter_in.at[0], half - 1, FILTER).wait_recv()
    mine = filter_in.at[parity]
    partner = 2 * pair + 1 - parity
    forward = transfer(mine, mine, FORWARD, partner, seq)
    forward.start()
    all_of(input_in, count - 1, INPUT).wait_recv()

    @pl.when(upper == 0)
    def _():
        all_of(near_input_in, near_count - 1, NEAR_INPUT).wait_recv()
        for where in range(groups):
            far = slice(where * seqs + half_seqs, (where + 1) * seqs)
            input_in[far] = input_in[far] + near_input_in[where * half_seqs : (where + 1) * half_seqs]

    gradient = input_in[...].reshape(channels, rows).T + skip_ref[...] * grad_ref[...].astype(F32)
    input_ref[...] = gradient.astype(BF16)
    forward.wait_recv()
    for kind in (GRAD, SIGNAL, NEAR_GRAD, NEAR_SIGNAL):
        all_of(grad_in, near_count - 1, kind).wait_send()
    all_of(grad_in, other_far, CROSS).wait_send()
    all_of(grad_in, own_far, CROSS_OWN).wait_send()
    all_of(part_in, half_seqs, PART).wait_send()

    @pl.when(upper == 0)
    def _():
        all_of(grad_in, near_count - 1, NEAR_INPUT).wait_send()
        all_of(tap_in, half_seqs - 1, NEAR_TAPS).wait_send()

    all_of(input_in, count - 1, INPUT).wait_send()
    all_of(filter_in.at[0], half - 1, FILTER).wait_send()
    forward.wait_send()
    all_of(tap_in, seqs - 1, TAPS).wait_send()


def finish_kernel(groups, seqs, input_ref, filter_in, input_hbm, filter_hbm, filter_ref, sems):
    own, rows = filter_in.shape[2:]
    input_store = pltpu.make_async_copy(input_ref, input_hbm, sems.at[0])
    input_store.start()
    parts = [
        filter_in[which, first * seqs : (first + 1) * seqs].reshape(seqs * own, rows)
        for first in range(groups // 2)
        for which in range(2)
    ]
    filter_ref[...] = jnp.concatenate(parts, axis=0).T
    filter_store = pltpu.make_async_copy(filter_ref, filter_hbm, sems.at[1])
    filter_store.start()
    input_store.wait()
    filter_store.wait()


def fine_tables(rows):
    grid = np.arange(rows)
    angle = 2.0 * np.pi / rows * (np.outer(grid, grid) % rows)
    table = np.block([[np.cos(angle), -np.sin(angle)], [np.sin(angle), np.cos(angle)]]).astype(np.float32)
    high = table.astype(BF16)
    return high, (table - high.astype(np.float32)).astype(BF16)


def turn_tables(seqs, rows, lines):
    angle = np.pi / (seqs * rows) * np.outer(np.arange(seqs + 1), np.arange(rows))
    wide = np.broadcast_to(angle[:, None, :], (seqs + 1, lines, rows))
    return np.cos(wide).astype(np.float32), np.sin(wide).astype(np.float32)


def fused_shards(groups, seqs, signal, grad_out, filter_taps, skip_gain):
    rows, channels = filter_taps.shape
    count, coarse = groups * seqs, seqs + 1
    own = channels // count
    high, low = fine_tables(rows)
    cos_turn, sin_turn = turn_tables(seqs, rows, own)
    blocks = pltpu.VMEM((count, own, rows), F32)
    few = pltpu.VMEM((seqs, own, rows), F32)
    half_blocks = pltpu.VMEM((count // 2, own, rows), F32)
    half_few = pltpu.VMEM((seqs // 2, own, rows), F32)
    near = lambda number: pltpu.VMEM((seqs // 2 + 1, number * own, 2 * rows), F32)
    lines = lambda number: pltpu.VMEM((coarse, number * own, 2 * rows), F32)
    pairs = pltpu.VMEM((groups // 2, coarse, 2 * own, 2 * rows), F32)
    hbm = pl.BlockSpec(memory_space=pltpu.HBM)
    turns = pltpu.VMEM((coarse, own, rows), F32)
    table = pltpu.VMEM((2 * rows, 2 * rows), BF16)
    vmem = pl.BlockSpec(memory_space=pltpu.VMEM)
    gathered = pl.pallas_call(
        functools.partial(fused_kernel, groups, seqs),
        out_shape=(
            pltpu.VMEM((rows, channels), BF16),
            pltpu.VMEM((2, count // 2, own, rows), F32),
        ),
        in_specs=[hbm] * 8,
        out_specs=(vmem, vmem),
        scratch_shapes=[
            pltpu.VMEM((rows, channels), BF16), pltpu.VMEM((rows, channels), BF16),
            pltpu.VMEM((rows, channels), F32), pltpu.VMEM((1, channels), F32),
            table, table, turns, turns,
            blocks, blocks, blocks, blocks, blocks, few,
            blocks, few, blocks,
            lines(1), lines(1), pairs, pairs, lines(groups), lines(groups),
            pairs, lines(1), lines(1),
            half_blocks, half_blocks, half_few, half_blocks, half_blocks, half_few, half_few,
            near(groups), near(groups), near(1), near(groups), near(1),
            pltpu.SemaphoreType.DMA((13,)),
            pltpu.SemaphoreType.DMA((13,)),
            pltpu.SemaphoreType.DMA((8,)),
        ],
        compiler_params=pltpu.CompilerParams(
            collective_id=0, has_side_effects=True, vmem_limit_bytes=24 << 20
        ),
    )(
        *(
            pltpu.with_memory_space_constraint(array, pltpu.HBM)
            for array in (
                signal[0], grad_out[0], filter_taps, skip_gain[None, :],
                jnp.asarray(high), jnp.asarray(low), jnp.asarray(cos_turn), jnp.asarray(sin_turn),
            )
        )
    )
    input_grad, filter_grad = pl.pallas_call(
        functools.partial(finish_kernel, groups, seqs),
        out_shape=(
            jax.ShapeDtypeStruct((rows, channels), BF16),
            jax.ShapeDtypeStruct((rows, channels), F32),
        ),
        in_specs=[vmem] * 2,
        out_specs=(hbm, hbm),
        scratch_shapes=[
            pltpu.VMEM((rows, channels), F32),
            pltpu.SemaphoreType.DMA((2,)),
        ],
        compiler_params=pltpu.CompilerParams(vmem_limit_bytes=24 << 20),
    )(*gathered)
    return input_grad[None], filter_grad


def fits_fused(groups, seqs, signal, filter_taps):
    rows, channels = filter_taps.shape
    return (
        signal.shape[0] == 1
        and seqs % 4 == 0
        and groups % 2 == 0
        and groups > 2
        and rows % 128 == 0
        and channels % (8 * groups * seqs) == 0
    )


def angle_table(height, width, period):
    product = lax.broadcasted_iota(jnp.int32, (height, width), 0) * lax.broadcasted_iota(
        jnp.int32, (height, width), 1
    )
    return 2.0 * jnp.pi / period * (product % period).astype(jnp.float32)


def angle_of(product, period):
    return 2.0 * jnp.pi / period * (product % period).astype(jnp.float32)


def coarse_order(slot, seq_count):
    pair_index = slot // 2
    odd_slot = slot % 2
    return jnp.where(
        pair_index == 0,
        odd_slot * seq_count,
        jnp.where(odd_slot == 0, pair_index, 2 * seq_count - pair_index),
    )


def contract(form, table, operand):
    return jnp.einsum(form, table, operand, precision=lax.Precision.HIGHEST)


def forward_spectra(columns):
    seq_count = lax.axis_size("seq")
    row_count = columns.shape[0]
    part_rows = row_count // seq_count
    period_len = 2 * row_count * seq_count
    spread = lax.all_to_all(
        columns.reshape(1, row_count, columns.shape[1]),
        "seq",
        split_axis=1,
        concat_axis=0,
        tiled=True,
    )
    slot_grid = lax.broadcasted_iota(jnp.int32, (2 * seq_count, seq_count), 0)
    source_grid = lax.broadcasted_iota(jnp.int32, (2 * seq_count, seq_count), 1)
    first_table = angle_of(coarse_order(slot_grid, seq_count) * source_grid, 2 * seq_count)
    cos_first = jnp.cos(first_table)
    sin_first = jnp.sin(first_table)
    half_width = spread.shape[2] // 2
    real_in = spread[:, :, :half_width]
    imag_in = spread[:, :, half_width:]
    real_part = contract("ks,srw->krw", cos_first, real_in) + contract(
        "ks,srw->krw", sin_first, imag_in
    )
    imag_part = contract("ks,srw->krw", cos_first, imag_in) - contract(
        "ks,srw->krw", sin_first, real_in
    )
    global_row = lax.axis_index("seq") * part_rows + lax.broadcasted_iota(
        jnp.int32, (2 * seq_count, part_rows), 1
    )
    coarse = coarse_order(lax.broadcasted_iota(jnp.int32, (2 * seq_count, part_rows), 0), seq_count)
    phases = angle_of(global_row * coarse, period_len)
    cos_turn = jnp.cos(phases)[:, :, None]
    sin_turn = jnp.sin(phases)[:, :, None]
    rotated = jnp.stack(
        [real_part * cos_turn + imag_part * sin_turn, imag_part * cos_turn - real_part * sin_turn]
    )
    inner_table = angle_table(row_count, row_count, row_count)
    cos_inner = jnp.cos(inner_table)
    sin_inner = jnp.sin(inner_table)
    pieces = lax.all_to_all(rotated, "seq", split_axis=1, concat_axis=2, tiled=True)
    real_sum = contract("qr,krw->kqw", cos_inner, pieces[0]) + contract(
        "qr,krw->kqw", sin_inner, pieces[1]
    )
    imag_sum = contract("qr,krw->kqw", cos_inner, pieces[1]) - contract(
        "qr,krw->kqw", sin_inner, pieces[0]
    )
    return jnp.stack([real_sum, imag_sum])


def split_pairs(packed):
    reversed_q = packed[:, :, ::-1]
    zero_row = jnp.roll(reversed_q[:, 0], 1, axis=1)
    own_pair = jnp.stack([zero_row, reversed_q[:, 1]], axis=1)
    partner = jnp.where(lax.axis_index("seq") == 0, own_pair, reversed_q[:, ::-1])
    first = jnp.stack([0.5 * (packed[0] + partner[0]), 0.5 * (packed[1] - partner[1])])
    second = jnp.stack([0.5 * (packed[1] + partner[1]), 0.5 * (partner[0] - packed[0])])
    return (first, second)


def inverse_rows(spectra):
    seq_count = lax.axis_size("seq")
    row_count = spectra.shape[2]
    period_len = 2 * row_count * seq_count
    inner_table = angle_table(row_count, row_count, row_count)
    cos_inner = jnp.cos(inner_table)
    sin_inner = jnp.sin(inner_table)
    real_sum = contract("qr,krw->kqw", cos_inner, spectra[0]) - contract(
        "qr,krw->kqw", sin_inner, spectra[1]
    )
    imag_sum = contract("qr,krw->kqw", cos_inner, spectra[1]) + contract(
        "qr,krw->kqw", sin_inner, spectra[0]
    )
    coarse = coarse_order(
        2 * lax.axis_index("seq") + lax.broadcasted_iota(jnp.int32, (2, row_count), 0), seq_count
    )
    position = lax.broadcasted_iota(jnp.int32, (2, row_count), 1)
    phases = angle_of(position * coarse, period_len)
    cos_turn = jnp.cos(phases)[:, :, None]
    sin_turn = jnp.sin(phases)[:, :, None]
    rotated = jnp.stack(
        [real_sum * cos_turn - imag_sum * sin_turn, real_sum * sin_turn + imag_sum * cos_turn]
    )
    target_grid = lax.broadcasted_iota(jnp.int32, (seq_count, 2 * seq_count), 0)
    slot_grid = lax.broadcasted_iota(jnp.int32, (seq_count, 2 * seq_count), 1)
    last_table = angle_of(target_grid * coarse_order(slot_grid, seq_count), 2 * seq_count)
    cos_last = jnp.cos(last_table)
    sin_last = jnp.sin(last_table)
    pieces = lax.all_to_all(rotated, "seq", split_axis=2, concat_axis=1, tiled=True)
    value = contract("sk,krw->srw", cos_last, pieces[0]) - contract(
        "sk,krw->srw", sin_last, pieces[1]
    )
    other = contract("sk,krw->srw", sin_last, pieces[0]) + contract(
        "sk,krw->srw", cos_last, pieces[1]
    )
    gathered = (value / period_len, other / period_len)
    gathered = jnp.concatenate([gathered[0], gathered[1]], axis=2)
    home_rows = lax.all_to_all(gathered, "seq", split_axis=0, concat_axis=1, tiled=True)
    return home_rows.reshape(row_count, home_rows.shape[2])


def invert_all(spectra):
    half_width = spectra.shape[3] // 2
    joined = jnp.stack(
        [
            spectra[0, :, :, :half_width] - spectra[1, :, :, half_width:],
            spectra[1, :, :, :half_width] + spectra[0, :, :, half_width:],
        ]
    )
    return inverse_rows(joined)


def shards(signal, grad_out, filter_taps, skip_gain):
    channels = filter_taps.shape[1]
    signal_rows = signal[0].astype(jnp.float32)
    grad_rows = grad_out[0].astype(jnp.float32)
    tap_half = filter_taps.shape[1] // 2
    columns = jnp.concatenate(
        [signal_rows, filter_taps[:, :tap_half], grad_rows, filter_taps[:, tap_half:]], axis=1
    )
    first, second = split_pairs(forward_spectra(columns))
    signal_spec = first[:, :, :, :channels]
    grad_spec = second[:, :, :, :channels]
    own_spec = jnp.concatenate([first[:, :, :, channels:], second[:, :, :, channels:]], axis=3)
    input_spec = jnp.stack(
        [
            grad_spec[0] * own_spec[0] + grad_spec[1] * own_spec[1],
            grad_spec[1] * own_spec[0] - grad_spec[0] * own_spec[1],
        ]
    )
    filter_terms = jnp.stack(
        [
            grad_spec[0] * signal_spec[0] + grad_spec[1] * signal_spec[1],
            grad_spec[1] * signal_spec[0] - grad_spec[0] * signal_spec[1],
        ]
    )
    summed = lax.psum(filter_terms, "batch")
    rows_back = invert_all(jnp.concatenate([input_spec, summed], axis=3))
    filter_grad = rows_back[:, channels:]
    input_grad = (rows_back[:, :channels] + skip_gain[None, :] * grad_rows).astype(jnp.bfloat16)
    return (input_grad[None], filter_grad)


def solution(mesh):
    groups, seqs = mesh.shape["batch"], mesh.shape["seq"]

    def either(signal, grad_out, filter_taps, skip_gain):
        if fits_fused(groups, seqs, signal, filter_taps):
            return fused_shards(groups, seqs, signal, grad_out, filter_taps, skip_gain)
        return shards(signal, grad_out, filter_taps, skip_gain)

    return jax.shard_map(
        either,
        mesh=mesh,
        in_specs=(P("batch", "seq", None), P("batch", "seq", None), P("seq", None), P()),
        out_specs=(P("batch", "seq", None), P("seq", None)),
        check_vma=False,
    )
```

```python
import functools
import math

import jax
import jax.numpy as jnp
import numpy as np
from jax import lax
from jax.experimental import pallas as pl
from jax.experimental.pallas import tpu as pltpu
from jax.sharding import PartitionSpec as P

MESH = pl.DeviceIdType.MESH
F32 = jnp.float32
BF16 = jnp.bfloat16
GRAD, TAPS, SIGNAL, INPUT, FILTER, FORWARD, CROSS, NEAR_GRAD, NEAR_SIGNAL, NEAR_TAPS, PART, NEAR_INPUT, CROSS_OWN = range(13)


def weighted(terms):
    total = None
    for factor, array in terms:
        if array is None or abs(factor) < 1e-12:
            continue
        if total is None:
            if abs(factor - 1.0) < 1e-12:
                total = array
            else:
                total = array * factor
        elif abs(factor - 1.0) < 1e-12:
            total = total + array
        elif abs(factor + 1.0) < 1e-12:
            total = total - array
        else:
            total = total + array * factor
    return total


def added(left, right):
    return weighted([(1.0, left), (1.0, right)])


def subtracted(left, right):
    return weighted([(1.0, left), (-1.0, right)])


def turn(real, imag, cos_turn, sin_turn):
    if imag is None:
        return real * cos_turn, -(real * sin_turn)
    return real * cos_turn + imag * sin_turn, imag * cos_turn - real * sin_turn


def coarse_forward(blocks):
    count = len(blocks)
    result = [None] * (count + 1)
    for k in range(count // 2 + 1):
        sums = []
        for parity in (0, 1):
            angles = [(math.pi * ((s * k) % (2 * count)) / count, s) for s in range(parity, count, 2)]
            sums.append(
                (
                    weighted([(math.cos(a), blocks[s]) for a, s in angles]),
                    weighted([(-math.sin(a), blocks[s]) for a, s in angles]),
                )
            )
        (even_re, even_im), (odd_re, odd_im) = sums
        result[k] = (added(even_re, odd_re), added(even_im, odd_im))
        if k != count - k:
            result[count - k] = (subtracted(even_re, odd_re), subtracted(odd_im, even_im))
    return result


def coarse_inverse(terms, scale):
    count = len(terms) - 1
    pairs = []
    for k in range(count // 2 + 1):
        weight = scale if k == 0 else 2.0 * scale
        real, imag = terms[k]
        if k == count - k:
            pairs.append((weight, real, imag, real, imag))
        else:
            other_re, other_im = terms[count - k]
            pairs.append((weight, real + other_re, imag - other_im, real - other_re, imag + other_im))
    blocks = []
    for s in range(count):
        parts = []
        for k, (weight, even_re, even_im, odd_re, odd_im) in enumerate(pairs):
            angle = math.pi * ((s * k) % (2 * count)) / count
            parts.append((weight * math.cos(angle) * (1 if abs(math.cos(angle)) > 1e-9 else 0), odd_re if s % 2 else even_re))
            parts.append((weight * math.sin(angle) * (1 if abs(math.sin(angle)) > 1e-9 else 0), odd_im if s % 2 else even_im))
        blocks.append(weighted(parts))
    return blocks


def fused_kernel(
    groups, seqs,
    signal_hbm, grad_hbm, tap_hbm, skip_hbm, high_hbm, low_hbm, cos_hbm, sin_hbm,
    input_ref, filter_in,
    signal_ref, grad_ref, tap_ref, skip_ref, high_ref, low_ref, cos_ref, sin_ref,
    grad_out_buf, signal_out_buf, tap_out_buf, grad_in, signal_in, tap_in,
    input_out, filter_out, input_in,
    tap_rows, tap_spec, grad_rows, grad_spec, signal_rows, signal_spec, input_rows, filter_rows, filter_spec,
    near_grad_in, near_signal_in, near_tap_in, near_input_out, near_input_in, near_filter_out, part_in,
    near_grad, near_signal, near_tap, near_lines, near_filter,
    send_sems, recv_sems, load_sems,
):
    count = groups * seqs
    coarse = seqs + 1
    own, rows = grad_in.shape[1:]
    channels = count * own
    group, seq = lax.axis_index("batch"), lax.axis_index("seq")
    me = group * seqs + seq
    re, im = pl.ds(0, rows), pl.ds(rows, rows)

    parity, pair = lax.rem(group, 2), lax.div(group, 2)
    half_seqs, half_groups = seqs // 2, groups // 2
    upper, inner = lax.div(seq, half_seqs), lax.rem(seq, half_seqs)

    def load(index, source, target):
        return pltpu.make_async_copy(source, target, load_sems.at[index])

    loads = [
        load(index, source, target)
        for index, (source, target) in enumerate(
            (
                (grad_hbm, grad_ref), (tap_hbm, tap_ref), (signal_hbm, signal_ref),
                (cos_hbm, cos_ref), (sin_hbm, sin_ref), (high_hbm, high_ref),
                (low_hbm, low_ref), (skip_hbm, skip_ref),
            )
        )
    ]
    loads[GRAD].start()
    loads[TAPS].start()

    slot, near_count = group * half_seqs + inner, groups * half_seqs
    mate = lax.rem(seq + half_seqs, seqs)
    turns = [(half_seqs + seqs - step) % seqs for step in range(seqs)]

    def turned_seq(offset):
        return lax.rem(seq + offset, seqs) if offset else seq

    shifts = (half_groups, *range(half_groups - 1, -1, -1), *range(half_groups + 1, groups))

    def over_peers(body):
        for shift in shifts:
            to_group = lax.rem(group + shift, groups) if shift else group
            for offset in reversed(range(seqs)):
                if shift or offset:
                    body(to_group, turned_seq(offset), shift == 0)

    def signal(semaphore, to_group, to_seq):
        pl.semaphore_signal(
            semaphore, inc=1, device_id={"batch": to_group, "seq": to_seq}, device_id_type=MESH
        )

    barrier = pltpu.get_barrier_semaphore()

    def greet(to_group, to_seq, same):
        signal(barrier, to_group, to_seq)

    over_peers(greet)
    for copy in loads[2:]:
        copy.start()

    def transfer(source, target, kind, to_group, to_seq):
        return pltpu.make_async_remote_copy(
            src_ref=source,
            dst_ref=target,
            send_sem=send_sems.at[kind],
            recv_sem=recv_sems.at[kind],
            device_id={"batch": to_group, "seq": to_seq},
            device_id_type=MESH,
        )

    def all_of(buffer, blocks, kind):
        view = buffer.at[pl.ds(0, blocks)]
        return transfer(view, view, kind, group, turned_seq(1))

    @pl.when(upper == 0)
    def _():
        for where in range(groups):
            signal_in[where * seqs + half_seqs : (where + 1) * seqs] = jnp.zeros((half_seqs, own, rows), F32)

    @pl.when(upper == 1)
    def _():
        for where in range(groups):
            grad_in[where * seqs : where * seqs + half_seqs] = jnp.zeros((half_seqs, own, rows), F32)

    loads[GRAD].wait()
    grad_out_buf[...] = grad_ref[...].astype(F32).T.reshape(count, own, rows)
    loads[TAPS].wait()
    tap_out_buf[...] = tap_ref[...].T.reshape(count, own, rows)
    loads[SIGNAL].wait()
    signal_out_buf[...] = signal_ref[...].astype(F32).T.reshape(count, own, rows)
    pl.semaphore_wait(barrier, count - 1)

    def near_seq(ring):
        return upper * half_seqs + ring

    def far_seq(ring):
        return (1 - upper) * half_seqs + ring

    def far_block(shift, to_group, ring):
        to_seq, kind = far_seq(ring), CROSS if shift >= 2 else CROSS_OWN
        place = to_group * seqs + to_seq

        @pl.when(upper == 0)
        def _():
            transfer(signal_out_buf.at[place], signal_in.at[me], kind, to_group, to_seq).start()

        @pl.when(upper == 1)
        def _():
            transfer(grad_out_buf.at[place], grad_in.at[me], kind, to_group, to_seq).start()

    def far_taps(shift, to_group, ring):
        if shift == 0:
            place = group * seqs + far_seq(ring)
            transfer(tap_out_buf.at[place], tap_in.at[seq], TAPS, group, far_seq(ring)).start()

    def near_taps(shift, to_group, ring):
        if shift == 0:
            place = group * seqs + near_seq(ring)
            transfer(tap_out_buf.at[place], tap_in.at[seq], TAPS, group, near_seq(ring)).start()

    def near_grad_block(shift, to_group, ring):
        place = to_group * seqs + near_seq(ring)
        transfer(grad_out_buf.at[place], grad_in.at[me], GRAD, to_group, near_seq(ring)).start()

    def near_signal_block(shift, to_group, ring):
        place = to_group * seqs + near_seq(ring)
        transfer(signal_out_buf.at[place], signal_in.at[me], SIGNAL, to_group, near_seq(ring)).start()

    def mate_blocks(shift, to_group, ring):
        place, to_seq = to_group * seqs + far_seq(ring), near_seq(ring)
        transfer(grad_out_buf.at[place], near_grad_in.at[slot], NEAR_GRAD, to_group, to_seq).start()
        transfer(signal_out_buf.at[place], near_signal_in.at[slot], NEAR_SIGNAL, to_group, to_seq).start()

    def mate_taps(shift, to_group, ring):
        place, to_seq = group * seqs + far_seq(ring), near_seq(ring)
        if shift == 0:

            @pl.when(upper == 0)
            def _():
                transfer(tap_out_buf.at[place], near_tap_in.at[inner], NEAR_TAPS, group, to_seq).start()

    def in_turn(*sends):
        for shift in (*range(2, groups), 1, 0):
            to_group = 2 * lax.rem(pair + shift // 2, half_groups) + lax.rem(parity + shift, 2)
            for offset in reversed(range(half_seqs)):
                ring = lax.rem(inner + offset, half_seqs) if offset else inner
                for send in sends:
                    if shift or offset or send in (far_block, far_taps):
                        send(shift, to_group, ring)

    in_turn(far_taps, near_taps, mate_taps)
    in_turn(mate_blocks)
    in_turn(far_block, near_grad_block)
    in_turn(near_signal_block)
    grad_in[me] = grad_out_buf[me]
    tap_in[seq] = tap_out_buf[me]
    signal_in[me] = signal_out_buf[me]
    near_grad_in[slot] = grad_out_buf[group * seqs + mate]
    near_signal_in[slot] = signal_out_buf[group * seqs + mate]
    near_tap_in[inner] = tap_out_buf[group * seqs + mate]

    def spread(blocks, target, first_row):
        place = pl.ds(first_row, own)
        for k, (real, imag) in enumerate(coarse_forward(blocks)):
            row = k * (seqs // len(blocks))
            real, imag = turn(real, imag, cos_ref[row], sin_ref[row])
            target[k, place, re] = real
            target[k, place, im] = imag

    def fine(source, target):
        lines = source.shape[0] * source.shape[1]
        value = source[...].reshape(lines, 2 * rows)
        high = value.astype(BF16)
        low = (value - high.astype(F32)).astype(BF16)
        product = functools.partial(jnp.dot, preferred_element_type=F32)
        total = product(high, high_ref[...]) + product(low, high_ref[...]) + product(high, low_ref[...])
        target[...] = total.reshape(target.shape)

    def collect(source, first_row, pieces):
        place, stride = pl.ds(first_row, own), seqs // pieces
        terms = [
            turn(source[k, place, re], source[k, place, im], cos_ref[k * stride], sin_ref[k * stride])
            for k in range(pieces + 1)
        ]
        return coarse_inverse(terms, 1.0 / (2 * pieces * rows))

    def row_of(index):
        return pl.multiple_of(index * own, own)

    for copy in loads[3:]:
        copy.wait()
    all_of(tap_in, seqs - 1, TAPS).wait_recv()
    spread([tap_in[s] for s in range(seqs)], tap_rows, 0)
    fine(tap_rows, tap_spec)

    @pl.when(upper == 0)
    def _():
        all_of(near_tap_in, half_seqs - 1, NEAR_TAPS).wait_recv()
        spread([near_tap_in[s] for s in range(half_seqs)], near_tap, 0)
        fine(near_tap, near_tap)

    all_of(near_grad_in, near_count - 1, NEAR_GRAD).wait_recv()
    all_of(near_signal_in, near_count - 1, NEAR_SIGNAL).wait_recv()

    def spread_near(index, carry):
        for source, target in ((near_grad_in, near_grad), (near_signal_in, near_signal)):
            spread([source[index * half_seqs + s] for s in range(half_seqs)], target, row_of(index))
        return carry

    lax.fori_loop(0, groups, spread_near, 0)
    fine(near_grad, near_grad)
    fine(near_signal, near_signal)
    for k in range(half_seqs + 1):
        real, imag = None, None
        for index in range(groups):
            place = pl.ds(index * own, own)
            grad_re, grad_im = near_grad[k, place, re], near_grad[k, place, im]
            signal_re, signal_im = near_signal[k, place, re], near_signal[k, place, im]
            real = added(real, grad_re * signal_re + grad_im * signal_im)
            imag = added(imag, grad_re * signal_im - grad_im * signal_re)
        near_filter[k, :, re] = real
        near_filter[k, :, im] = imag
    fine(near_filter, near_filter)
    for s, block in enumerate(collect(near_filter, 0, half_seqs)):
        near_filter_out[s] = block
    transfer(near_filter_out, part_in, PART, group, mate).start()

    all_of(grad_in, near_count - 1, GRAD).wait_recv()
    own_far = 2 * half_seqs
    other_far = near_count - own_far
    pl.when(upper == 0)(lambda: all_of(grad_in, other_far, CROSS).wait_recv())

    def group_at(index):
        return lax.rem(2 * pair + index, groups)

    def input_part(first):
        source, spectrum, lines = grad_rows.at[first], grad_spec.at[first], input_rows.at[first]

        def spread_grad(index, carry):
            here = group_at(2 * first + index)
            spread([grad_in[here * seqs + s] for s in range(seqs)], source, row_of(index))
            return carry

        def transform():
            lax.fori_loop(0, 2, spread_grad, 0)
            fine(source, spectrum)

        def multiply_taps(index, carry):
            place = pl.ds(row_of(index), own)
            for k in range(coarse):
                grad_re, grad_im = spectrum[k, place, re], spectrum[k, place, im]
                tap_re, tap_im = tap_spec[k, :, re], tap_spec[k, :, im]
                lines[k, place, re] = grad_re * tap_re + grad_im * tap_im
                lines[k, place, im] = grad_re * tap_im - grad_im * tap_re
            return carry

        def collect_input(index, carry):
            here = group_at(2 * first + index)
            for s, block in enumerate(collect(lines, row_of(index), seqs)):
                input_out[here * seqs + s] = block
            return carry

        def finish():
            lax.fori_loop(0, 2, multiply_taps, 0)
            fine(lines, lines)
            lax.fori_loop(0, 2, collect_input, 0)

            for offset in turns:
                for flip in range(2):
                    if first or offset or flip:
                        to_group = group_at(2 * first + lax.rem(parity + flip, 2))
                        to_seq = turned_seq(offset)
                        place = to_group * seqs + to_seq
                        transfer(input_out.at[place], input_in.at[me], INPUT, to_group, to_seq).start()

        return transform, finish

    parts = [input_part(first) for first in reversed(range(half_groups))]
    parts[0][0]()
    parts[0][1]()

    @pl.when(upper == 0)
    def _():
        def multiply_near(index, carry):
            place = pl.ds(row_of(index), own)
            for k in range(half_seqs + 1):
                grad_re, grad_im = near_grad[k, place, re], near_grad[k, place, im]
                tap_re, tap_im = near_tap[k, :, re], near_tap[k, :, im]
                near_lines[k, place, re] = grad_re * tap_re + grad_im * tap_im
                near_lines[k, place, im] = grad_re * tap_im - grad_im * tap_re
            return carry

        lax.fori_loop(0, groups, multiply_near, 0)
        fine(near_lines, near_lines)

        def collect_near(index, carry):
            for s, block in enumerate(collect(near_lines, row_of(index), half_seqs)):
                near_input_out[index * half_seqs + s] = block
            return carry

        lax.fori_loop(0, groups, collect_near, 0)
        for shift in shifts:
            to_group = lax.rem(group + shift, groups) if shift else group
            for offset in reversed(range(half_seqs)):
                if shift or offset:
                    ring = lax.rem(inner + offset, half_seqs)
                    transfer(
                        near_input_out.at[to_group * half_seqs + ring], near_input_in.at[slot],
                        NEAR_INPUT, to_group, ring,
                    ).start()
        near_input_in[slot] = near_input_out[slot]

    pl.when(upper == 0)(lambda: all_of(grad_in, own_far, CROSS_OWN).wait_recv())
    for transform, _ in parts[1:]:
        transform()

    all_of(signal_in, near_count - 1, SIGNAL).wait_recv()

    @pl.when(upper == 1)
    def _():
        all_of(signal_in, other_far, CROSS).wait_recv()
        all_of(signal_in, own_far, CROSS_OWN).wait_recv()


    def spread_signal(index, carry):
        here = group_at(index)
        spread([signal_in[here * seqs + s] for s in range(seqs)], signal_rows, row_of(index))
        return carry

    lax.fori_loop(0, groups, spread_signal, 0)
    fine(signal_rows, signal_spec)
    for k in range(coarse):
        real, imag = None, None
        for index in range(groups):
            place = pl.ds(index * own, own)
            which, local = index // 2, pl.ds(index % 2 * own, own)
            grad_re, grad_im = grad_spec[which, k, local, re], grad_spec[which, k, local, im]
            signal_re, signal_im = signal_spec[k, place, re], signal_spec[k, place, im]
            real = added(real, grad_re * signal_re + grad_im * signal_im)
            imag = added(imag, grad_re * signal_im - grad_im * signal_re)
        filter_rows[k, :, re] = real
        filter_rows[k, :, im] = imag
    fine(filter_rows, filter_spec)
    all_of(part_in, half_seqs, PART).wait_recv()
    for s, block in enumerate(collect(filter_spec, 0, seqs)):
        filter_out[s] = block + part_in[s] if s < half_seqs else block

    for offset in turns:
        for flip in range(half_groups):
            if offset or flip:
                to_group = 2 * lax.rem(pair + flip, half_groups) + parity
                to_seq = turned_seq(offset)
                transfer(
                    filter_out.at[to_seq], filter_in.at[parity, pair * seqs + seq], FILTER, to_group, to_seq
                ).start()
    for _, finish in parts[1:]:
        finish()
    input_in[me] = input_out[me]
    filter_in[parity, pair * seqs + seq] = filter_out[seq]

    half = count // 2
    all_of(filter_in.at[0], half - 1, FILTER).wait_recv()
    mine = filter_in.at[parity]
    partner = 2 * pair + 1 - parity
    forward = transfer(mine, mine, FORWARD, partner, seq)
    forward.start()
    all_of(input_in, count - 1, INPUT).wait_recv()

    @pl.when(upper == 0)
    def _():
        all_of(near_input_in, near_count - 1, NEAR_INPUT).wait_recv()
        for where in range(groups):
            far = slice(where * seqs + half_seqs, (where + 1) * seqs)
            input_in[far] = input_in[far] + near_input_in[where * half_seqs : (where + 1) * half_seqs]

    gradient = input_in[...].reshape(channels, rows).T + skip_ref[...] * grad_ref[...].astype(F32)
    input_ref[...] = gradient.astype(BF16)
    forward.wait_recv()
    for kind in (GRAD, SIGNAL, NEAR_GRAD, NEAR_SIGNAL):
        all_of(grad_in, near_count - 1, kind).wait_send()
    all_of(grad_in, other_far, CROSS).wait_send()
    all_of(grad_in, own_far, CROSS_OWN).wait_send()
    all_of(part_in, half_seqs, PART).wait_send()

    @pl.when(upper == 0)
    def _():
        all_of(grad_in, near_count - 1, NEAR_INPUT).wait_send()
        all_of(tap_in, half_seqs - 1, NEAR_TAPS).wait_send()

    all_of(input_in, count - 1, INPUT).wait_send()
    all_of(filter_in.at[0], half - 1, FILTER).wait_send()
    forward.wait_send()
    all_of(tap_in, seqs - 1, TAPS).wait_send()


def finish_kernel(groups, seqs, input_ref, filter_in, input_hbm, filter_hbm, filter_ref, sems):
    own, rows = filter_in.shape[2:]
    input_store = pltpu.make_async_copy(input_ref, input_hbm, sems.at[0])
    input_store.start()
    parts = [
        filter_in[which, first * seqs : (first + 1) * seqs].reshape(seqs * own, rows)
        for first in range(groups // 2)
        for which in range(2)
    ]
    filter_ref[...] = jnp.concatenate(parts, axis=0).T
    filter_store = pltpu.make_async_copy(filter_ref, filter_hbm, sems.at[1])
    filter_store.start()
    input_store.wait()
    filter_store.wait()


def fine_tables(rows):
    grid = np.arange(rows)
    angle = 2.0 * np.pi / rows * (np.outer(grid, grid) % rows)
    table = np.block([[np.cos(angle), -np.sin(angle)], [np.sin(angle), np.cos(angle)]]).astype(np.float32)
    high = table.astype(BF16)
    return high, (table - high.astype(np.float32)).astype(BF16)


def turn_tables(seqs, rows, lines):
    angle = np.pi / (seqs * rows) * np.outer(np.arange(seqs + 1), np.arange(rows))
    wide = np.broadcast_to(angle[:, None, :], (seqs + 1, lines, rows))
    return np.cos(wide).astype(np.float32), np.sin(wide).astype(np.float32)


def fused_shards(groups, seqs, signal, grad_out, filter_taps, skip_gain):
    rows, channels = filter_taps.shape
    count, coarse = groups * seqs, seqs + 1
    own = channels // count
    high, low = fine_tables(rows)
    cos_turn, sin_turn = turn_tables(seqs, rows, own)
    blocks = pltpu.VMEM((count, own, rows), F32)
    few = pltpu.VMEM((seqs, own, rows), F32)
    half_blocks = pltpu.VMEM((count // 2, own, rows), F32)
    half_few = pltpu.VMEM((seqs // 2, own, rows), F32)
    near = lambda number: pltpu.VMEM((seqs // 2 + 1, number * own, 2 * rows), F32)
    lines = lambda number: pltpu.VMEM((coarse, number * own, 2 * rows), F32)
    pairs = pltpu.VMEM((groups // 2, coarse, 2 * own, 2 * rows), F32)
    hbm = pl.BlockSpec(memory_space=pltpu.HBM)
    turns = pltpu.VMEM((coarse, own, rows), F32)
    table = pltpu.VMEM((2 * rows, 2 * rows), BF16)
    vmem = pl.BlockSpec(memory_space=pltpu.VMEM)
    gathered = pl.pallas_call(
        functools.partial(fused_kernel, groups, seqs),
        out_shape=(
            pltpu.VMEM((rows, channels), BF16),
            pltpu.VMEM((2, count // 2, own, rows), F32),
        ),
        in_specs=[hbm] * 8,
        out_specs=(vmem, vmem),
        scratch_shapes=[
            pltpu.VMEM((rows, channels), BF16), pltpu.VMEM((rows, channels), BF16),
            pltpu.VMEM((rows, channels), F32), pltpu.VMEM((1, channels), F32),
            table, table, turns, turns,
            blocks, blocks, blocks, blocks, blocks, few,
            blocks, few, blocks,
            lines(1), lines(1), pairs, pairs, lines(groups), lines(groups),
            pairs, lines(1), lines(1),
            half_blocks, half_blocks, half_few, half_blocks, half_blocks, half_few, half_few,
            near(groups), near(groups), near(1), near(groups), near(1),
            pltpu.SemaphoreType.DMA((13,)),
            pltpu.SemaphoreType.DMA((13,)),
            pltpu.SemaphoreType.DMA((8,)),
        ],
        compiler_params=pltpu.CompilerParams(
            collective_id=0, has_side_effects=True, vmem_limit_bytes=24 << 20
        ),
    )(
        *(
            pltpu.with_memory_space_constraint(array, pltpu.HBM)
            for array in (
                signal[0], grad_out[0], filter_taps, skip_gain[None, :],
                jnp.asarray(high), jnp.asarray(low), jnp.asarray(cos_turn), jnp.asarray(sin_turn),
            )
        )
    )
    input_grad, filter_grad = pl.pallas_call(
        functools.partial(finish_kernel, groups, seqs),
        out_shape=(
            jax.ShapeDtypeStruct((rows, channels), BF16),
            jax.ShapeDtypeStruct((rows, channels), F32),
        ),
        in_specs=[vmem] * 2,
        out_specs=(hbm, hbm),
        scratch_shapes=[
            pltpu.VMEM((rows, channels), F32),
            pltpu.SemaphoreType.DMA((2,)),
        ],
        compiler_params=pltpu.CompilerParams(vmem_limit_bytes=24 << 20),
    )(*gathered)
    return input_grad[None], filter_grad


def fits_fused(groups, seqs, signal, filter_taps):
    rows, channels = filter_taps.shape
    return (
        signal.shape[0] == 1
        and seqs % 4 == 0
        and groups % 2 == 0
        and groups > 2
        and rows % 128 == 0
        and channels % (8 * groups * seqs) == 0
    )


def angle_table(height, width, period):
    product = lax.broadcasted_iota(jnp.int32, (height, width), 0) * lax.broadcasted_iota(
        jnp.int32, (height, width), 1
    )
    return 2.0 * jnp.pi / period * (product % period).astype(jnp.float32)


def angle_of(product, period):
    return 2.0 * jnp.pi / period * (product % period).astype(jnp.float32)


def coarse_order(slot, seq_count):
    pair_index = slot // 2
    odd_slot = slot % 2
    return jnp.where(
        pair_index == 0,
        odd_slot * seq_count,
        jnp.where(odd_slot == 0, pair_index, 2 * seq_count - pair_index),
    )


def contract(form, table, operand):
    return jnp.einsum(form, table, operand, precision=lax.Precision.HIGHEST)


def forward_spectra(columns):
    seq_count = lax.axis_size("seq")
    row_count = columns.shape[0]
    part_rows = row_count // seq_count
    period_len = 2 * row_count * seq_count
    spread = lax.all_to_all(
        columns.reshape(1, row_count, columns.shape[1]),
        "seq",
        split_axis=1,
        concat_axis=0,
        tiled=True,
    )
    slot_grid = lax.broadcasted_iota(jnp.int32, (2 * seq_count, seq_count), 0)
    source_grid = lax.broadcasted_iota(jnp.int32, (2 * seq_count, seq_count), 1)
    first_table = angle_of(coarse_order(slot_grid, seq_count) * source_grid, 2 * seq_count)
    cos_first = jnp.cos(first_table)
    sin_first = jnp.sin(first_table)
    half_width = spread.shape[2] // 2
    real_in = spread[:, :, :half_width]
    imag_in = spread[:, :, half_width:]
    real_part = contract("ks,srw->krw", cos_first, real_in) + contract(
        "ks,srw->krw", sin_first, imag_in
    )
    imag_part = contract("ks,srw->krw", cos_first, imag_in) - contract(
        "ks,srw->krw", sin_first, real_in
    )
    global_row = lax.axis_index("seq") * part_rows + lax.broadcasted_iota(
        jnp.int32, (2 * seq_count, part_rows), 1
    )
    coarse = coarse_order(lax.broadcasted_iota(jnp.int32, (2 * seq_count, part_rows), 0), seq_count)
    phases = angle_of(global_row * coarse, period_len)
    cos_turn = jnp.cos(phases)[:, :, None]
    sin_turn = jnp.sin(phases)[:, :, None]
    rotated = jnp.stack(
        [real_part * cos_turn + imag_part * sin_turn, imag_part * cos_turn - real_part * sin_turn]
    )
    inner_table = angle_table(row_count, row_count, row_count)
    cos_inner = jnp.cos(inner_table)
    sin_inner = jnp.sin(inner_table)
    pieces = lax.all_to_all(rotated, "seq", split_axis=1, concat_axis=2, tiled=True)
    real_sum = contract("qr,krw->kqw", cos_inner, pieces[0]) + contract(
        "qr,krw->kqw", sin_inner, pieces[1]
    )
    imag_sum = contract("qr,krw->kqw", cos_inner, pieces[1]) - contract(
        "qr,krw->kqw", sin_inner, pieces[0]
    )
    return jnp.stack([real_sum, imag_sum])


def split_pairs(packed):
    reversed_q = packed[:, :, ::-1]
    zero_row = jnp.roll(reversed_q[:, 0], 1, axis=1)
    own_pair = jnp.stack([zero_row, reversed_q[:, 1]], axis=1)
    partner = jnp.where(lax.axis_index("seq") == 0, own_pair, reversed_q[:, ::-1])
    first = jnp.stack([0.5 * (packed[0] + partner[0]), 0.5 * (packed[1] - partner[1])])
    second = jnp.stack([0.5 * (packed[1] + partner[1]), 0.5 * (partner[0] - packed[0])])
    return (first, second)


def inverse_rows(spectra):
    seq_count = lax.axis_size("seq")
    row_count = spectra.shape[2]
    period_len = 2 * row_count * seq_count
    inner_table = angle_table(row_count, row_count, row_count)
    cos_inner = jnp.cos(inner_table)
    sin_inner = jnp.sin(inner_table)
    real_sum = contract("qr,krw->kqw", cos_inner, spectra[0]) - contract(
        "qr,krw->kqw", sin_inner, spectra[1]
    )
    imag_sum = contract("qr,krw->kqw", cos_inner, spectra[1]) + contract(
        "qr,krw->kqw", sin_inner, spectra[0]
    )
    coarse = coarse_order(
        2 * lax.axis_index("seq") + lax.broadcasted_iota(jnp.int32, (2, row_count), 0), seq_count
    )
    position = lax.broadcasted_iota(jnp.int32, (2, row_count), 1)
    phases = angle_of(position * coarse, period_len)
    cos_turn = jnp.cos(phases)[:, :, None]
    sin_turn = jnp.sin(phases)[:, :, None]
    rotated = jnp.stack(
        [real_sum * cos_turn - imag_sum * sin_turn, real_sum * sin_turn + imag_sum * cos_turn]
    )
    target_grid = lax.broadcasted_iota(jnp.int32, (seq_count, 2 * seq_count), 0)
    slot_grid = lax.broadcasted_iota(jnp.int32, (seq_count, 2 * seq_count), 1)
    last_table = angle_of(target_grid * coarse_order(slot_grid, seq_count), 2 * seq_count)
    cos_last = jnp.cos(last_table)
    sin_last = jnp.sin(last_table)
    pieces = lax.all_to_all(rotated, "seq", split_axis=2, concat_axis=1, tiled=True)
    value = contract("sk,krw->srw", cos_last, pieces[0]) - contract(
        "sk,krw->srw", sin_last, pieces[1]
    )
    other = contract("sk,krw->srw", sin_last, pieces[0]) + contract(
        "sk,krw->srw", cos_last, pieces[1]
    )
    gathered = (value / period_len, other / period_len)
    gathered = jnp.concatenate([gathered[0], gathered[1]], axis=2)
    home_rows = lax.all_to_all(gathered, "seq", split_axis=0, concat_axis=1, tiled=True)
    return home_rows.reshape(row_count, home_rows.shape[2])


def invert_all(spectra):
    half_width = spectra.shape[3] // 2
    joined = jnp.stack(
        [
            spectra[0, :, :, :half_width] - spectra[1, :, :, half_width:],
            spectra[1, :, :, :half_width] + spectra[0, :, :, half_width:],
        ]
    )
    return inverse_rows(joined)


def shards(signal, grad_out, filter_taps, skip_gain):
    channels = filter_taps.shape[1]
    signal_rows = signal[0].astype(jnp.float32)
    grad_rows = grad_out[0].astype(jnp.float32)
    tap_half = filter_taps.shape[1] // 2
    columns = jnp.concatenate(
        [signal_rows, filter_taps[:, :tap_half], grad_rows, filter_taps[:, tap_half:]], axis=1
    )
    first, second = split_pairs(forward_spectra(columns))
    signal_spec = first[:, :, :, :channels]
    grad_spec = second[:, :, :, :channels]
    own_spec = jnp.concatenate([first[:, :, :, channels:], second[:, :, :, channels:]], axis=3)
    input_spec = jnp.stack(
        [
            grad_spec[0] * own_spec[0] + grad_spec[1] * own_spec[1],
            grad_spec[1] * own_spec[0] - grad_spec[0] * own_spec[1],
        ]
    )
    filter_terms = jnp.stack(
        [
            grad_spec[0] * signal_spec[0] + grad_spec[1] * signal_spec[1],
            grad_spec[1] * signal_spec[0] - grad_spec[0] * signal_spec[1],
        ]
    )
    summed = lax.psum(filter_terms, "batch")
    rows_back = invert_all(jnp.concatenate([input_spec, summed], axis=3))
    filter_grad = rows_back[:, channels:]
    input_grad = (rows_back[:, :channels] + skip_gain[None, :] * grad_rows).astype(jnp.bfloat16)
    return (input_grad[None], filter_grad)


def solution(mesh):
    groups, seqs = mesh.shape["batch"], mesh.shape["seq"]

    def either(signal, grad_out, filter_taps, skip_gain):
        if fits_fused(groups, seqs, signal, filter_taps):
            return fused_shards(groups, seqs, signal, grad_out, filter_taps, skip_gain)
        return shards(signal, grad_out, filter_taps, skip_gain)

    return jax.shard_map(
        either,
        mesh=mesh,
        in_specs=(P("batch", "seq", None), P("batch", "seq", None), P("seq", None), P()),
        out_specs=(P("batch", "seq", None), P("seq", None)),
        check_vma=False,
    )
```
